256 devices in a mesh: lat: 8 (over x_lo, y), lon: 16 (over x_hi, z), lev: 2 (over core).
Axes of the slice: x: 4 (x_hi: 2, x_lo: 2; x = x_hi * 2 + x_lo), y: 4, z: 8, core: 2. Of those that a mesh axis runs over, the one named last changes fastest.
Arguments:
- increment: float32 [80, 128, 2048], P('lev', 'lat', 'lon'), may hold values from -6 to 6
- wind_u: float32 [80, 128, 2048], P('lev', 'lat', 'lon'), may hold values from -0.4 to 0.4
- wind_v: float32 [80, 128, 2048], P('lev', 'lat', 'lon'), may hold values from -0.4 to 0.4
- diffusion: float32 [80], P('lev'), may hold values from 0.02 to 0.2
- mixing: float32 [80, 80], P('lev'), may hold values from -0.15625 to 0.15625
- jacobian: bfloat16 [128, 80], P(None, 'lev'), may hold values from -0.625 to 0.625
- obs_weight: float32 [128], replicated, may hold values from 0.5 to 4
- innovation: bfloat16 [2, 8, 16, 16, 128, 128], P(None, 'lat', 'lon'), may hold values from -6 to 6
- counts: int32 [8, 16], P('lat', 'lon'), may hold values from 1 to 16, as said below
- column_lookup: int32 [8, 16, 2048], P('lat', 'lon'), may hold values from 0 to 2047, each once within a row
Outputs:
- gradient: float32 [80, 128, 2048], P('lev', 'lat', 'lon')
- cost: float32 [], replicated
The draws below stay inside these ranges and needn't reach their ends.
Inputs may be any that keep to these rules, and one draw needn't show every extreme that they name: In every row of tiles with one latitude index the counts sum to 96, and the largest of them is 16.
All inputs are finite; a program needn't handle non-finite values.
Results may differ from the reference program's by a relative error of at most 0.005.
Values may be sent and summed in bfloat16 or wider, within the bound.
A program may use at most 64 MiB of HBM per device.

```python
import math
import jax
import jax.numpy as jnp
from jax import lax

MODEL_LEVELS = 80
CHANNEL_TOTAL = 128
WINDOW_STEPS = 2
BLOCK_COLUMNS = 128
CLON = 128
CLAT = 16
SLOTS_PER_TILE = 16
MEAN_LIVE_BLOCKS = 6
LATITUDE_TILES = 8
LONGITUDE_TILES = 16
NLAT = 128
NLON = 2048


def draw_counts(key, part):
    folded = jax.random.fold_in(key, 7331)
    key_swath, key_extra = jax.random.split(folded, 2)
    swath = jax.random.randint(key_swath, (LATITUDE_TILES,), 0, LONGITUDE_TILES)
    place = jnp.arange(LONGITUDE_TILES, dtype=jnp.int32)[None, :]
    swath_flag = place == swath[:, None]
    remaining_slots = MEAN_LIVE_BLOCKS * LONGITUDE_TILES - SLOTS_PER_TILE
    tile_portion = remaining_slots // (LONGITUDE_TILES - 1)
    leftover = remaining_slots - tile_portion * (LONGITUDE_TILES - 1)
    scores = jax.random.randint(key_extra, (LATITUDE_TILES, LONGITUDE_TILES), 0, 1 << 20) * LONGITUDE_TILES + place
    scores = jnp.where(swath_flag, -1, scores)
    order = jnp.argsort(-scores, axis=1)
    ranks = jnp.argsort(order, axis=1)
    surplus_blocks = (ranks < leftover).astype(jnp.int32)
    return jnp.where(swath_flag, SLOTS_PER_TILE, tile_portion + surplus_blocks).astype(jnp.int32)


def steps_of(own_key, extent, pieces, low, high):
    level, own = 1.0, jax.random.fold_in(own_key, 6)
    for position, parts in pieces:
        steps = jnp.exp(jax.random.uniform(jax.random.fold_in(own, position), (parts,), jnp.float32, low / len(pieces), high / len(pieces)))
        level = level * jnp.repeat(steps, extent[position] // parts).reshape([-1 if axis == position else 1 for axis in range(len(extent))])
    return level


def bell_draw(stream_key, shape, deviation, limit, shards=(), held_as=jnp.bfloat16):
    factor_of = steps_of(stream_key, shape, shards, -0.22, 0.18) if shards else 1.0
    values = jax.random.normal(stream_key, shape, jnp.float32) * deviation * factor_of
    return jnp.minimum(jnp.maximum(values, -limit), limit).astype(held_as)


def setup_inputs(seed: int = 0) -> dict:
    streams_of = jax.random.split(jax.random.key(seed), 11)
    return {
        "increment": bell_draw(streams_of[0], (MODEL_LEVELS, NLAT, NLON), 1.0, 6.0, ((0, 2), (1, 8), (2, 16)), jnp.float32),
        "wind_u": jnp.clip(jax.random.uniform(streams_of[1], (MODEL_LEVELS, NLAT, NLON), jnp.float32, -0.4, 0.4) * steps_of(streams_of[1], (MODEL_LEVELS, NLAT, NLON), ((0, 2), (1, 8), (2, 16)), -0.4, 0.0), -0.4, 0.4),
        "wind_v": jnp.clip(jax.random.uniform(streams_of[2], (MODEL_LEVELS, NLAT, NLON), jnp.float32, -0.4, 0.4) * steps_of(streams_of[2], (MODEL_LEVELS, NLAT, NLON), ((0, 2), (1, 8), (2, 16)), -0.4, 0.0), -0.4, 0.4),
        "diffusion": jnp.clip(jnp.exp(math.log(0.2) - 2.3025851 * jax.random.uniform(streams_of[3], (MODEL_LEVELS,), jnp.float32) ** steps_of(streams_of[3], (MODEL_LEVELS,), ((0, 2),), -0.2, 0.2)), 0.02, 0.2),
        "mixing": bell_draw(streams_of[4], (MODEL_LEVELS, MODEL_LEVELS), (16 * MODEL_LEVELS) ** -0.5, 0.15625, ((0, 2),), jnp.float32),
        "jacobian": bell_draw(streams_of[5], (CHANNEL_TOTAL, MODEL_LEVELS), MODEL_LEVELS ** -0.5, 0.625, ((1, 2),)),
        "obs_weight": jnp.clip(jnp.exp(jax.random.uniform(streams_of[6], (CHANNEL_TOTAL,), jnp.float32, math.log(0.5), math.log(4.0))), 0.5, 4.0),
        "innovation": bell_draw(streams_of[7], (WINDOW_STEPS, LATITUDE_TILES, LONGITUDE_TILES, SLOTS_PER_TILE, CHANNEL_TOTAL, BLOCK_COLUMNS), 1.0, 6.0, ((1, 8), (2, 16))),
        "counts": draw_counts(jax.random.fold_in(streams_of[10], 71), 0),
        "column_lookup": jax.vmap(lambda own: jax.random.permutation(own, SLOTS_PER_TILE * BLOCK_COLUMNS))(jax.random.split(streams_of[9], LATITUDE_TILES * LONGITUDE_TILES)).reshape((LATITUDE_TILES, LONGITUDE_TILES, SLOTS_PER_TILE * BLOCK_COLUMNS)).astype(jnp.int32),
    }


def horizontal(field, diffusion, wind_u, wind_v):
    lat_pad = jnp.pad(field, ((0, 0), (1, 1), (0, 0)))
    northern = lat_pad[:, 2:, :]
    southern = lat_pad[:, :-2, :]
    eastern = jnp.roll(field, -1, axis=2)
    western = jnp.roll(field, 1, axis=2)
    coefficient = diffusion[:, None, None]
    result = field + coefficient * (northern + southern + eastern + western - 4.0 * field)
    return result - 0.5 * wind_u * (eastern - western) - 0.5 * wind_v * (northern - southern)

def vertical(smooth, mixing):
    flat = smooth.reshape(MODEL_LEVELS, -1)
    mixed = jnp.dot(mixing, flat, precision=lax.Precision.HIGHEST, preferred_element_type=jnp.float32)
    return smooth + mixed.reshape(smooth.shape)

def to_tiles(field):
    shaped = field.reshape(MODEL_LEVELS, LATITUDE_TILES, CLAT, LONGITUDE_TILES, CLON).transpose(1, 3, 0, 2, 4)
    return shaped.reshape(LATITUDE_TILES, LONGITUDE_TILES, MODEL_LEVELS, CLAT * CLON)

def from_tiles(tiled):
    shaped = tiled.reshape(LATITUDE_TILES, LONGITUDE_TILES, MODEL_LEVELS, CLAT, CLON).transpose(2, 0, 3, 1, 4)
    return shaped.reshape(MODEL_LEVELS, NLAT, NLON)

def pick_columns(tiled, table):
    return jax.vmap(jax.vmap(lambda field, index: jnp.take(field, index, axis=1)))(tiled, table)

def reference(increment, wind_u, wind_v, diffusion, mixing, jacobian, obs_weight, innovation, counts, column_lookup):
    jac_wide = jacobian.astype(jnp.float32)
    active_blocks = (jnp.arange(SLOTS_PER_TILE)[None, None, :] < counts[:, :, None]).astype(jnp.float32)
    inverse = jnp.argsort(column_lookup, axis=2).astype(jnp.int32)
    state = increment
    forcings = []
    misfit_total = jnp.zeros((), jnp.float32)
    for step in range(WINDOW_STEPS):
        state = vertical(horizontal(state, diffusion, wind_u, wind_v), mixing)
        selected_columns = pick_columns(to_tiles(state), column_lookup)
        column_profile = selected_columns.astype(jnp.bfloat16).reshape(LATITUDE_TILES, LONGITUDE_TILES, MODEL_LEVELS, SLOTS_PER_TILE, BLOCK_COLUMNS)
        column_profile = lax.optimization_barrier(column_profile).astype(jnp.float32)
        evolved = jnp.einsum('nl,ijlsc->ijsnc', jac_wide, column_profile, precision=lax.Precision.HIGHEST)
        misfit = active_blocks[..., None, None] * (evolved - innovation[step].astype(jnp.float32))
        scaled = obs_weight[:, None] * misfit
        misfit_total = misfit_total + jnp.sum(misfit * scaled)
        scaled_half = lax.optimization_barrier(scaled.astype(jnp.bfloat16)).astype(jnp.float32)
        return_path = jnp.einsum('nl,ijsnc->ijlsc', jac_wide, scaled_half, precision=lax.Precision.HIGHEST)
        return_path = return_path.astype(jnp.bfloat16)
        dispersed_blocks = lax.optimization_barrier(return_path).astype(jnp.float32).reshape(LATITUDE_TILES, LONGITUDE_TILES, MODEL_LEVELS, SLOTS_PER_TILE * BLOCK_COLUMNS)
        forcings.append(from_tiles(pick_columns(dispersed_blocks, inverse)))
    zero_field = jnp.zeros_like(increment)
    adjoint = zero_field
    for step in range(WINDOW_STEPS - 1, -1, -1):
        adjoint = adjoint + forcings[step]
        coupled = adjoint + jnp.dot(mixing.T, adjoint.reshape(MODEL_LEVELS, -1), precision=lax.Precision.HIGHEST, preferred_element_type=jnp.float32).reshape(adjoint.shape)
        pullback = jax.vjp(lambda field: horizontal(field, diffusion, wind_u, wind_v), zero_field)[1]
        adjoint = pullback(coupled)[0]
    gradient = increment + adjoint
    cost = (0.5 * jnp.sum(increment * increment) + 0.5 * misfit_total) / (MODEL_LEVELS * NLAT * NLON)
    return (gradient, cost)
```

```python
import functools

import jax
import jax.numpy as jnp
from jax import lax
from jax.experimental import pallas as pl
from jax.experimental.pallas import tpu as pltpu
from jax.sharding import PartitionSpec as P

F32 = jnp.float32
BF16 = jnp.bfloat16
MESH = pl.DeviceIdType.MESH
HALO = 4
GROUPS = (0, 3, 6, 8, 10, 13)
LANES = 128


def dot(a, b):
    return lax.dot_general(a, b, (((1,), (0,)), ((), ())), preferred_element_type=F32)


def dot_nt(a, b):
    return lax.dot_general(a, b, (((1,), (1,)), ((), ())), preferred_element_type=F32)


def dot_tn(a, b):
    return lax.dot_general(a, b, (((0,), (0,)), ((), ())), preferred_element_type=F32)


def iota(shape, dim):
    return lax.broadcasted_iota(jnp.int32, shape, dim)


def one_hot(condition):
    return jnp.where(condition, 1.0, 0.0).astype(BF16)


def at_row(e):
    return slice(LANES * e, LANES * (e + 1))


def kernel(
    sizes,
    inc_h, u_h, v_h, dif_h, mix_h, jac_h, w_h, y_h, cnt_s, lut_h,
    out_ref, cost_ref,
    inc, u, v, dif, mix, jac, w, y, lut,
    own, partner, misc, misc_in, full,
    south, north, south_in, north_in,
    strip_e, strip_w, strip_in, strip_s, strip_n,
    slots, pick, grid, grid_s, grid_n, edge, edge_in, edge_s, edge_n,
    x0, x1, hu, hv, sm, f1, back, back_in,
    load_sem, send_sem, recv_sem,
):
    nlat, nlon, half, rows = sizes
    full_levels = 2 * half
    i, j, h = lax.axis_index("lat"), lax.axis_index("lon"), lax.axis_index("lev")
    other = 1 - h
    up, down = lax.rem(i + 1, nlat), lax.rem(i + nlat - 1, nlat)
    east, west = lax.rem(j + 1, nlon), lax.rem(j + nlon - 1, nlon)
    side = lax.rem(j + nlon - 1 + 2 * h, nlon)

    barrier = pltpu.get_barrier_semaphore()
    senders = [(up, j, h), (down, j, h), (i, j, other)]
    senders += [(a, side, k) for a in (i, up, down) for k in (0, 1)]
    for device in senders:
        pl.semaphore_signal(barrier, inc=1, device_id=device, device_id_type=MESH)

    loads = {}
    pairs = ((inc_h, inc), (u_h, u), (v_h, v), (dif_h, dif), (mix_h, mix), (jac_h, jac), (w_h, w), (lut_h, lut), (y_h, y))
    for n, (source, target) in enumerate(pairs):
        loads[n] = pltpu.make_async_copy(source, target, load_sem.at[n])
        loads[n].start()

    def remote(n, source, target, device, arrival=None):
        return pltpu.make_async_remote_copy(
            src_ref=source,
            dst_ref=target,
            send_sem=send_sem.at[n],
            recv_sem=recv_sem.at[n if arrival is None else arrival],
            device_id=device,
            device_id_type=MESH,
        )

    for n in range(3):
        loads[n].wait()
    fields = (inc, u, v)

    def own_row(f, r):
        value = fields[f][pl.ds(r, half, stride=rows), :]
        return value if f == 0 else 0.5 * value

    for q in range(rows // 2):
        for f in range(3):
            own[f, q] = jnp.concatenate([own_row(f, 2 * q), own_row(f, 2 * q + 1)], axis=0).astype(BF16)

    wide = (32, 3 * LANES)
    number, lane = iota(wide, 0), iota(wide, 1)
    inner = number & 15
    west_edge = number >> 4
    spot = (inner >> 2) * LANES + (inner & 3) + (1 - west_edge) * (LANES - HALO)
    selector = one_hot((spot == lane) & (inner < 12))
    for g, start in enumerate(GROUPS):
        block = jnp.concatenate(
            [
                jnp.concatenate([own_row(f, start + t) for t in range(3)], axis=0).astype(BF16)
                for f in range(3)
            ],
            axis=1,
        )
        strip = dot_nt(selector, block).astype(BF16)
        strip_e[g, :, 0 : 3 * half] = strip[0:16]
        strip_w[g, :, 0 : 3 * half] = strip[16:32]
        strip_e[g, :, 3 * half : LANES] = jnp.zeros((16, LANES - 3 * half), BF16)
        strip_w[g, :, 3 * half : LANES] = jnp.zeros((16, LANES - 3 * half), BF16)

    for n in range(3, 8):
        loads[n].wait()
    misc[0] = jnp.zeros((half, LANES), F32)
    misc[0, :, 0:full_levels] = mix[...]
    eye = iota((half, half), 0) == iota((half, half), 1)
    misc[1] = dot_nt(one_hot(eye), jac[...])
    column = jnp.sum(jnp.where(eye, dif[...], 0.0), axis=1, keepdims=True)
    misc[2] = jnp.broadcast_to(column, (half, LANES))

    pl.semaphore_wait(barrier, len(senders))

    copies = [
        remote(2, own.at[:, 6:8], south, (up, j, h)),
        remote(3, own.at[:, 0:2], north, (down, j, h)),
        remote(6, strip_e, strip_in.at[h], (i, east, 0), 6 + h),
        remote(7, strip_w, strip_in.at[h], (i, west, 1), 6 + h),
        remote(8, strip_e.at[5], strip_s.at[h], (up, east, 0), 8 + h),
        remote(9, strip_e.at[0], strip_n.at[h], (down, east, 0), 10 + h),
        remote(10, strip_w.at[5], strip_s.at[h], (up, west, 1), 8 + h),
        remote(11, strip_w.at[0], strip_n.at[h], (down, west, 1), 10 + h),
        remote(1, misc, misc_in, (i, j, other)),
        remote(0, own, partner, (i, j, other)),
    ]
    for copy in copies:
        copy.start()

    table = lut[...]
    low = dot_nt(one_hot(iota((LANES, LANES), 0) == iota((LANES, LANES), 1)), (table & 255).astype(F32).astype(BF16))
    pair_lane = iota((LANES, 2 * LANES), 1).astype(F32)
    for s in range(16):
        pick[LANES * s : LANES * (s + 1)] = one_hot(jnp.broadcast_to(low[:, s : s + 1], (LANES, 2 * LANES)) == pair_lane)
    pair_of = (table >> 8).astype(F32)

    count = cnt_s[0, 0]
    live = [jnp.where(count > s, 1.0, 0.0).astype(F32) for s in range(16)]
    loads[8].wait()
    w_row = w[...]
    w_column = jnp.sum(
        jnp.where(iota((LANES, LANES), 0) == iota((LANES, LANES), 1), w_row, 0.0), axis=1, keepdims=True
    )
    squares = jnp.zeros((LANES, LANES), F32)
    for s in range(16):
        first, second = y[s].astype(F32), y[16 + s].astype(F32)
        squares = squares + live[s] * (first * first + second * second)
    squares = squares * w_column

    copies[8].wait_recv()
    here, there = pl.ds(pl.multiple_of(h * half, 8), half), pl.ds(pl.multiple_of(other * half, 8), half)
    for n in range(3):
        full[n, here, :] = misc[n]
        full[n, there, :] = misc_in[n]
    mixing = full[0][:, 0:full_levels].astype(BF16)
    eye80 = one_hot(iota((full_levels, full_levels), 0) == iota((full_levels, full_levels), 1))
    mixing_back = dot_nt(eye80, full[0].astype(BF16)[:, 0:full_levels]) if False else dot_tn(mixing, eye80)
    mixing_back = mixing_back.astype(BF16)
    jac_t = full[1].astype(BF16)
    weighted = (full[1] * w_row).astype(BF16)
    gram = dot_nt(weighted, jac_t).astype(BF16)

    for s in range(16):
        span = slice(LANES * s, LANES * (s + 1))
        first = dot(weighted, y[s]) * live[s]
        second = dot(weighted, y[16 + s]) * live[s]
        slots[:, span] = jnp.concatenate(
            [first, second, jnp.broadcast_to(live[s], (16, LANES))], axis=0
        ).astype(BF16)
    for q in range(rows // 2):
        masked = jnp.concatenate(
            [
                slots[:, LANES * s : LANES * (s + 1)]
                * jnp.broadcast_to(jnp.where(pair_of[s : s + 1, :] == q, 1.0, 0.0), (slots.shape[0], LANES)).astype(BF16)
                for s in range(16)
            ],
            axis=1,
        )
        grid[:, 2 * LANES * q : 2 * LANES * (q + 1)] = dot(masked, pick[...]).astype(BF16)

    def edge_selector(core):
        number, lane = iota((16, 4 * LANES), 0), iota((16, 4 * LANES), 1)
        return one_hot((number >> 2) * LANES + (number & 3) + core * (LANES - HALO) == lane)

    outgoing, incoming = edge_selector(h), edge_selector(other)
    depth = slots.shape[0]
    for q in range(4):
        block = jnp.concatenate([grid[:, at_row(4 * g + q)] for g in range(4)], axis=1)
        edge[:, 256 * q : 256 * q + depth] = dot_nt(outgoing, block).astype(BF16)
        edge[:, 256 * q + depth : 256 * (q + 1)] = jnp.zeros((16, 256 - depth), BF16)
    late = [
        remote(12, grid.at[:, 14 * LANES : 16 * LANES], grid_s, (up, j, h)),
        remote(13, grid.at[:, 0 : 2 * LANES], grid_n, (down, j, h)),
        remote(14, edge, edge_in, (i, side, other)),
        remote(15, edge.at[:, 768:1024], edge_s, (up, side, other)),
        remote(16, edge.at[:, 0:256], edge_n, (down, side, other)),
    ]
    for copy in late:
        copy.start()

    copies[0].wait_recv()
    relay_s = remote(4, south, south_in, (i, j, other))
    relay_s.start()
    copies[1].wait_recv()
    relay_n = remote(5, north, north_in, (i, j, other))
    relay_n.start()

    lane_row = iota((1, LANES), 1)
    patched = jnp.where(h == 0, lane_row - (LANES - HALO), HALO - 1 - lane_row) >= 0
    own_lanes = jnp.where(h == 0, LANES // 2 - 1 - lane_row, lane_row - LANES // 2) >= 0
    number, lane = iota((16, 3 * LANES), 0), iota((16, 3 * LANES), 1)
    place = one_hot(((number >> 2) * LANES + (number & 3) + other * (LANES - HALO) == lane) & (number < 12))
    mask_s = jnp.where(i > 0, 1.0, 0.0).astype(F32)
    mask_n = jnp.where(i < nlat - 1, 1.0, 0.0).astype(F32)

    def row_mask(e):
        return mask_s if e < HALO else mask_n if e >= HALO + rows else None

    def keep(e, value):
        mask = row_mask(e)
        return value if mask is None else value * mask

    targets = (x0, hu, hv)

    def assemble(e, sources, patches):
        for f in range(3):
            for span, source, patch in zip((here, there), sources, patches):
                value = source[f]
                if patch is not None:
                    value = jnp.where(patched, patch[:, at_row(f)], value)
                targets[f][span, at_row(e)] = keep(e, value)

    def rows_of(ref, q):
        blocks = [ref[f, q].astype(F32) for f in range(3)]
        return [[block[half * t : half * (t + 1)] for block in blocks] for t in (0, 1)]

    def patch_of(ref):
        return dot_tn(ref[:, 0 : 3 * half], place)

    copies[9].wait_recv()
    for k in (0, 1):
        remote(6, strip_e, strip_in.at[k], (i, east, 0), 6 + k).wait_recv()
    group_of = {}
    for r in range(rows):
        g = max(n for n, start in enumerate(GROUPS) if start <= r and r < start + 3)
        if r in (6, 7, 8):
            g = 2
        if r in (9, 10):
            g = 3
        group_of[r] = (g, r - GROUPS[g])
    found = {}

    def patches_for(r):
        g, t = group_of[r]
        if g not in found:
            found.clear()
            found[g] = (patch_of(strip_in.at[h, g]), patch_of(strip_in.at[other, g]))
        return [value[half * t : half * (t + 1)] for value in found[g]]

    for q in range(rows // 2):
        mine, theirs = rows_of(own, q), rows_of(partner, q)
        for t in (0, 1):
            r = 2 * q + t
            assemble(HALO + r, (mine[t], theirs[t]), patches_for(r))
    relay_s.wait_recv()
    relay_n.wait_recv()
    for k in (0, 1):
        remote(8, strip_e.at[5], strip_s.at[k], (i, east, 0), 8 + k).wait_recv()
        remote(9, strip_e.at[0], strip_n.at[k], (i, east, 0), 10 + k).wait_recv()
    patch = (patch_of(strip_s.at[h]), patch_of(strip_s.at[other]))
    for q in (0, 1):
        mine, theirs = rows_of(south, q), rows_of(south_in, q)
        for t in (0, 1):
            e = 2 * q + t
            fit = [None if e == 0 else value[half * (e - 1) : half * e] for value in patch]
            assemble(e, (mine[t], theirs[t]), fit)
    patch = (patch_of(strip_n.at[h]), patch_of(strip_n.at[other]))
    for q in (0, 1):
        mine, theirs = rows_of(north, q), rows_of(north_in, q)
        for t in (0, 1):
            e = 2 * q + t
            fit = [None if e == 3 else value[half * e : half * (e + 1)] for value in patch]
            assemble(HALO + rows + e, (mine[t], theirs[t]), fit)

    diffusion = full[2]
    centre = 1.0 - 4.0 * diffusion

    def step_row(x, e):
        value, above, below = x[:, at_row(e)], x[:, at_row(e + 1)], x[:, at_row(e - 1)]
        eastern = pltpu.roll(value, LANES - 1, 1)
        western = pltpu.roll(value, 1, 1)
        return (
            centre * value
            + diffusion * ((above + below) + (eastern + western))
            + hu[:, at_row(e)] * (western - eastern)
            + hv[:, at_row(e)] * (below - above)
        )

    def back_row(x, e):
        value, above, below = x[:, at_row(e)], x[:, at_row(e + 1)], x[:, at_row(e - 1)]
        spread, drift = diffusion * value, hu[:, at_row(e)] * value
        eastern = pltpu.roll(spread + drift, LANES - 1, 1)
        western = pltpu.roll(spread - drift, 1, 1)
        return (
            centre * value
            + (eastern + western)
            + (diffusion + hv[:, at_row(e + 1)]) * above
            + (diffusion - hv[:, at_row(e - 1)]) * below
        )

    def coupled(matrix, values):
        joined = jnp.concatenate(values, axis=1).astype(BF16)
        mixed = dot(matrix, joined)
        return [value + mixed[:, at_row(n)] for n, value in enumerate(values)]

    def pairwise(first, last):
        return [tuple(range(e, min(e + 2, last + 1))) for e in range(first, last + 1, 2)]

    for copy in late:
        copy.wait_recv()
    for q in range(4):
        value = dot_tn(edge_in[:, 256 * q : 256 * q + depth], incoming)
        for g in range(4):
            r = 4 * g + q
            f1[:, at_row(r + 2)] = jnp.where(patched, value[:, at_row(g)], grid[:, at_row(r)].astype(F32))
    f1[:, at_row(0)] = grid_s[:, at_row(0)].astype(F32)
    value = dot_tn(edge_s[:, 0:depth], incoming)
    f1[:, at_row(1)] = jnp.where(patched, value[:, at_row(3)], grid_s[:, at_row(1)].astype(F32))
    value = dot_tn(edge_n[:, 0:depth], incoming)
    f1[:, at_row(18)] = jnp.where(patched, value[:, at_row(0)], grid_n[:, at_row(0)].astype(F32))
    f1[:, at_row(19)] = grid_n[:, at_row(1)].astype(F32)

    for pair in pairwise(1, 22):
        values = coupled(mixing, [step_row(x0, e) for e in pair])
        for e, value in zip(pair, values):
            x1[:, at_row(e)] = keep(e, value)

    total = jnp.zeros((full_levels, LANES), F32)

    def forced(states, pair, step, total):
        halves = [state.astype(BF16) for state in states]
        image = dot(gram, jnp.concatenate(halves, axis=1))
        result = []
        for n, e in enumerate(pair):
            moved = f1[full_levels * step : full_levels * (step + 1), at_row(e - 2)]
            alive = f1[2 * full_levels : 2 * full_levels + 1, at_row(e - 2)]
            force = alive * image[:, at_row(n)] - moved
            if HALO <= e < HALO + rows:
                total = total + halves[n].astype(F32) * (force - moved)
            result.append(force)
        return result, total

    for pair in pairwise(2, 21):
        states = coupled(mixing, [step_row(x1, e) for e in pair])
        forces, total = forced(states, pair, 1, total)
        for e, value in zip(pair, coupled(mixing_back, forces)):
            x0[:, at_row(e)] = keep(e, value)

    for pair in pairwise(3, 20):
        forces, total = forced([x1[:, at_row(e)] for e in pair], pair, 0, total)
        values = [back_row(x0, e) + force for e, force in zip(pair, forces)]
        for e, value in zip(pair, coupled(mixing_back, values)):
            sm[:, at_row(e)] = keep(e, value)

    for r in range(rows):
        x1[:, at_row(r)] = back_row(sm, r + HALO)
    for q in range(rows // 2):
        back[q] = jnp.concatenate([x1[there, at_row(2 * q)], x1[there, at_row(2 * q + 1)]], axis=0).astype(BF16)
    final = remote(17, back, back_in, (i, j, other))
    final.start()

    increment = inc[...]
    part = 0.5 * jnp.sum(increment * increment, axis=0, keepdims=True)
    part = part + 0.25 * jnp.sum(squares, axis=0, keepdims=True)
    part = part + 0.5 * jnp.sum(jnp.where(own_lanes, total, 0.0), axis=0, keepdims=True)
    cost_ref[...] = part

    final.wait_recv()
    for q in range(rows // 2):
        received = back_in[q].astype(F32)
        for t in (0, 1):
            r = 2 * q + t
            adjoint = jnp.where(own_lanes, x1[here, at_row(r)], received[half * t : half * (t + 1)])
            out_ref[pl.ds(r, half, stride=rows), :] = inc[pl.ds(r, half, stride=rows), :] + adjoint
    for copy in copies + late + [relay_s, relay_n, final]:
        copy.wait_send()


def body(nlat, nlon, increment, wind_u, wind_v, diffusion, mixing, jacobian, obs_weight, innovation, counts, column_lookup):
    half, rows, width = increment.shape
    channels = jacobian.shape[0]
    wide = (HALO * 2 + rows) * width
    levels = 2 * half
    depth = 2 * levels + 16
    anywhere = pl.BlockSpec(memory_space=pl.ANY)
    vmem = pl.BlockSpec(memory_space=pltpu.VMEM)
    smem = pl.BlockSpec(memory_space=pltpu.SMEM)
    grid_size = rows * width
    strip = (16, width)
    scratch = [
        ((half * rows, width), F32), ((half * rows, width), F32), ((half * rows, width), F32),
        ((1, half), F32), ((half, levels), F32), ((channels, half), BF16), ((1, channels), F32),
        ((32, channels, width), BF16), ((16, width), jnp.int32),
        ((3, 8, levels, width), BF16), ((3, 8, levels, width), BF16),
        ((3, half, width), F32), ((3, half, width), F32), ((3, levels, width), F32),
        ((3, 2, levels, width), BF16), ((3, 2, levels, width), BF16),
        ((3, 2, levels, width), BF16), ((3, 2, levels, width), BF16),
        ((6, *strip), BF16), ((6, *strip), BF16), ((2, 6, *strip), BF16), ((2, *strip), BF16), ((2, *strip), BF16),
        ((depth, grid_size), BF16), ((grid_size, 2 * width), BF16), ((depth, grid_size), BF16),
        ((depth, 2 * width), BF16), ((depth, 2 * width), BF16),
        ((16, 1024), BF16), ((16, 1024), BF16), ((16, 256), BF16), ((16, 256), BF16),
        ((levels, wide), F32), ((levels, wide), F32), ((levels, wide), F32), ((levels, wide), F32), ((levels, wide), F32),
        ((depth, 20 * width), F32),
        ((8, levels, width), BF16), ((8, levels, width), BF16),
    ]
    gradient, part = pl.pallas_call(
        functools.partial(kernel, (nlat, nlon, half, rows)),
        out_shape=(
            jax.ShapeDtypeStruct((half * rows, width), F32),
            jax.ShapeDtypeStruct((1, width), F32),
        ),
        in_specs=[anywhere] * 8 + [smem, anywhere],
        out_specs=(vmem, vmem),
        scratch_shapes=[pltpu.VMEM(shape, dtype) for shape, dtype in scratch]
        + [
            pltpu.SemaphoreType.DMA((9,)),
            pltpu.SemaphoreType.DMA((18,)),
            pltpu.SemaphoreType.DMA((18,)),
        ],
        compiler_params=pltpu.CompilerParams(
            collective_id=0, has_side_effects=True, vmem_limit_bytes=60 * 1024 * 1024
        ),
    )(
        increment.reshape(half * rows, width),
        wind_u.reshape(half * rows, width),
        wind_v.reshape(half * rows, width),
        diffusion.reshape(1, half),
        mixing,
        jacobian,
        obs_weight.reshape(1, channels),
        innovation.reshape(32, channels, width),
        counts,
        column_lookup.reshape(16, width),
    )
    total_cells = increment.size * nlat * nlon * 2
    cost = lax.psum(jnp.sum(part), ("lat", "lon", "lev")) / total_cells
    return gradient.reshape(increment.shape), cost


def solution(mesh):
    field = P("lev", "lat", "lon")
    in_specs = (
        field,
        field,
        field,
        P("lev"),
        P("lev", None),
        P(None, "lev"),
        P(),
        P(None, "lat", "lon", None, None, None),
        P("lat", "lon"),
        P("lat", "lon", None),
    )
    return jax.shard_map(
        functools.partial(body, mesh.shape["lat"], mesh.shape["lon"]),
        mesh=mesh,
        in_specs=in_specs,
        out_specs=(field, P()),
        check_vma=False,
    )
```

```python
import functools

import jax
import jax.numpy as jnp
from jax import lax
from jax.experimental import pallas as pl
from jax.experimental.pallas import tpu as pltpu
from jax.sharding import PartitionSpec as P

F32 = jnp.float32
BF16 = jnp.bfloat16
MESH = pl.DeviceIdType.MESH
HALO = 4
GROUPS = (0, 3, 6, 8, 10, 13)
LANES = 128


def dot(a, b):
    return lax.dot_general(a, b, (((1,), (0,)), ((), ())), preferred_element_type=F32)


def dot_nt(a, b):
    return lax.dot_general(a, b, (((1,), (1,)), ((), ())), preferred_element_type=F32)


def dot_tn(a, b):
    return lax.dot_general(a, b, (((0,), (0,)), ((), ())), preferred_element_type=F32)


def iota(shape, dim):
    return lax.broadcasted_iota(jnp.int32, shape, dim)


def one_hot(condition):
    return jnp.where(condition, 1.0, 0.0).astype(BF16)


def at_row(e):
    return slice(LANES * e, LANES * (e + 1))


def kernel(
    sizes,
    inc_h, u_h, v_h, dif_h, mix_h, jac_h, w_h, y_h, cnt_s, lut_h,
    out_ref, cost_ref,
    inc, u, v, dif, mix, jac, w, y, lut,
    own, partner, misc, misc_in, full,
    south, north, south_in, north_in,
    strip_e, strip_w, strip_in, strip_s, strip_n,
    slots, pick, grid, grid_s, grid_n, edge, edge_in, edge_s, edge_n,
    x0, x1, hu, hv, sm, f1, hold, back, back_in, near, far,
    load_sem, send_sem, recv_sem,
):
    nlat, nlon, half, rows = sizes
    full_levels = 2 * half
    i, j, h = lax.axis_index("lat"), lax.axis_index("lon"), lax.axis_index("lev")
    other = 1 - h
    up, down = lax.rem(i + 1, nlat), lax.rem(i + nlat - 1, nlat)
    east, west = lax.rem(j + 1, nlon), lax.rem(j + nlon - 1, nlon)
    side = lax.rem(j + nlon - 1 + 2 * h, nlon)

    barrier = pltpu.get_barrier_semaphore()
    senders = [(up, j, h), (down, j, h), (i, j, other)]
    senders += [(a, side, k) for a in (i, up, down) for k in (0, 1)]
    ring = nlon // 2 if nlon % 2 == 0 else nlon
    laps = nlon // ring
    crowd = nlat * laps * 2
    lap, place_in_ring = lax.div(j, ring), lax.rem(j, ring)
    me = (i * laps + lap) * 2 + h

    def companion(t):
        index = lax.rem(me + t, crowd)
        return (
            lax.div(index, 2 * laps),
            lax.rem(lax.div(index, 2), laps) * ring + place_in_ring,
            lax.rem(index, 2),
        )

    def follower(t):
        return (i, lap * ring + lax.rem(place_in_ring + t, ring), h)

    senders += [companion(t) for t in range(1, crowd)] + [follower(t) for t in range(1, ring)]
    for device in senders:
        pl.semaphore_signal(barrier, inc=1, device_id=device, device_id_type=MESH)

    loads = {}
    pairs = ((inc_h, inc), (u_h, u), (v_h, v), (dif_h, dif), (mix_h, mix), (jac_h, jac), (w_h, w), (lut_h, lut), (y_h, y))
    for n, (source, target) in enumerate(pairs):
        loads[n] = pltpu.make_async_copy(source, target, load_sem.at[n])
        loads[n].start()

    def remote(n, source, target, device, arrival=None):
        return pltpu.make_async_remote_copy(
            src_ref=source,
            dst_ref=target,
            send_sem=send_sem.at[n],
            recv_sem=recv_sem.at[n if arrival is None else arrival],
            device_id=device,
            device_id_type=MESH,
        )

    for n in range(3):
        loads[n].wait()
    fields = (inc, u, v)

    def own_row(f, r):
        value = fields[f][pl.ds(r, half, stride=rows), :]
        return value if f == 0 else 0.5 * value

    for q in range(rows // 2):
        for f in range(3):
            own[f, q] = jnp.concatenate([own_row(f, 2 * q), own_row(f, 2 * q + 1)], axis=0).astype(BF16)

    wide = (32, 3 * LANES)
    number, lane = iota(wide, 0), iota(wide, 1)
    inner = number & 15
    west_edge = number >> 4
    spot = (inner >> 2) * LANES + (inner & 3) + (1 - west_edge) * (LANES - HALO)
    selector = one_hot((spot == lane) & (inner < 12))
    for g, start in enumerate(GROUPS):
        block = jnp.concatenate(
            [
                jnp.concatenate([own_row(f, start + t) for t in range(3)], axis=0).astype(BF16)
                for f in range(3)
            ],
            axis=1,
        )
        strip = dot_nt(selector, block).astype(BF16)
        strip_e[g, :, 0 : 3 * half] = strip[0:16]
        strip_w[g, :, 0 : 3 * half] = strip[16:32]
        strip_e[g, :, 3 * half : LANES] = jnp.zeros((16, LANES - 3 * half), BF16)
        strip_w[g, :, 3 * half : LANES] = jnp.zeros((16, LANES - 3 * half), BF16)

    for n in range(3, 8):
        loads[n].wait()
    misc[0] = jnp.zeros((half, LANES), F32)
    misc[0, :, 0:full_levels] = mix[...]
    eye = iota((half, half), 0) == iota((half, half), 1)
    misc[1] = jac[...].astype(F32)
    column = jnp.sum(jnp.where(eye, dif[...], 0.0), axis=1, keepdims=True)
    misc[2] = jnp.broadcast_to(column, (half, LANES))

    pl.semaphore_wait(barrier, len(senders))

    copies = [
        remote(2, own.at[:, 6:8], south, (up, j, h)),
        remote(3, own.at[:, 0:2], north, (down, j, h)),
        remote(6, strip_e, strip_in.at[h], (i, east, 0), 6 + h),
        remote(7, strip_w, strip_in.at[h], (i, west, 1), 6 + h),
        remote(8, strip_e.at[5], strip_s.at[h], (up, east, 0), 8 + h),
        remote(9, strip_e.at[0], strip_n.at[h], (down, east, 0), 10 + h),
        remote(10, strip_w.at[5], strip_s.at[h], (up, west, 1), 8 + h),
        remote(11, strip_w.at[0], strip_n.at[h], (down, west, 1), 10 + h),
        remote(1, misc, misc_in, (i, j, other)),
        remote(0, own, partner, (i, j, other)),
    ]
    for copy in copies:
        copy.start()

    table = lut[...]
    low = dot_nt(one_hot(iota((LANES, LANES), 0) == iota((LANES, LANES), 1)), (table & 255).astype(F32).astype(BF16))
    pair_lane = iota((LANES, 2 * LANES), 1).astype(F32)
    for s in range(16):
        pick[LANES * s : LANES * (s + 1)] = one_hot(jnp.broadcast_to(low[:, s : s + 1], (LANES, 2 * LANES)) == pair_lane)
    pair_of = (table >> 8).astype(F32)

    count = cnt_s[0, 0]
    live = [jnp.where(count > s, 1.0, 0.0).astype(F32) for s in range(16)]
    loads[8].wait()
    w_row = w[...]
    w_column = jnp.sum(
        jnp.where(iota((LANES, LANES), 0) == iota((LANES, LANES), 1), w_row, 0.0), axis=1, keepdims=True
    )
    squares = jnp.zeros((LANES, LANES), F32)
    for s in range(16):
        first, second = y[s].astype(F32), y[16 + s].astype(F32)
        squares = squares + live[s] * (first * first + second * second)
    squares = squares * w_column

    copies[8].wait_recv()
    here, there = pl.ds(pl.multiple_of(h * half, 8), half), pl.ds(pl.multiple_of(other * half, 8), half)
    for n in range(3):
        full[n, here, :] = misc[n]
        full[n, there, :] = misc_in[n]
    mixing = full[0][:, 0:full_levels].astype(BF16)
    eye80 = one_hot(iota((full_levels, full_levels), 0) == iota((full_levels, full_levels), 1))
    mixing_back = dot_tn(mixing, eye80).astype(BF16)
    jac_t = full[1].astype(BF16)
    weighted = (full[1] * w_row).astype(BF16)
    gram_full = dot_nt(weighted, jac_t)
    gram = gram_full.astype(BF16)
    gram = jnp.concatenate([gram, (gram_full - gram.astype(F32)).astype(BF16)], axis=1)

    for s in range(16):
        span = slice(LANES * s, LANES * (s + 1))
        first = dot(weighted, y[s]) * live[s]
        second = dot(weighted, y[16 + s]) * live[s]
        slots[:, span] = jnp.concatenate(
            [first, second, jnp.broadcast_to(live[s], (16, LANES))], axis=0
        ).astype(BF16)
    for q in range(rows // 2):
        masked = jnp.concatenate(
            [
                slots[:, LANES * s : LANES * (s + 1)]
                * jnp.broadcast_to(jnp.where(pair_of[s : s + 1, :] == q, 1.0, 0.0), (slots.shape[0], LANES)).astype(BF16)
                for s in range(16)
            ],
            axis=1,
        )
        grid[:, 2 * LANES * q : 2 * LANES * (q + 1)] = dot(masked, pick[...]).astype(BF16)

    def edge_selector(core):
        number, lane = iota((16, 4 * LANES), 0), iota((16, 4 * LANES), 1)
        return one_hot((number >> 2) * LANES + (number & 3) + core * (LANES - HALO) == lane)

    outgoing, incoming = edge_selector(h), edge_selector(other)
    depth = slots.shape[0]
    for q in range(4):
        block = jnp.concatenate([grid[:, at_row(4 * g + q)] for g in range(4)], axis=1)
        edge[:, 256 * q : 256 * q + depth] = dot_nt(outgoing, block).astype(BF16)
        edge[:, 256 * q + depth : 256 * (q + 1)] = jnp.zeros((16, 256 - depth), BF16)
    late = [
        remote(12, grid.at[:, 14 * LANES : 16 * LANES], grid_s, (up, j, h)),
        remote(13, grid.at[:, 0 : 2 * LANES], grid_n, (down, j, h)),
        remote(14, edge, edge_in, (i, side, other)),
        remote(15, edge.at[:, 768:1024], edge_s, (up, side, other)),
        remote(16, edge.at[:, 0:256], edge_n, (down, side, other)),
    ]
    for copy in late:
        copy.start()

    copies[0].wait_recv()
    relay_s = remote(4, south, south_in, (i, j, other))
    relay_s.start()
    copies[1].wait_recv()
    relay_n = remote(5, north, north_in, (i, j, other))
    relay_n.start()

    lane_row = iota((1, LANES), 1)
    patched = jnp.where(h == 0, lane_row - (LANES - HALO), HALO - 1 - lane_row) >= 0
    own_lanes = jnp.where(h == 0, LANES // 2 - 1 - lane_row, lane_row - LANES // 2) >= 0
    number, lane = iota((16, 3 * LANES), 0), iota((16, 3 * LANES), 1)
    place = one_hot(((number >> 2) * LANES + (number & 3) + other * (LANES - HALO) == lane) & (number < 12))
    mask_s = jnp.where(i > 0, 1.0, 0.0).astype(F32)
    mask_n = jnp.where(i < nlat - 1, 1.0, 0.0).astype(F32)

    def row_mask(e):
        return mask_s if e < HALO else mask_n if e >= HALO + rows else None

    def keep(e, value):
        mask = row_mask(e)
        return value if mask is None else value * mask

    targets = (x0, hu, hv)

    def assemble(e, sources, patches):
        for f in range(3):
            for span, source, patch in zip((here, there), sources, patches):
                value = source[f]
                if patch is not None:
                    value = jnp.where(patched, patch[:, at_row(f)], value)
                targets[f][span, at_row(e)] = keep(e, value)

    def rows_of(ref, q):
        blocks = [ref[f, q].astype(F32) for f in range(3)]
        return [[block[half * t : half * (t + 1)] for block in blocks] for t in (0, 1)]

    def patch_of(ref):
        return dot_tn(ref[:, 0 : 3 * half], place)

    copies[9].wait_recv()
    for k in (0, 1):
        remote(6, strip_e, strip_in.at[k], (i, east, 0), 6 + k).wait_recv()
    group_of = {}
    for r in range(rows):
        g = max(n for n, start in enumerate(GROUPS) if start <= r and r < start + 3)
        if r in (6, 7, 8):
            g = 2
        if r in (9, 10):
            g = 3
        group_of[r] = (g, r - GROUPS[g])
    found = {}

    def patches_for(r):
        g, t = group_of[r]
        if g not in found:
            found.clear()
            found[g] = (patch_of(strip_in.at[h, g]), patch_of(strip_in.at[other, g]))
        return [value[half * t : half * (t + 1)] for value in found[g]]

    for q in range(rows // 2):
        mine, theirs = rows_of(own, q), rows_of(partner, q)
        for t in (0, 1):
            r = 2 * q + t
            assemble(HALO + r, (mine[t], theirs[t]), patches_for(r))
    relay_s.wait_recv()
    relay_n.wait_recv()
    for k in (0, 1):
        remote(8, strip_e.at[5], strip_s.at[k], (i, east, 0), 8 + k).wait_recv()
        remote(9, strip_e.at[0], strip_n.at[k], (i, east, 0), 10 + k).wait_recv()
    patch = (patch_of(strip_s.at[h]), patch_of(strip_s.at[other]))
    for q in (0, 1):
        mine, theirs = rows_of(south, q), rows_of(south_in, q)
        for t in (0, 1):
            e = 2 * q + t
            fit = [None if e == 0 else value[half * (e - 1) : half * e] for value in patch]
            assemble(e, (mine[t], theirs[t]), fit)
    patch = (patch_of(strip_n.at[h]), patch_of(strip_n.at[other]))
    for q in (0, 1):
        mine, theirs = rows_of(north, q), rows_of(north_in, q)
        for t in (0, 1):
            e = 2 * q + t
            fit = [None if e == 3 else value[half * e : half * (e + 1)] for value in patch]
            assemble(HALO + rows + e, (mine[t], theirs[t]), fit)

    diffusion = full[2]
    centre = 1.0 - 4.0 * diffusion

    def step_row(x, e):
        value, above, below = x[:, at_row(e)], x[:, at_row(e + 1)], x[:, at_row(e - 1)]
        eastern = pltpu.roll(value, LANES - 1, 1)
        western = pltpu.roll(value, 1, 1)
        return (
            centre * value
            + diffusion * ((above + below) + (eastern + western))
            + hu[:, at_row(e)] * (western - eastern)
            + hv[:, at_row(e)] * (below - above)
        )

    def back_row(x, e):
        value, above, below = x[:, at_row(e)], x[:, at_row(e + 1)], x[:, at_row(e - 1)]
        spread, drift = diffusion * value, hu[:, at_row(e)] * value
        eastern = pltpu.roll(spread + drift, LANES - 1, 1)
        western = pltpu.roll(spread - drift, 1, 1)
        return (
            centre * value
            + (eastern + western)
            + (diffusion + hv[:, at_row(e + 1)]) * above
            + (diffusion - hv[:, at_row(e - 1)]) * below
        )

    def coupled(matrix, values):
        joined = jnp.concatenate(values, axis=1).astype(BF16)
        mixed = dot(matrix, joined)
        return [value + mixed[:, at_row(n)] for n, value in enumerate(values)]

    def pairwise(first, last):
        return [tuple(range(e, min(e + 2, last + 1))) for e in range(first, last + 1, 2)]

    for copy in late:
        copy.wait_recv()
    for q in range(4):
        value = dot_tn(edge_in[:, 256 * q : 256 * q + depth], incoming)
        for g in range(4):
            r = 4 * g + q
            f1[:, at_row(r + 2)] = jnp.where(patched, value[:, at_row(g)], grid[:, at_row(r)].astype(F32))
    f1[:, at_row(0)] = grid_s[:, at_row(0)].astype(F32)
    value = dot_tn(edge_s[:, 0:depth], incoming)
    f1[:, at_row(1)] = jnp.where(patched, value[:, at_row(3)], grid_s[:, at_row(1)].astype(F32))
    value = dot_tn(edge_n[:, 0:depth], incoming)
    f1[:, at_row(18)] = jnp.where(patched, value[:, at_row(0)], grid_n[:, at_row(0)].astype(F32))
    f1[:, at_row(19)] = grid_n[:, at_row(1)].astype(F32)

    def advance(pair):
        values = coupled(mixing, [step_row(x0, e) for e in pair])
        for e, value in zip(pair, values):
            x1[:, at_row(e)] = keep(e, value)

    def forced(states, pair, step):
        halves = [state.astype(BF16) for state in states]
        joined = jnp.concatenate(halves, axis=1)
        image = dot(gram, jnp.concatenate([joined, joined], axis=0))
        result, parts = [], []
        for n, e in enumerate(pair):
            moved = f1[full_levels * step : full_levels * (step + 1), at_row(e - 2)]
            alive = f1[2 * full_levels : 2 * full_levels + 1, at_row(e - 2)]
            force = alive * image[:, at_row(n)] - moved
            parts.append(halves[n].astype(F32) * (force - moved))
            result.append(force)
        return result, sum(parts)

    def force_first(pair):
        forces, part = forced([x1[:, at_row(e)] for e in pair], pair, 0)
        for e, force in zip(pair, forces):
            hold[:, at_row(e)] = force
        return part

    def force_second(pair):
        states = coupled(mixing, [step_row(x1, e) for e in pair])
        forces, part = forced(states, pair, 1)
        for e, force in zip(pair, forces):
            sm[:, at_row(e)] = force
        return part

    inside = pairwise(HALO, HALO + rows - 1)
    for pair in pairwise(3, 20):
        advance(pair)
    total = jnp.zeros((full_levels, LANES), F32)
    for pair in inside:
        total = total + force_first(pair)
        total = total + force_second(pair)

    increment = inc[...]
    part = 0.5 * jnp.sum(increment * increment, axis=0, keepdims=True)
    part = part + 0.25 * jnp.sum(squares, axis=0, keepdims=True)
    part = part + 0.5 * jnp.sum(jnp.where(own_lanes, total, 0.0), axis=0, keepdims=True)
    near[0] = part
    first_round = [remote(18 + t, near.at[0], near.at[t], companion(t)) for t in range(1, crowd)]
    for copy in first_round:
        copy.start()

    for pair in ((1, 2), (21, 22)):
        advance(pair)
    for pair in ((3,), (20,)):
        force_first(pair)
    for pair in ((2, 3), (20, 21)):
        force_second(pair)
    for pair in pairwise(2, 21):
        values = coupled(mixing_back, [sm[:, at_row(e)] for e in pair])
        for e, value in zip(pair, values):
            x0[:, at_row(e)] = keep(e, value)

    for pair in pairwise(3, 20):
        values = [back_row(x0, e) + hold[:, at_row(e)] for e in pair]
        for e, value in zip(pair, coupled(mixing_back, values)):
            sm[:, at_row(e)] = keep(e, value)

    for r in range(rows):
        x1[:, at_row(r)] = back_row(sm, r + HALO)
    for q in range(rows // 2):
        back[q] = jnp.concatenate([x1[there, at_row(2 * q)], x1[there, at_row(2 * q + 1)]], axis=0).astype(BF16)
    final = remote(17, back, back_in, (i, j, other))
    final.start()

    for copy in first_round:
        copy.wait_recv()
    part = near[0]
    for t in range(1, crowd):
        part = part + near[t]
    far[0] = part
    second_round = [remote(18 + crowd + t, far.at[0], far.at[t], follower(t)) for t in range(1, ring)]
    for copy in second_round:
        copy.start()

    final.wait_recv()
    for q in range(rows // 2):
        received = back_in[q].astype(F32)
        for t in (0, 1):
            r = 2 * q + t
            adjoint = jnp.where(own_lanes, x1[here, at_row(r)], received[half * t : half * (t + 1)])
            out_ref[pl.ds(r, half, stride=rows), :] = inc[pl.ds(r, half, stride=rows), :] + adjoint
    for copy in second_round:
        copy.wait_recv()
    part = far[0]
    for t in range(1, ring):
        part = part + far[t]
    cells = full_levels * rows * LANES * nlat * nlon
    cost_ref[0, 0] = jnp.sum(part) / cells
    for copy in copies + late + [relay_s, relay_n, final] + first_round + second_round:
        copy.wait_send()


def body(nlat, nlon, increment, wind_u, wind_v, diffusion, mixing, jacobian, obs_weight, innovation, counts, column_lookup):
    half, rows, width = increment.shape
    channels = jacobian.shape[0]
    wide = (HALO * 2 + rows) * width
    levels = 2 * half
    depth = 2 * levels + 16
    anywhere = pl.BlockSpec(memory_space=pl.ANY)
    vmem = pl.BlockSpec(memory_space=pltpu.VMEM)
    smem = pl.BlockSpec(memory_space=pltpu.SMEM)
    grid_size = rows * width
    far = nlon // 2 if nlon % 2 == 0 else nlon
    near = nlat * (nlon // far) * 2
    copies = 18 + near + far
    strip = (16, width)
    scratch = [
        ((half * rows, width), F32), ((half * rows, width), F32), ((half * rows, width), F32),
        ((1, half), F32), ((half, levels), F32), ((half, channels), BF16), ((1, channels), F32),
        ((32, channels, width), BF16), ((16, width), jnp.int32),
        ((3, 8, levels, width), BF16), ((3, 8, levels, width), BF16),
        ((3, half, width), F32), ((3, half, width), F32), ((3, levels, width), F32),
        ((3, 2, levels, width), BF16), ((3, 2, levels, width), BF16),
        ((3, 2, levels, width), BF16), ((3, 2, levels, width), BF16),
        ((6, *strip), BF16), ((6, *strip), BF16), ((2, 6, *strip), BF16), ((2, *strip), BF16), ((2, *strip), BF16),
        ((depth, grid_size), BF16), ((grid_size, 2 * width), BF16), ((depth, grid_size), BF16),
        ((depth, 2 * width), BF16), ((depth, 2 * width), BF16),
        ((16, 1024), BF16), ((16, 1024), BF16), ((16, 256), BF16), ((16, 256), BF16),
        ((levels, wide), F32), ((levels, wide), F32), ((levels, wide), F32), ((levels, wide), F32), ((levels, wide), F32),
        ((depth, 20 * width), F32),
        ((levels, wide), F32), ((8, levels, width), BF16), ((8, levels, width), BF16),
        ((near, 1, width), F32), ((far, 1, width), F32),
    ]
    gradient, cost = pl.pallas_call(
        functools.partial(kernel, (nlat, nlon, half, rows)),
        out_shape=(
            jax.ShapeDtypeStruct((half * rows, width), F32),
            jax.ShapeDtypeStruct((1, 1), F32),
        ),
        in_specs=[anywhere] * 8 + [smem, anywhere],
        out_specs=(vmem, smem),
        scratch_shapes=[pltpu.VMEM(shape, dtype) for shape, dtype in scratch]
        + [
            pltpu.SemaphoreType.DMA((9,)),
            pltpu.SemaphoreType.DMA((copies,)),
            pltpu.SemaphoreType.DMA((copies,)),
        ],
        compiler_params=pltpu.CompilerParams(
            collective_id=0, has_side_effects=True, vmem_limit_bytes=60 * 1024 * 1024
        ),
    )(
        increment.reshape(half * rows, width),
        wind_u.reshape(half * rows, width),
        wind_v.reshape(half * rows, width),
        diffusion.reshape(1, half),
        mixing,
        jacobian.T,
        obs_weight.reshape(1, channels),
        innovation.reshape(32, channels, width),
        counts,
        column_lookup.reshape(16, width),
    )
    return gradient.reshape(increment.shape), cost.reshape(())


def solution(mesh):
    field = P("lev", "lat", "lon")
    in_specs = (
        field,
        field,
        field,
        P("lev"),
        P("lev", None),
        P(None, "lev"),
        P(),
        P(None, "lat", "lon", None, None, None),
        P("lat", "lon"),
        P("lat", "lon", None),
    )
    return jax.shard_map(
        functools.partial(body, mesh.shape["lat"], mesh.shape["lon"]),
        mesh=mesh,
        in_specs=in_specs,
        out_specs=(field, P()),
        check_vma=False,
    )
```

```python
import functools

import jax
import jax.numpy as jnp
from jax import lax
from jax.experimental import pallas as pl
from jax.experimental.pallas import tpu as pltpu
from jax.sharding import PartitionSpec as P

F32 = jnp.float32
BF16 = jnp.bfloat16
MESH = pl.DeviceIdType.MESH
HALO = 4
GROUPS = (0, 3, 6, 8, 10, 13)
LANES = 128


def dot(a, b):
    return lax.dot_general(a, b, (((1,), (0,)), ((), ())), preferred_element_type=F32)


def dot_nt(a, b):
    return lax.dot_general(a, b, (((1,), (1,)), ((), ())), preferred_element_type=F32)


def dot_tn(a, b):
    return lax.dot_general(a, b, (((0,), (0,)), ((), ())), preferred_element_type=F32)


def iota(shape, dim):
    return lax.broadcasted_iota(jnp.int32, shape, dim)


def one_hot(condition):
    return jnp.where(condition, 1.0, 0.0).astype(BF16)


def at_row(e):
    return slice(LANES * e, LANES * (e + 1))


def kernel(
    sizes,
    inc_h, u_h, v_h, dif_h, mix_h, jac_h, w_h, y_h, lut_h, cnt,
    out_ref, cost_ref,
    inc, u, v, dif, mix, jac, w, y, lut,
    own, partner, misc, misc_in, full,
    south, north, south_in, north_in,
    strip_e, strip_w, strip_in, strip_s, strip_n,
    slots, pick, grid, grid_s, grid_n, edge, edge_in, edge_s, edge_n,
    x0, x1, hu, hv, sm, f1, hold, back, back_in, near, far,
    load_sem, send_sem, recv_sem,
):
    nlat, nlon, half, rows = sizes
    full_levels = 2 * half
    i, j, h = lax.axis_index("lat"), lax.axis_index("lon"), lax.axis_index("lev")
    other = 1 - h
    up, down = lax.rem(i + 1, nlat), lax.rem(i + nlat - 1, nlat)
    east, west = lax.rem(j + 1, nlon), lax.rem(j + nlon - 1, nlon)
    side = lax.rem(j + nlon - 1 + 2 * h, nlon)

    barrier = pltpu.get_barrier_semaphore()
    senders = [(up, j, h), (down, j, h), (i, j, other)]
    senders += [(a, side, k) for a in (i, up, down) for k in (0, 1)]
    ring = nlon // 2 if nlon % 2 == 0 else nlon
    laps = nlon // ring
    crowd = nlat * laps * 2
    lap, place_in_ring = lax.div(j, ring), lax.rem(j, ring)
    me = (i * laps + lap) * 2 + h

    def companion(t):
        index = lax.rem(me + t, crowd)
        return (
            lax.div(index, 2 * laps),
            lax.rem(lax.div(index, 2), laps) * ring + place_in_ring,
            lax.rem(index, 2),
        )

    def follower(t):
        return (i, lap * ring + lax.rem(place_in_ring + t, ring), h)

    senders += [companion(t) for t in range(1, crowd)] + [follower(t) for t in range(1, ring)]
    for device in senders:
        pl.semaphore_signal(barrier, inc=1, device_id=device, device_id_type=MESH)

    loads = {}
    pairs = ((inc_h, inc), (u_h, u), (v_h, v), (dif_h, dif), (mix_h, mix), (jac_h, jac), (w_h, w), (lut_h, lut), (y_h, y))
    for n, (source, target) in enumerate(pairs):
        loads[n] = pltpu.make_async_copy(source, target, load_sem.at[n])
        loads[n].start()

    def remote(n, source, target, device, arrival=None):
        return pltpu.make_async_remote_copy(
            src_ref=source,
            dst_ref=target,
            send_sem=send_sem.at[n],
            recv_sem=recv_sem.at[n if arrival is None else arrival],
            device_id=device,
            device_id_type=MESH,
        )

    for n in range(3):
        loads[n].wait()
    fields = (inc, u, v)

    def own_row(f, r):
        value = fields[f][pl.ds(r, half, stride=rows), :]
        return value if f == 0 else 0.5 * value

    for q in range(rows // 2):
        for f in range(3):
            own[q, f] = jnp.concatenate([own_row(f, 2 * q), own_row(f, 2 * q + 1)], axis=0).astype(BF16)

    wide = (32, 3 * LANES)
    number, lane = iota(wide, 0), iota(wide, 1)
    inner = number & 15
    west_edge = number >> 4
    spot = (inner >> 2) * LANES + (inner & 3) + (1 - west_edge) * (LANES - HALO)
    selector = one_hot((spot == lane) & (inner < 12))
    for g, start in enumerate(GROUPS):
        block = jnp.concatenate(
            [
                jnp.concatenate([own_row(f, start + t) for t in range(3)], axis=0).astype(BF16)
                for f in range(3)
            ],
            axis=1,
        )
        strip = dot_nt(selector, block).astype(BF16)
        strip_e[g, :, 0 : 3 * half] = strip[0:16]
        strip_w[g, :, 0 : 3 * half] = strip[16:32]
        strip_e[g, :, 3 * half : LANES] = jnp.zeros((16, LANES - 3 * half), BF16)
        strip_w[g, :, 3 * half : LANES] = jnp.zeros((16, LANES - 3 * half), BF16)

    for n in range(3, 8):
        loads[n].wait()
    misc[0] = jnp.zeros((half, LANES), F32)
    misc[0, :, 0:full_levels] = mix[...]
    eye = iota((half, half), 0) == iota((half, half), 1)
    misc[1] = jac[...].astype(F32)
    column = jnp.sum(jnp.where(eye, dif[...], 0.0), axis=1, keepdims=True)
    misc[2] = jnp.broadcast_to(column, (half, LANES))

    table = lut[...]
    low = dot_nt(one_hot(iota((LANES, LANES), 0) == iota((LANES, LANES), 1)), (table & 255).astype(F32).astype(BF16))
    pair_lane = iota((LANES, 2 * LANES), 1).astype(F32)
    for s in range(16):
        pick[LANES * s : LANES * (s + 1)] = one_hot(jnp.broadcast_to(low[:, s : s + 1], (LANES, 2 * LANES)) == pair_lane)
    pair_of = (table >> 8).astype(F32)

    count = cnt[...]
    live = [jnp.where(count > s, 1.0, 0.0).astype(F32) for s in range(16)]
    loads[8].wait()
    w_row = w[...]
    w_column = jnp.sum(
        jnp.where(iota((LANES, LANES), 0) == iota((LANES, LANES), 1), w_row, 0.0), axis=1, keepdims=True
    )
    squares = jnp.zeros((LANES, LANES), F32)
    for s in range(16):
        first, second = y[s].astype(F32), y[16 + s].astype(F32)
        squares = squares + live[s] * (first * first + second * second)
    squares = squares * w_column

    increment = inc[...]
    known = 0.5 * jnp.sum(increment * increment, axis=0, keepdims=True)
    known = known + 0.25 * jnp.sum(squares, axis=0, keepdims=True)

    pl.semaphore_wait(barrier, len(senders))

    copies = [
        remote(8, strip_e.at[5], strip_s.at[h], (up, east, 0), 8 + h),
        remote(9, strip_e.at[0], strip_n.at[h], (down, east, 0), 10 + h),
        remote(10, strip_w.at[5], strip_s.at[h], (up, west, 1), 8 + h),
        remote(11, strip_w.at[0], strip_n.at[h], (down, west, 1), 10 + h),
        remote(2, own.at[7], south.at[1], (up, j, h)),
        remote(3, own.at[0], north.at[0], (down, j, h)),
        remote(6, strip_e, strip_in.at[h], (i, east, 0), 6 + h),
        remote(7, strip_w, strip_in.at[h], (i, west, 1), 6 + h),
        remote(1, misc, misc_in, (i, j, other)),
        remote(0, own, partner, (i, j, other)),
        remote(17, own.at[6], south.at[0], (up, j, h)),
        remote(18, own.at[1], north.at[1], (down, j, h)),
    ]
    near_s, near_n, misc_copy, own_copy, far_s, far_n = copies[4], copies[5], copies[8], copies[9], copies[10], copies[11]
    for copy in copies:
        copy.start()

    misc_copy.wait_recv()
    here, there = pl.ds(pl.multiple_of(h * half, 8), half), pl.ds(pl.multiple_of(other * half, 8), half)
    for n in range(3):
        full[n, here, :] = misc[n]
        full[n, there, :] = misc_in[n]
    mixing = full[0][:, 0:full_levels].astype(BF16)
    eye80 = one_hot(iota((full_levels, full_levels), 0) == iota((full_levels, full_levels), 1))
    mixing_back = dot_tn(mixing, eye80).astype(BF16)
    jac_t = full[1].astype(BF16)
    weighted = (full[1] * w_row).astype(BF16)
    gram_full = dot_nt(weighted, jac_t)
    gram = gram_full.astype(BF16)
    gram = jnp.concatenate([gram, (gram_full - gram.astype(F32)).astype(BF16)], axis=1)

    for s in range(16):
        span = slice(LANES * s, LANES * (s + 1))
        first = dot(weighted, y[s]) * live[s]
        second = dot(weighted, y[16 + s]) * live[s]
        slots[:, span] = jnp.concatenate(
            [first, second, jnp.broadcast_to(live[s], (16, LANES))], axis=0
        ).astype(BF16)
    for q in range(rows // 2):
        masked = jnp.concatenate(
            [
                slots[:, LANES * s : LANES * (s + 1)]
                * jnp.broadcast_to(jnp.where(pair_of[s : s + 1, :] == q, 1.0, 0.0), (slots.shape[0], LANES)).astype(BF16)
                for s in range(16)
            ],
            axis=1,
        )
        grid[:, 2 * LANES * q : 2 * LANES * (q + 1)] = dot(masked, pick[...]).astype(BF16)

    def edge_selector(core):
        number, lane = iota((16, 4 * LANES), 0), iota((16, 4 * LANES), 1)
        return one_hot((number >> 2) * LANES + (number & 3) + core * (LANES - HALO) == lane)

    outgoing, incoming = edge_selector(h), edge_selector(other)
    depth = slots.shape[0]
    for q in range(4):
        block = jnp.concatenate([grid[:, at_row(4 * g + q)] for g in range(4)], axis=1)
        edge[:, 256 * q : 256 * q + depth] = dot_nt(outgoing, block).astype(BF16)
        edge[:, 256 * q + depth : 256 * (q + 1)] = jnp.zeros((16, 256 - depth), BF16)
    late = [
        remote(12, grid.at[:, 14 * LANES : 16 * LANES], grid_s, (up, j, h)),
        remote(13, grid.at[:, 0 : 2 * LANES], grid_n, (down, j, h)),
        remote(14, edge, edge_in, (i, side, other)),
        remote(15, edge.at[:, 768:1024], edge_s, (up, side, other)),
        remote(16, edge.at[:, 0:256], edge_n, (down, side, other)),
    ]
    for copy in late:
        copy.start()

    near_s.wait_recv()
    relays = [remote(4, south.at[1], south_in.at[1], (i, j, other))]
    relays[0].start()
    near_n.wait_recv()
    relays.append(remote(5, north.at[0], north_in.at[0], (i, j, other)))
    relays[1].start()

    lane_row = iota((1, LANES), 1)
    patched = jnp.where(h == 0, lane_row - (LANES - HALO), HALO - 1 - lane_row) >= 0
    own_lanes = jnp.where(h == 0, LANES // 2 - 1 - lane_row, lane_row - LANES // 2) >= 0
    number, lane = iota((16, 3 * LANES), 0), iota((16, 3 * LANES), 1)
    place = one_hot(((number >> 2) * LANES + (number & 3) + other * (LANES - HALO) == lane) & (number < 12))
    mask_s = jnp.where(i > 0, 1.0, 0.0).astype(F32)
    mask_n = jnp.where(i < nlat - 1, 1.0, 0.0).astype(F32)

    def row_mask(e):
        return mask_s if e < HALO else mask_n if e >= HALO + rows else None

    def keep(e, value):
        mask = row_mask(e)
        return value if mask is None else value * mask

    targets = (x0, hu, hv)

    def assemble(e, sources, patches):
        for f in range(3):
            for span, source, patch in zip((here, there), sources, patches):
                value = source[f]
                if patch is not None:
                    value = jnp.where(patched, patch[:, at_row(f)], value)
                targets[f][span, at_row(e)] = keep(e, value)

    def rows_of(ref, q):
        blocks = [ref[q, f].astype(F32) for f in range(3)]
        return [[block[half * t : half * (t + 1)] for block in blocks] for t in (0, 1)]

    def patch_of(ref):
        return dot_tn(ref[:, 0 : 3 * half], place)

    own_copy.wait_recv()
    for k in (0, 1):
        remote(6, strip_e, strip_in.at[k], (i, east, 0), 6 + k).wait_recv()
    group_of = {}
    for r in range(rows):
        g = max(n for n, start in enumerate(GROUPS) if start <= r and r < start + 3)
        if r in (6, 7, 8):
            g = 2
        if r in (9, 10):
            g = 3
        group_of[r] = (g, r - GROUPS[g])
    found = {}

    def patches_for(r):
        g, t = group_of[r]
        if g not in found:
            found.clear()
            found[g] = (patch_of(strip_in.at[h, g]), patch_of(strip_in.at[other, g]))
        return [value[half * t : half * (t + 1)] for value in found[g]]

    for q in range(rows // 2):
        mine, theirs = rows_of(own, q), rows_of(partner, q)
        for t in (0, 1):
            r = 2 * q + t
            assemble(HALO + r, (mine[t], theirs[t]), patches_for(r))
    diffusion = full[2]
    centre = 1.0 - 4.0 * diffusion

    def step_row(x, e):
        value, above, below = x[:, at_row(e)], x[:, at_row(e + 1)], x[:, at_row(e - 1)]
        eastern = pltpu.roll(value, LANES - 1, 1)
        western = pltpu.roll(value, 1, 1)
        return (
            centre * value
            + diffusion * ((above + below) + (eastern + western))
            + hu[:, at_row(e)] * (western - eastern)
            + hv[:, at_row(e)] * (below - above)
        )

    def back_row(x, e):
        value, above, below = x[:, at_row(e)], x[:, at_row(e + 1)], x[:, at_row(e - 1)]
        spread, drift = diffusion * value, hu[:, at_row(e)] * value
        eastern = pltpu.roll(spread + drift, LANES - 1, 1)
        western = pltpu.roll(spread - drift, 1, 1)
        return (
            centre * value
            + (eastern + western)
            + (diffusion + hv[:, at_row(e + 1)]) * above
            + (diffusion - hv[:, at_row(e - 1)]) * below
        )

    def coupled(matrix, values):
        joined = jnp.concatenate(values, axis=1).astype(BF16)
        mixed = dot(matrix, joined)
        return [value + mixed[:, at_row(n)] for n, value in enumerate(values)]

    def pairwise(first, last):
        return [tuple(range(e, min(e + 2, last + 1))) for e in range(first, last + 1, 2)]

    def advance(pair):
        values = coupled(mixing, [step_row(x0, e) for e in pair])
        for e, value in zip(pair, values):
            x1[:, at_row(e)] = keep(e, value)

    def image_of(states, pair, target):
        halves = [state.astype(BF16) for state in states]
        joined = jnp.concatenate(halves, axis=1)
        image = dot(gram, jnp.concatenate([joined, joined], axis=0))
        for n, e in enumerate(pair):
            target[:, at_row(e)] = image[:, at_row(n)]
        return halves

    def misfit(halves, pair, target, step):
        parts = []
        for half_state, e in zip(halves, pair):
            r = e - HALO
            moved = grid[full_levels * step : full_levels * (step + 1), at_row(r)].astype(F32)
            alive = grid[2 * full_levels : depth, at_row(r)].astype(F32)[0:1]
            parts.append(half_state.astype(F32) * (alive * target[:, at_row(e)] - 2.0 * moved))
        return sum(parts)

    def image_first(pair):
        return image_of([x1[:, at_row(e)] for e in pair], pair, hold)

    def image_second(pair):
        return image_of(coupled(mixing, [step_row(x1, e) for e in pair]), pair, sm)

    for pair in pairwise(5, 18):
        advance(pair)
    total = jnp.zeros((full_levels, LANES), F32)
    for pair in pairwise(6, 17):
        total = total + misfit(image_first(pair), pair, hold, 0)
        total = total + misfit(image_second(pair), pair, sm, 1)

    for copy in relays:
        copy.wait_recv()
    for k in (0, 1):
        remote(8, strip_e.at[5], strip_s.at[k], (i, east, 0), 8 + k).wait_recv()
        remote(9, strip_e.at[0], strip_n.at[k], (i, east, 0), 10 + k).wait_recv()
    patch_s = (patch_of(strip_s.at[h]), patch_of(strip_s.at[other]))
    patch_n = (patch_of(strip_n.at[h]), patch_of(strip_n.at[other]))

    def outer_rows(which):
        q = 1 - which
        mine, theirs = rows_of(south, q), rows_of(south_in, q)
        for t in (0, 1):
            e = 2 * q + t
            fit = [None if e == 0 else value[half * (e - 1) : half * e] for value in patch_s]
            assemble(e, (mine[t], theirs[t]), fit)
        q = which
        mine, theirs = rows_of(north, q), rows_of(north_in, q)
        for t in (0, 1):
            e = 2 * q + t
            fit = [None if e == 3 else value[half * e : half * (e + 1)] for value in patch_n]
            assemble(HALO + rows + e, (mine[t], theirs[t]), fit)

    outer_rows(0)
    for pair in ((3, 4), (19, 20)):
        advance(pair)
    for pair in ((4, 5), (18, 19)):
        total = total + misfit(image_first(pair), pair, hold, 0)
        total = total + misfit(image_second(pair), pair, sm, 1)
    near[0] = known + 0.5 * jnp.sum(jnp.where(own_lanes, total, 0.0), axis=0, keepdims=True)
    first_round = [remote(21 + t, near.at[0], near.at[t], companion(t)) for t in range(1, crowd)]
    for copy in first_round:
        copy.start()

    far_s.wait_recv()
    relays.append(remote(19, south.at[0], south_in.at[0], (i, j, other)))
    relays[2].start()
    far_n.wait_recv()
    relays.append(remote(20, north.at[1], north_in.at[1], (i, j, other)))
    relays[3].start()
    for copy in late:
        copy.wait_recv()
    for q in range(4):
        value = dot_tn(edge_in[:, 256 * q : 256 * q + depth], incoming)
        for g in range(4):
            r = 4 * g + q
            f1[:, at_row(r + 2)] = jnp.where(patched, value[:, at_row(g)], grid[:, at_row(r)].astype(F32))
    f1[:, at_row(0)] = grid_s[:, at_row(0)].astype(F32)
    value = dot_tn(edge_s[:, 0:depth], incoming)
    f1[:, at_row(1)] = jnp.where(patched, value[:, at_row(3)], grid_s[:, at_row(1)].astype(F32))
    value = dot_tn(edge_n[:, 0:depth], incoming)
    f1[:, at_row(18)] = jnp.where(patched, value[:, at_row(0)], grid_n[:, at_row(0)].astype(F32))
    f1[:, at_row(19)] = grid_n[:, at_row(1)].astype(F32)

    for copy in relays[2:]:
        copy.wait_recv()
    outer_rows(1)
    for pair in ((1, 2), (21, 22)):
        advance(pair)
    for pair in ((3,), (20,)):
        image_first(pair)
    for pair in ((2, 3), (20, 21)):
        image_second(pair)

    def force(e, target, step):
        moved = f1[full_levels * step : full_levels * (step + 1), at_row(e - 2)]
        alive = f1[2 * full_levels : 2 * full_levels + 1, at_row(e - 2)]
        return alive * target[:, at_row(e)] - moved

    for pair in pairwise(2, 21):
        values = coupled(mixing_back, [force(e, sm, 1) for e in pair])
        for e, value in zip(pair, values):
            x0[:, at_row(e)] = keep(e, value)

    for pair in pairwise(3, 20):
        values = [back_row(x0, e) + force(e, hold, 0) for e in pair]
        for e, value in zip(pair, coupled(mixing_back, values)):
            sm[:, at_row(e)] = keep(e, value)

    for r in range(rows):
        x1[:, at_row(r)] = back_row(sm, r + HALO)
    for q in range(rows // 2):
        back[q] = jnp.concatenate([x1[there, at_row(2 * q)], x1[there, at_row(2 * q + 1)]], axis=0).astype(BF16)
    final = remote(21, back, back_in, (i, j, other))
    final.start()

    for copy in first_round:
        copy.wait_recv()
    part = near[0]
    for t in range(1, crowd):
        part = part + near[t]
    far[0] = part
    second_round = [remote(21 + crowd + t, far.at[0], far.at[t], follower(t)) for t in range(1, ring)]
    for copy in second_round:
        copy.start()

    final.wait_recv()
    for q in range(rows // 2):
        received = back_in[q].astype(F32)
        for t in (0, 1):
            r = 2 * q + t
            adjoint = jnp.where(own_lanes, x1[here, at_row(r)], received[half * t : half * (t + 1)])
            out_ref[pl.ds(r, half, stride=rows), :] = inc[pl.ds(r, half, stride=rows), :] + adjoint
    for copy in second_round:
        copy.wait_recv()
    part = far[0]
    for t in range(1, ring):
        part = part + far[t]
    cells = full_levels * rows * LANES * nlat * nlon
    cost_ref[0, 0] = jnp.sum(part) / cells
    for copy in copies + late + relays + [final] + first_round + second_round:
        copy.wait_send()


def deliver(gradient, cost, gradient_out, cost_out, sem):
    copy = pltpu.make_async_copy(gradient, gradient_out, sem)
    copy.start()
    cost_out[0, 0] = cost[0, 0]
    copy.wait()


def body(nlat, nlon, increment, wind_u, wind_v, diffusion, mixing, jacobian, obs_weight, innovation, counts, column_lookup):
    half, rows, width = increment.shape
    channels = jacobian.shape[0]
    wide = (HALO * 2 + rows) * width
    levels = 2 * half
    depth = 2 * levels + 16
    anywhere = pl.BlockSpec(memory_space=pltpu.MemorySpace.HBM)
    vmem = pl.BlockSpec(memory_space=pltpu.VMEM)
    smem = pl.BlockSpec(memory_space=pltpu.SMEM)
    grid_size = rows * width
    far = nlon // 2 if nlon % 2 == 0 else nlon
    near = nlat * (nlon // far) * 2
    copies = 21 + near + far
    strip = (16, width)
    scratch = [
        ((half * rows, width), F32), ((half * rows, width), F32), ((half * rows, width), F32),
        ((1, half), F32), ((half, levels), F32), ((half, channels), BF16), ((1, channels), F32),
        ((32, channels, width), BF16), ((16, width), jnp.int32),
        ((8, 3, levels, width), BF16), ((8, 3, levels, width), BF16),
        ((3, half, width), F32), ((3, half, width), F32), ((3, levels, width), F32),
        ((2, 3, levels, width), BF16), ((2, 3, levels, width), BF16),
        ((2, 3, levels, width), BF16), ((2, 3, levels, width), BF16),
        ((6, *strip), BF16), ((6, *strip), BF16), ((2, 6, *strip), BF16), ((2, *strip), BF16), ((2, *strip), BF16),
        ((depth, grid_size), BF16), ((grid_size, 2 * width), BF16), ((depth, grid_size), BF16),
        ((depth, 2 * width), BF16), ((depth, 2 * width), BF16),
        ((16, 1024), BF16), ((16, 1024), BF16), ((16, 256), BF16), ((16, 256), BF16),
        ((levels, wide), F32), ((levels, wide), F32), ((levels, wide), F32), ((levels, wide), F32), ((levels, wide), F32),
        ((depth, 20 * width), F32),
        ((levels, wide), F32), ((8, levels, width), BF16), ((8, levels, width), BF16),
        ((near, 1, width), F32), ((far, 1, width), F32),
    ]
    gradient, cost = pl.pallas_call(
        functools.partial(kernel, (nlat, nlon, half, rows)),
        out_shape=(
            jax.ShapeDtypeStruct((half * rows, width), F32),
            jax.ShapeDtypeStruct((1, 1), F32),
        ),
        in_specs=[anywhere] * 9 + [vmem],
        out_specs=(vmem, smem),
        scratch_shapes=[pltpu.VMEM(*entry) for entry in scratch]
        + [
            pltpu.SemaphoreType.DMA((9,)),
            pltpu.SemaphoreType.DMA((copies,)),
            pltpu.SemaphoreType.DMA((copies,)),
        ],
        compiler_params=pltpu.CompilerParams(
            collective_id=0, has_side_effects=True, vmem_limit_bytes=24 * 1024 * 1024
        ),
    )(
        *[
            pltpu.with_memory_space_constraint(operand, pltpu.MemorySpace.HBM)
            for operand in (
                increment.reshape(half * rows, width),
                wind_u.reshape(half * rows, width),
                wind_v.reshape(half * rows, width),
                diffusion.reshape(1, half),
                mixing,
                jacobian.T,
                obs_weight.reshape(1, channels),
                innovation.reshape(32, channels, width),
                column_lookup.reshape(16, width),
            )
        ],
        counts,
    )
    gradient, cost = pl.pallas_call(
        deliver,
        out_shape=(
            jax.ShapeDtypeStruct((half * rows, width), F32),
            jax.ShapeDtypeStruct((1, 1), F32),
        ),
        in_specs=[vmem, smem],
        out_specs=(pl.BlockSpec(memory_space=pl.ANY), smem),
        scratch_shapes=[pltpu.SemaphoreType.DMA],
        compiler_params=pltpu.CompilerParams(vmem_limit_bytes=1024 * 1024),
    )(gradient, cost)
    return gradient.reshape(increment.shape), cost.reshape(())


def solution(mesh):
    field = P("lev", "lat", "lon")
    in_specs = (
        field,
        field,
        field,
        P("lev"),
        P("lev", None),
        P(None, "lev"),
        P(),
        P(None, "lat", "lon", None, None, None),
        P("lat", "lon"),
        P("lat", "lon", None),
    )
    return jax.shard_map(
        functools.partial(body, mesh.shape["lat"], mesh.shape["lon"]),
        mesh=mesh,
        in_specs=in_specs,
        out_specs=(field, P()),
        check_vma=False,
    )
```

```python
import functools

import jax
import jax.numpy as jnp
from jax import lax
from jax.experimental import pallas as pl
from jax.experimental.pallas import tpu as pltpu
from jax.sharding import PartitionSpec as P

F32 = jnp.float32
BF16 = jnp.bfloat16
MESH = pl.DeviceIdType.MESH
HALO = 4
GROUPS = (0, 3, 6, 8, 10, 13)
LANES = 128


def dot(a, b):
    return lax.dot_general(a, b, (((1,), (0,)), ((), ())), preferred_element_type=F32)


def dot_nt(a, b):
    return lax.dot_general(a, b, (((1,), (1,)), ((), ())), preferred_element_type=F32)


def dot_tn(a, b):
    return lax.dot_general(a, b, (((0,), (0,)), ((), ())), preferred_element_type=F32)


def iota(shape, dim):
    return lax.broadcasted_iota(jnp.int32, shape, dim)


def one_hot(condition):
    return jnp.where(condition, 1.0, 0.0).astype(BF16)


def at_row(e):
    return slice(LANES * e, LANES * (e + 1))


def kernel(
    sizes,
    inc_h, u_h, v_h, dif_h, mix_h, jac_h, w_h, y_h, lut_h, cnt,
    out_ref, cost_ref,
    inc, u, v, dif, mix, jac, w, y, lut,
    own, partner, misc, misc_in, full,
    south, north, south_in, north_in,
    strip_e, strip_w, strip_in, strip_s, strip_n,
    slots, pick, grid, grid_s, grid_n, edge, edge_in, edge_s, edge_n,
    x0, x1, hu, hv, sm, f1, hold, back, back_in, near, far,
    load_sem, send_sem, recv_sem,
):
    nlat, nlon, half, rows = sizes
    full_levels = 2 * half
    i, j, h = lax.axis_index("lat"), lax.axis_index("lon"), lax.axis_index("lev")
    other = 1 - h
    up, down = lax.rem(i + 1, nlat), lax.rem(i + nlat - 1, nlat)
    east, west = lax.rem(j + 1, nlon), lax.rem(j + nlon - 1, nlon)
    side = lax.rem(j + nlon - 1 + 2 * h, nlon)

    loads = {}
    pairs = ((inc_h, inc), (u_h, u), (v_h, v), (dif_h, dif), (mix_h, mix), (jac_h, jac), (w_h, w), (lut_h, lut), (y_h, y))
    for n, (source, target) in enumerate(pairs):
        loads[n] = pltpu.make_async_copy(source, target, load_sem.at[n])
        loads[n].start()

    barrier = pltpu.get_barrier_semaphore()
    senders = [(up, j, h), (down, j, h), (i, j, other)]
    senders += [(a, side, k) for a in (i, up, down) for k in (0, 1)]
    ring = nlon // 2 if nlon % 2 == 0 else nlon
    laps = nlon // ring
    crowd = nlat * laps * 2
    lap, place_in_ring = lax.div(j, ring), lax.rem(j, ring)
    me = (i * laps + lap) * 2 + h

    def companion(t):
        index = lax.rem(me + t, crowd)
        return (
            lax.div(index, 2 * laps),
            lax.rem(lax.div(index, 2), laps) * ring + place_in_ring,
            lax.rem(index, 2),
        )

    def follower(t):
        return (i, lap * ring + lax.rem(place_in_ring + t, ring), h)

    senders += [companion(t) for t in range(1, crowd)] + [follower(t) for t in range(1, ring)]
    for device in senders:
        pl.semaphore_signal(barrier, inc=1, device_id=device, device_id_type=MESH)

    def remote(n, source, target, device, arrival=None):
        return pltpu.make_async_remote_copy(
            src_ref=source,
            dst_ref=target,
            send_sem=send_sem.at[n],
            recv_sem=recv_sem.at[n if arrival is None else arrival],
            device_id=device,
            device_id_type=MESH,
        )

    for n in range(3):
        loads[n].wait()
    fields = (inc, u, v)

    def own_row(f, r):
        value = fields[f][pl.ds(r, half, stride=rows), :]
        return value if f == 0 else 0.5 * value

    def pack(q):
        for f in range(3):
            own[q, f] = jnp.concatenate([own_row(f, 2 * q), own_row(f, 2 * q + 1)], axis=0).astype(BF16)

    pack(7)
    pack(0)
    pl.semaphore_wait(barrier, len(senders))
    near_s = remote(2, own.at[7], south.at[1], (up, j, h))
    near_n = remote(3, own.at[0], north.at[0], (down, j, h))
    near_s.start()
    near_n.start()

    wide = (32, 3 * LANES)
    number, lane = iota(wide, 0), iota(wide, 1)
    inner = number & 15
    west_edge = number >> 4
    spot = (inner >> 2) * LANES + (inner & 3) + (1 - west_edge) * (LANES - HALO)
    selector = one_hot((spot == lane) & (inner < 12))
    for g, start in enumerate(GROUPS):
        block = jnp.concatenate(
            [
                jnp.concatenate([own_row(f, start + t) for t in range(3)], axis=0).astype(BF16)
                for f in range(3)
            ],
            axis=1,
        )
        strip = dot_nt(selector, block).astype(BF16)
        strip_e[g, :, 0 : 3 * half] = strip[0:16]
        strip_w[g, :, 0 : 3 * half] = strip[16:32]
        strip_e[g, :, 3 * half : LANES] = jnp.zeros((16, LANES - 3 * half), BF16)
        strip_w[g, :, 3 * half : LANES] = jnp.zeros((16, LANES - 3 * half), BF16)

    copies = [
        remote(8, strip_e.at[5], strip_s.at[h], (up, east, 0), 8 + h),
        remote(9, strip_e.at[0], strip_n.at[h], (down, east, 0), 10 + h),
        remote(10, strip_w.at[5], strip_s.at[h], (up, west, 1), 8 + h),
        remote(11, strip_w.at[0], strip_n.at[h], (down, west, 1), 10 + h),
        remote(6, strip_e, strip_in.at[h], (i, east, 0), 6 + h),
        remote(7, strip_w, strip_in.at[h], (i, west, 1), 6 + h),
    ]
    for copy in copies:
        copy.start()

    for n in range(3, 8):
        loads[n].wait()
    misc[0] = jnp.zeros((half, LANES), F32)
    misc[0, :, 0:full_levels] = mix[...]
    eye = iota((half, half), 0) == iota((half, half), 1)
    misc[1] = jac[...].astype(F32)
    column = jnp.sum(jnp.where(eye, dif[...], 0.0), axis=1, keepdims=True)
    misc[2] = jnp.broadcast_to(column, (half, LANES))
    misc_copy = remote(1, misc, misc_in, (i, j, other))
    misc_copy.start()
    for q in range(1, 7):
        pack(q)
    own_copy = remote(0, own, partner, (i, j, other))
    far_s = remote(17, own.at[6], south.at[0], (up, j, h))
    far_n = remote(18, own.at[1], north.at[1], (down, j, h))
    own_copy.start()
    far_s.start()
    far_n.start()
    copies += [near_s, near_n, misc_copy, own_copy, far_s, far_n]

    table = lut[...]
    low = dot_nt(one_hot(iota((LANES, LANES), 0) == iota((LANES, LANES), 1)), (table & 255).astype(F32).astype(BF16))
    pair_lane = iota((LANES, 2 * LANES), 1).astype(F32)
    for s in range(16):
        pick[LANES * s : LANES * (s + 1)] = one_hot(jnp.broadcast_to(low[:, s : s + 1], (LANES, 2 * LANES)) == pair_lane)
    pair_of = (table >> 8).astype(F32)

    count = cnt[...]
    live = [jnp.where(count > s, 1.0, 0.0).astype(F32) for s in range(16)]
    loads[8].wait()
    w_row = w[...]
    w_column = jnp.sum(
        jnp.where(iota((LANES, LANES), 0) == iota((LANES, LANES), 1), w_row, 0.0), axis=1, keepdims=True
    )
    squares = jnp.zeros((LANES, LANES), F32)
    for s in range(16):
        first, second = y[s].astype(F32), y[16 + s].astype(F32)
        squares = squares + live[s] * (first * first + second * second)
    squares = squares * w_column

    increment = inc[...]
    known = 0.5 * jnp.sum(increment * increment, axis=0, keepdims=True)
    known = known + 0.25 * jnp.sum(squares, axis=0, keepdims=True)

    misc_copy.wait_recv()
    here, there = pl.ds(pl.multiple_of(h * half, 8), half), pl.ds(pl.multiple_of(other * half, 8), half)
    for n in range(3):
        full[n, here, :] = misc[n]
        full[n, there, :] = misc_in[n]
    mixing = full[0][:, 0:full_levels].astype(BF16)
    eye80 = one_hot(iota((full_levels, full_levels), 0) == iota((full_levels, full_levels), 1))
    mixing_back = dot_tn(mixing, eye80).astype(BF16)
    jac_t = full[1].astype(BF16)
    weighted = (full[1] * w_row).astype(BF16)
    gram_full = dot_nt(weighted, jac_t)
    gram = gram_full.astype(BF16)
    gram = jnp.concatenate([gram, (gram_full - gram.astype(F32)).astype(BF16)], axis=1)

    for s in range(16):
        span = slice(LANES * s, LANES * (s + 1))
        first = dot(weighted, y[s]) * live[s]
        second = dot(weighted, y[16 + s]) * live[s]
        slots[:, span] = jnp.concatenate(
            [first, second, jnp.broadcast_to(live[s], (16, LANES))], axis=0
        ).astype(BF16)
    for q in range(rows // 2):
        masked = jnp.concatenate(
            [
                slots[:, LANES * s : LANES * (s + 1)]
                * jnp.broadcast_to(jnp.where(pair_of[s : s + 1, :] == q, 1.0, 0.0), (slots.shape[0], LANES)).astype(BF16)
                for s in range(16)
            ],
            axis=1,
        )
        grid[:, 2 * LANES * q : 2 * LANES * (q + 1)] = dot(masked, pick[...]).astype(BF16)

    def edge_selector(core):
        number, lane = iota((16, 4 * LANES), 0), iota((16, 4 * LANES), 1)
        return one_hot((number >> 2) * LANES + (number & 3) + core * (LANES - HALO) == lane)

    outgoing, incoming = edge_selector(h), edge_selector(other)
    depth = slots.shape[0]
    for q in range(4):
        block = jnp.concatenate([grid[:, at_row(4 * g + q)] for g in range(4)], axis=1)
        edge[:, 256 * q : 256 * q + depth] = dot_nt(outgoing, block).astype(BF16)
        edge[:, 256 * q + depth : 256 * (q + 1)] = jnp.zeros((16, 256 - depth), BF16)
    late = [
        remote(12, grid.at[:, 14 * LANES : 16 * LANES], grid_s, (up, j, h)),
        remote(13, grid.at[:, 0 : 2 * LANES], grid_n, (down, j, h)),
        remote(14, edge, edge_in, (i, side, other)),
        remote(15, edge.at[:, 768:1024], edge_s, (up, side, other)),
        remote(16, edge.at[:, 0:256], edge_n, (down, side, other)),
    ]
    for copy in late:
        copy.start()

    near_s.wait_recv()
    relays = [remote(4, south.at[1], south_in.at[1], (i, j, other))]
    relays[0].start()
    near_n.wait_recv()
    relays.append(remote(5, north.at[0], north_in.at[0], (i, j, other)))
    relays[1].start()

    lane_row = iota((1, LANES), 1)
    patched = jnp.where(h == 0, lane_row - (LANES - HALO), HALO - 1 - lane_row) >= 0
    own_lanes = jnp.where(h == 0, LANES // 2 - 1 - lane_row, lane_row - LANES // 2) >= 0
    number, lane = iota((16, 3 * LANES), 0), iota((16, 3 * LANES), 1)
    place = one_hot(((number >> 2) * LANES + (number & 3) + other * (LANES - HALO) == lane) & (number < 12))
    mask_s = jnp.where(i > 0, 1.0, 0.0).astype(F32)
    mask_n = jnp.where(i < nlat - 1, 1.0, 0.0).astype(F32)

    def row_mask(e):
        return mask_s if e < HALO else mask_n if e >= HALO + rows else None

    def keep(e, value):
        mask = row_mask(e)
        return value if mask is None else value * mask

    targets = (x0, hu, hv)

    def assemble(e, sources, patches):
        for f in range(3):
            for span, source, patch in zip((here, there), sources, patches):
                value = source[f]
                if patch is not None:
                    value = jnp.where(patched, patch[:, at_row(f)], value)
                targets[f][span, at_row(e)] = keep(e, value)

    def rows_of(ref, q):
        blocks = [ref[q, f].astype(F32) for f in range(3)]
        return [[block[half * t : half * (t + 1)] for block in blocks] for t in (0, 1)]

    def patch_of(ref):
        return dot_tn(ref[:, 0 : 3 * half], place)

    own_copy.wait_recv()
    for k in (0, 1):
        remote(6, strip_e, strip_in.at[k], (i, east, 0), 6 + k).wait_recv()
    group_of = {}
    for r in range(rows):
        g = max(n for n, start in enumerate(GROUPS) if start <= r and r < start + 3)
        if r in (6, 7, 8):
            g = 2
        if r in (9, 10):
            g = 3
        group_of[r] = (g, r - GROUPS[g])
    found = {}

    def patches_for(r):
        g, t = group_of[r]
        if g not in found:
            found.clear()
            found[g] = (patch_of(strip_in.at[h, g]), patch_of(strip_in.at[other, g]))
        return [value[half * t : half * (t + 1)] for value in found[g]]

    for q in range(rows // 2):
        mine, theirs = rows_of(own, q), rows_of(partner, q)
        for t in (0, 1):
            r = 2 * q + t
            assemble(HALO + r, (mine[t], theirs[t]), patches_for(r))
    diffusion = full[2]
    centre = 1.0 - 4.0 * diffusion

    def step_row(x, e):
        value, above, below = x[:, at_row(e)], x[:, at_row(e + 1)], x[:, at_row(e - 1)]
        eastern = pltpu.roll(value, LANES - 1, 1)
        western = pltpu.roll(value, 1, 1)
        return (
            centre * value
            + diffusion * ((above + below) + (eastern + western))
            + hu[:, at_row(e)] * (western - eastern)
            + hv[:, at_row(e)] * (below - above)
        )

    def back_row(x, e):
        value, above, below = x[:, at_row(e)], x[:, at_row(e + 1)], x[:, at_row(e - 1)]
        spread, drift = diffusion * value, hu[:, at_row(e)] * value
        eastern = pltpu.roll(spread + drift, LANES - 1, 1)
        western = pltpu.roll(spread - drift, 1, 1)
        return (
            centre * value
            + (eastern + western)
            + (diffusion + hv[:, at_row(e + 1)]) * above
            + (diffusion - hv[:, at_row(e - 1)]) * below
        )

    def coupled(matrix, values):
        joined = jnp.concatenate(values, axis=1).astype(BF16)
        mixed = dot(matrix, joined)
        return [value + mixed[:, at_row(n)] for n, value in enumerate(values)]

    def pairwise(first, last):
        return [tuple(range(e, min(e + 2, last + 1))) for e in range(first, last + 1, 2)]

    def advance(pair):
        values = coupled(mixing, [step_row(x0, e) for e in pair])
        for e, value in zip(pair, values):
            x1[:, at_row(e)] = keep(e, value)

    def image_of(states, pair, target):
        halves = [state.astype(BF16) for state in states]
        joined = jnp.concatenate(halves, axis=1)
        image = dot(gram, jnp.concatenate([joined, joined], axis=0))
        for n, e in enumerate(pair):
            target[:, at_row(e)] = image[:, at_row(n)]
        return halves

    def misfit(halves, pair, target, step):
        parts = []
        for half_state, e in zip(halves, pair):
            r = e - HALO
            moved = grid[full_levels * step : full_levels * (step + 1), at_row(r)].astype(F32)
            alive = grid[2 * full_levels : depth, at_row(r)].astype(F32)[0:1]
            parts.append(half_state.astype(F32) * (alive * target[:, at_row(e)] - 2.0 * moved))
        return sum(parts)

    def image_first(pair):
        return image_of([x1[:, at_row(e)] for e in pair], pair, hold)

    def image_second(pair):
        return image_of(coupled(mixing, [step_row(x1, e) for e in pair]), pair, sm)

    for pair in pairwise(5, 18):
        advance(pair)
    total = jnp.zeros((full_levels, LANES), F32)
    for pair in pairwise(6, 17):
        total = total + misfit(image_first(pair), pair, hold, 0)
        total = total + misfit(image_second(pair), pair, sm, 1)

    for copy in relays:
        copy.wait_recv()
    for k in (0, 1):
        remote(8, strip_e.at[5], strip_s.at[k], (i, east, 0), 8 + k).wait_recv()
        remote(9, strip_e.at[0], strip_n.at[k], (i, east, 0), 10 + k).wait_recv()
    patch_s = (patch_of(strip_s.at[h]), patch_of(strip_s.at[other]))
    patch_n = (patch_of(strip_n.at[h]), patch_of(strip_n.at[other]))

    def outer_rows(which):
        q = 1 - which
        mine, theirs = rows_of(south, q), rows_of(south_in, q)
        for t in (0, 1):
            e = 2 * q + t
            fit = [None if e == 0 else value[half * (e - 1) : half * e] for value in patch_s]
            assemble(e, (mine[t], theirs[t]), fit)
        q = which
        mine, theirs = rows_of(north, q), rows_of(north_in, q)
        for t in (0, 1):
            e = 2 * q + t
            fit = [None if e == 3 else value[half * e : half * (e + 1)] for value in patch_n]
            assemble(HALO + rows + e, (mine[t], theirs[t]), fit)

    outer_rows(0)
    for pair in ((3, 4), (19, 20)):
        advance(pair)
    for pair in ((4, 5), (18, 19)):
        total = total + misfit(image_first(pair), pair, hold, 0)
        total = total + misfit(image_second(pair), pair, sm, 1)
    near[0] = known + 0.5 * jnp.sum(jnp.where(own_lanes, total, 0.0), axis=0, keepdims=True)
    first_round = [remote(21 + t, near.at[0], near.at[t], companion(t)) for t in range(1, crowd)]
    for copy in first_round:
        copy.start()

    far_s.wait_recv()
    relays.append(remote(19, south.at[0], south_in.at[0], (i, j, other)))
    relays[2].start()
    far_n.wait_recv()
    relays.append(remote(20, north.at[1], north_in.at[1], (i, j, other)))
    relays[3].start()
    for copy in late:
        copy.wait_recv()
    for q in range(4):
        value = dot_tn(edge_in[:, 256 * q : 256 * q + depth], incoming)
        for g in range(4):
            r = 4 * g + q
            f1[:, at_row(r + 2)] = jnp.where(patched, value[:, at_row(g)], grid[:, at_row(r)].astype(F32))
    f1[:, at_row(0)] = grid_s[:, at_row(0)].astype(F32)
    value = dot_tn(edge_s[:, 0:depth], incoming)
    f1[:, at_row(1)] = jnp.where(patched, value[:, at_row(3)], grid_s[:, at_row(1)].astype(F32))
    value = dot_tn(edge_n[:, 0:depth], incoming)
    f1[:, at_row(18)] = jnp.where(patched, value[:, at_row(0)], grid_n[:, at_row(0)].astype(F32))
    f1[:, at_row(19)] = grid_n[:, at_row(1)].astype(F32)

    for copy in relays[2:]:
        copy.wait_recv()
    outer_rows(1)
    for pair in ((1, 2), (21, 22)):
        advance(pair)
    for pair in ((3,), (20,)):
        image_first(pair)
    for pair in ((2, 3), (20, 21)):
        image_second(pair)

    def force(e, target, step):
        moved = f1[full_levels * step : full_levels * (step + 1), at_row(e - 2)]
        alive = f1[2 * full_levels : 2 * full_levels + 1, at_row(e - 2)]
        return alive * target[:, at_row(e)] - moved

    for pair in pairwise(2, 21):
        values = coupled(mixing_back, [force(e, sm, 1) for e in pair])
        for e, value in zip(pair, values):
            x0[:, at_row(e)] = keep(e, value)

    for pair in pairwise(3, 20):
        values = [back_row(x0, e) + force(e, hold, 0) for e in pair]
        for e, value in zip(pair, coupled(mixing_back, values)):
            sm[:, at_row(e)] = keep(e, value)

    for r in range(rows):
        x1[:, at_row(r)] = back_row(sm, r + HALO)
    for q in range(rows // 2):
        back[q] = jnp.concatenate([x1[there, at_row(2 * q)], x1[there, at_row(2 * q + 1)]], axis=0).astype(BF16)
    final = remote(21, back, back_in, (i, j, other))
    final.start()

    for copy in first_round:
        copy.wait_recv()
    part = near[0]
    for t in range(1, crowd):
        part = part + near[t]
    far[0] = part
    second_round = [remote(21 + crowd + t, far.at[0], far.at[t], follower(t)) for t in range(1, ring)]
    for copy in second_round:
        copy.start()

    final.wait_recv()
    for q in range(rows // 2):
        received = back_in[q].astype(F32)
        for t in (0, 1):
            r = 2 * q + t
            adjoint = jnp.where(own_lanes, x1[here, at_row(r)], received[half * t : half * (t + 1)])
            out_ref[pl.ds(r, half, stride=rows), :] = inc[pl.ds(r, half, stride=rows), :] + adjoint
    for copy in second_round:
        copy.wait_recv()
    part = far[0]
    for t in range(1, ring):
        part = part + far[t]
    cells = full_levels * rows * LANES * nlat * nlon
    cost_ref[...] = jnp.broadcast_to(jnp.sum(part, axis=1, keepdims=True) * (1.0 / cells), (1, LANES))
    for copy in copies + late + relays + [final] + first_round + second_round:
        copy.wait_send()


def deliver(gradient, cost, gradient_out, cost_out, single, sem):
    single[...] = cost[:, 0:1]
    copies = (
        pltpu.make_async_copy(gradient, gradient_out, sem.at[0]),
        pltpu.make_async_copy(single, cost_out, sem.at[1]),
    )
    for copy in copies:
        copy.start()
    for copy in copies:
        copy.wait()


def body(nlat, nlon, increment, wind_u, wind_v, diffusion, mixing, jacobian, obs_weight, innovation, counts, column_lookup):
    half, rows, width = increment.shape
    channels = jacobian.shape[0]
    wide = (HALO * 2 + rows) * width
    levels = 2 * half
    depth = 2 * levels + 16
    anywhere = pl.BlockSpec(memory_space=pltpu.MemorySpace.HBM)
    vmem = pl.BlockSpec(memory_space=pltpu.VMEM)
    grid_size = rows * width
    far = nlon // 2 if nlon % 2 == 0 else nlon
    near = nlat * (nlon // far) * 2
    copies = 21 + near + far
    strip = (16, width)
    scratch = [
        ((half * rows, width), F32), ((half * rows, width), F32), ((half * rows, width), F32),
        ((1, half), F32), ((half, levels), F32), ((half, channels), BF16), ((1, channels), F32),
        ((32, channels, width), BF16), ((16, width), jnp.int32),
        ((8, 3, levels, width), BF16), ((8, 3, levels, width), BF16),
        ((3, half, width), F32), ((3, half, width), F32), ((3, levels, width), F32),
        ((2, 3, levels, width), BF16), ((2, 3, levels, width), BF16),
        ((2, 3, levels, width), BF16), ((2, 3, levels, width), BF16),
        ((6, *strip), BF16), ((6, *strip), BF16), ((2, 6, *strip), BF16), ((2, *strip), BF16), ((2, *strip), BF16),
        ((depth, grid_size), BF16), ((grid_size, 2 * width), BF16), ((depth, grid_size), BF16),
        ((depth, 2 * width), BF16), ((depth, 2 * width), BF16),
        ((16, 1024), BF16), ((16, 1024), BF16), ((16, 256), BF16), ((16, 256), BF16),
        ((levels, wide), F32), ((levels, wide), F32), ((levels, wide), F32), ((levels, wide), F32), ((levels, wide), F32),
        ((depth, 20 * width), F32),
        ((levels, wide), F32), ((8, levels, width), BF16), ((8, levels, width), BF16),
        ((near, 1, width), F32), ((far, 1, width), F32),
    ]
    gradient, cost = pl.pallas_call(
        functools.partial(kernel, (nlat, nlon, half, rows)),
        out_shape=(
            jax.ShapeDtypeStruct((half * rows, width), F32),
            jax.ShapeDtypeStruct((1, width), F32),
        ),
        in_specs=[anywhere] * 9 + [vmem],
        out_specs=(vmem, vmem),
        scratch_shapes=[pltpu.VMEM(*entry) for entry in scratch]
        + [
            pltpu.SemaphoreType.DMA((9,)),
            pltpu.SemaphoreType.DMA((copies,)),
            pltpu.SemaphoreType.DMA((copies,)),
        ],
        compiler_params=pltpu.CompilerParams(
            collective_id=0, has_side_effects=True, vmem_limit_bytes=24 * 1024 * 1024
        ),
    )(
        *[
            pltpu.with_memory_space_constraint(operand, pltpu.MemorySpace.HBM)
            for operand in (
                increment.reshape(half * rows, width),
                wind_u.reshape(half * rows, width),
                wind_v.reshape(half * rows, width),
                diffusion.reshape(1, half),
                mixing,
                jacobian.T,
                obs_weight.reshape(1, channels),
                innovation.reshape(32, channels, width),
                column_lookup.reshape(16, width),
            )
        ],
        counts,
    )
    gradient, cost = pl.pallas_call(
        deliver,
        out_shape=(
            jax.ShapeDtypeStruct((half * rows, width), F32),
            jax.ShapeDtypeStruct((1, 1), F32),
        ),
        in_specs=[vmem, vmem],
        out_specs=(pl.BlockSpec(memory_space=pl.ANY), pl.BlockSpec(memory_space=pl.ANY)),
        scratch_shapes=[pltpu.VMEM((1, 1), F32), pltpu.SemaphoreType.DMA((2,))],
        compiler_params=pltpu.CompilerParams(vmem_limit_bytes=1024 * 1024),
    )(gradient, cost)
    return gradient.reshape(increment.shape), cost.reshape(())


def solution(mesh):
    field = P("lev", "lat", "lon")
    in_specs = (
        field,
        field,
        field,
        P("lev"),
        P("lev", None),
        P(None, "lev"),
        P(),
        P(None, "lat", "lon", None, None, None),
        P("lat", "lon"),
        P("lat", "lon", None),
    )
    return jax.shard_map(
        functools.partial(body, mesh.shape["lat"], mesh.shape["lon"]),
        mesh=mesh,
        in_specs=in_specs,
        out_specs=(field, P()),
        check_vma=False,
    )
```

```python
import functools

import jax
import jax.numpy as jnp
from jax import lax
from jax.experimental import pallas as pl
from jax.experimental.pallas import tpu as pltpu
from jax.sharding import PartitionSpec as P

F32 = jnp.float32
BF16 = jnp.bfloat16
MESH = pl.DeviceIdType.MESH
HALO = 4
GROUPS = (0, 3, 6, 8, 10, 13)
LANES = 128


def dot(a, b):
    return lax.dot_general(a, b, (((1,), (0,)), ((), ())), preferred_element_type=F32)


def dot_nt(a, b):
    return lax.dot_general(a, b, (((1,), (1,)), ((), ())), preferred_element_type=F32)


def dot_tn(a, b):
    return lax.dot_general(a, b, (((0,), (0,)), ((), ())), preferred_element_type=F32)


def iota(shape, dim):
    return lax.broadcasted_iota(jnp.int32, shape, dim)


def one_hot(condition):
    return jnp.where(condition, 1.0, 0.0).astype(BF16)


def at_row(e):
    return slice(LANES * e, LANES * (e + 1))


def kernel(
    sizes,
    inc_h, u_h, v_h, dif_h, mix_h, jac_h, w_h, y_h, lut_h, cnt,
    out_ref, cost_ref,
    inc, u, v, dif, mix, jac, w, y, lut,
    own, partner, misc, misc_in, full,
    south, north, south_in, north_in,
    strip_e, strip_w, strip_in, strip_s, strip_n,
    slots, pick, grid, grid_s, grid_n, edge, edge_in, edge_s, edge_n,
    x0, x1, hu, hv, sm, f1, hold, back, back_in, near, far,
    load_sem, send_sem, recv_sem,
):
    nlat, nlon, half, rows = sizes
    full_levels = 2 * half
    i, j, h = lax.axis_index("lat"), lax.axis_index("lon"), lax.axis_index("lev")
    other = 1 - h
    up, down = lax.rem(i + 1, nlat), lax.rem(i + nlat - 1, nlat)
    east, west = lax.rem(j + 1, nlon), lax.rem(j + nlon - 1, nlon)
    side = lax.rem(j + nlon - 1 + 2 * h, nlon)

    loads = {}
    pairs = ((inc_h, inc), (u_h, u), (v_h, v), (dif_h, dif), (mix_h, mix), (jac_h, jac), (w_h, w), (lut_h, lut), (y_h, y))
    for n, (source, target) in enumerate(pairs):
        loads[n] = pltpu.make_async_copy(source, target, load_sem.at[n])
        loads[n].start()

    barrier = pltpu.get_barrier_semaphore()
    has_up, has_down = i < nlat - 1, i > 0

    def signal(device):
        pl.semaphore_signal(barrier, inc=1, device_id=device, device_id_type=MESH)

    for device in [(i, j, other), (i, side, 0), (i, side, 1)]:
        signal(device)

    @pl.when(has_up)
    def _():
        for device in [(up, j, h), (up, side, 0), (up, side, 1)]:
            signal(device)

    @pl.when(has_down)
    def _():
        for device in [(down, j, h), (down, side, 0), (down, side, 1)]:
            signal(device)

    ring = nlon // 2 if nlon % 2 == 0 else nlon
    laps = nlon // ring
    crowd = nlat * laps * 2
    lap = lax.div(j, ring)
    latitudes = [lax.rem(i + k, nlat) for k in range(nlat)]
    longitudes = [lax.rem(j + ring * k, nlon) for k in range(laps)]
    companions = [(a, b, c) for a in latitudes for b in longitudes for c in (h, other)][1:]
    followers = [(i, lap * ring + lax.rem(j - lap * ring + t, ring), h) for t in range(1, ring)]
    for device in companions + followers:
        signal(device)
    arrivals = 3 + 3 * has_up.astype(jnp.int32) + 3 * has_down.astype(jnp.int32) + len(companions) + len(followers)

    def remote(n, source, target, device, arrival=None):
        return pltpu.make_async_remote_copy(
            src_ref=source,
            dst_ref=target,
            send_sem=send_sem.at[n],
            recv_sem=recv_sem.at[n if arrival is None else arrival],
            device_id=device,
            device_id_type=MESH,
        )

    for n in range(3):
        loads[n].wait()
    fields = (inc, u, v)

    def own_row(f, r):
        value = fields[f][pl.ds(r, half, stride=rows), :]
        return value if f == 0 else 0.5 * value

    def pack(q):
        for f in range(3):
            own[q, f] = jnp.concatenate([own_row(f, 2 * q), own_row(f, 2 * q + 1)], axis=0).astype(BF16)

    pack(7)
    pack(0)
    pl.semaphore_wait(barrier, arrivals)
    near_s = remote(2, own.at[7], south.at[1], (up, j, h))
    near_n = remote(3, own.at[0], north.at[0], (down, j, h))

    def launch(copies_up=(), copies_down=(), copies_both=()):
        for condition, group in ((has_up, copies_up), (has_down, copies_down)):
            if group:

                @pl.when(condition)
                def _(group=group):
                    for copy in group:
                        copy.start()

        for copy in copies_both:
            copy.start()

    ups, downs, boths = [near_s], [near_n], []
    launch([near_s], [near_n])

    @pl.when(jnp.logical_not(has_down))
    def _():
        for ref in (south, south_in, strip_s, grid_s, edge_s):
            ref[...] = jnp.zeros(ref.shape, ref.dtype)

    @pl.when(jnp.logical_not(has_up))
    def _():
        for ref in (north, north_in, strip_n, grid_n, edge_n):
            ref[...] = jnp.zeros(ref.shape, ref.dtype)

    wide = (32, 3 * LANES)
    number, lane = iota(wide, 0), iota(wide, 1)
    inner = number & 15
    west_edge = number >> 4
    spot = (inner >> 2) * LANES + (inner & 3) + (1 - west_edge) * (LANES - HALO)
    selector = one_hot((spot == lane) & (inner < 12))
    for g, start in enumerate(GROUPS):
        block = jnp.concatenate(
            [
                jnp.concatenate([own_row(f, start + t) for t in range(3)], axis=0).astype(BF16)
                for f in range(3)
            ],
            axis=1,
        )
        strip = dot_nt(selector, block).astype(BF16)
        strip_e[g, :, 0 : 3 * half] = strip[0:16]
        strip_w[g, :, 0 : 3 * half] = strip[16:32]
        strip_e[g, :, 3 * half : LANES] = jnp.zeros((16, LANES - 3 * half), BF16)
        strip_w[g, :, 3 * half : LANES] = jnp.zeros((16, LANES - 3 * half), BF16)

    up_copies = [
        remote(8, strip_e.at[5], strip_s.at[h], (up, east, 0), 8 + h),
        remote(10, strip_w.at[5], strip_s.at[h], (up, west, 1), 8 + h),
    ]
    down_copies = [
        remote(9, strip_e.at[0], strip_n.at[h], (down, east, 0), 10 + h),
        remote(11, strip_w.at[0], strip_n.at[h], (down, west, 1), 10 + h),
    ]
    side_copies = [
        remote(6, strip_e, strip_in.at[h], (i, east, 0), 6 + h),
        remote(7, strip_w, strip_in.at[h], (i, west, 1), 6 + h),
    ]
    launch(up_copies, down_copies, side_copies)
    ups, downs, boths = ups + up_copies, downs + down_copies, boths + side_copies

    for n in range(3, 8):
        loads[n].wait()
    misc[0] = jnp.zeros((half, LANES), F32)
    misc[0, :, 0:full_levels] = mix[...]
    eye = iota((half, half), 0) == iota((half, half), 1)
    misc[1] = jac[...].astype(F32)
    column = jnp.sum(jnp.where(eye, dif[...], 0.0), axis=1, keepdims=True)
    misc[2] = jnp.broadcast_to(column, (half, LANES))
    misc_copy = remote(1, misc, misc_in, (i, j, other))
    misc_copy.start()
    for q in range(1, 7):
        pack(q)
    own_copy = remote(0, own, partner, (i, j, other))
    far_s = remote(17, own.at[6], south.at[0], (up, j, h))
    far_n = remote(18, own.at[1], north.at[1], (down, j, h))
    own_copy.start()
    launch([far_s], [far_n])
    ups, downs, boths = ups + [far_s], downs + [far_n], boths + [misc_copy, own_copy]

    table = lut[...]
    low = dot_nt(one_hot(iota((LANES, LANES), 0) == iota((LANES, LANES), 1)), (table & 255).astype(F32).astype(BF16))
    pair_lane = iota((LANES, 2 * LANES), 1).astype(F32)
    for s in range(16):
        pick[LANES * s : LANES * (s + 1)] = one_hot(jnp.broadcast_to(low[:, s : s + 1], (LANES, 2 * LANES)) == pair_lane)
    pair_of = (table >> 8).astype(F32)

    count = cnt[...]
    live = [jnp.where(count > s, 1.0, 0.0).astype(F32) for s in range(16)]
    loads[8].wait()
    w_row = w[...]
    w_column = jnp.sum(
        jnp.where(iota((LANES, LANES), 0) == iota((LANES, LANES), 1), w_row, 0.0), axis=1, keepdims=True
    )
    squares = jnp.zeros((LANES, LANES), F32)
    for s in range(16):
        first, second = y[s].astype(F32), y[16 + s].astype(F32)
        squares = squares + live[s] * (first * first + second * second)
    squares = squares * w_column

    increment = inc[...]
    known = 0.5 * jnp.sum(increment * increment, axis=0, keepdims=True)
    known = known + 0.25 * jnp.sum(squares, axis=0, keepdims=True)

    misc_copy.wait_recv()
    here, there = pl.ds(pl.multiple_of(h * half, 8), half), pl.ds(pl.multiple_of(other * half, 8), half)
    for n in range(3):
        full[n, here, :] = misc[n]
        full[n, there, :] = misc_in[n]
    mixing = full[0][:, 0:full_levels].astype(BF16)
    eye80 = one_hot(iota((full_levels, full_levels), 0) == iota((full_levels, full_levels), 1))
    mixing_back = dot_tn(mixing, eye80).astype(BF16)
    jac_t = full[1].astype(BF16)
    weighted = (full[1] * w_row).astype(BF16)
    gram_full = dot_nt(weighted, jac_t)
    gram = gram_full.astype(BF16)
    gram = jnp.concatenate([gram, (gram_full - gram.astype(F32)).astype(BF16)], axis=1)

    for s in range(16):
        span = slice(LANES * s, LANES * (s + 1))
        first = dot(weighted, y[s]) * live[s]
        second = dot(weighted, y[16 + s]) * live[s]
        slots[:, span] = jnp.concatenate(
            [first, second, jnp.broadcast_to(live[s], (16, LANES))], axis=0
        ).astype(BF16)
    for q in range(rows // 2):
        masked = jnp.concatenate(
            [
                slots[:, LANES * s : LANES * (s + 1)]
                * jnp.broadcast_to(jnp.where(pair_of[s : s + 1, :] == q, 1.0, 0.0), (slots.shape[0], LANES)).astype(BF16)
                for s in range(16)
            ],
            axis=1,
        )
        grid[:, 2 * LANES * q : 2 * LANES * (q + 1)] = dot(masked, pick[...]).astype(BF16)

    def edge_selector(core):
        number, lane = iota((16, 4 * LANES), 0), iota((16, 4 * LANES), 1)
        return one_hot((number >> 2) * LANES + (number & 3) + core * (LANES - HALO) == lane)

    outgoing, incoming = edge_selector(h), edge_selector(other)
    depth = slots.shape[0]
    for q in range(4):
        block = jnp.concatenate([grid[:, at_row(4 * g + q)] for g in range(4)], axis=1)
        edge[:, 256 * q : 256 * q + depth] = dot_nt(outgoing, block).astype(BF16)
        edge[:, 256 * q + depth : 256 * (q + 1)] = jnp.zeros((16, 256 - depth), BF16)
    late_up = [
        remote(12, grid.at[:, 14 * LANES : 16 * LANES], grid_s, (up, j, h)),
        remote(15, edge.at[:, 768:1024], edge_s, (up, side, other)),
    ]
    late_down = [
        remote(13, grid.at[:, 0 : 2 * LANES], grid_n, (down, j, h)),
        remote(16, edge.at[:, 0:256], edge_n, (down, side, other)),
    ]
    late_side = [remote(14, edge, edge_in, (i, side, other))]
    launch(late_up, late_down, late_side)
    ups, downs, boths = ups + late_up, downs + late_down, boths + late_side

    lane_row = iota((1, LANES), 1)
    patched = jnp.where(h == 0, lane_row - (LANES - HALO), HALO - 1 - lane_row) >= 0
    own_lanes = jnp.where(h == 0, LANES // 2 - 1 - lane_row, lane_row - LANES // 2) >= 0
    number, lane = iota((16, 3 * LANES), 0), iota((16, 3 * LANES), 1)
    place = one_hot(((number >> 2) * LANES + (number & 3) + other * (LANES - HALO) == lane) & (number < 12))
    mask_s = jnp.where(i > 0, 1.0, 0.0).astype(F32)
    mask_n = jnp.where(i < nlat - 1, 1.0, 0.0).astype(F32)

    def row_mask(e):
        return mask_s if e < HALO else mask_n if e >= HALO + rows else None

    def keep(e, value):
        mask = row_mask(e)
        return value if mask is None else value * mask

    targets = (x0, hu, hv)

    def assemble(e, sources, patches):
        for f in range(3):
            for span, source, patch in zip((here, there), sources, patches):
                value = source[f]
                if patch is not None:
                    value = jnp.where(patched, patch[:, at_row(f)], value)
                targets[f][span, at_row(e)] = keep(e, value)

    def rows_of(ref, q):
        blocks = [ref[q, f].astype(F32) for f in range(3)]
        return [[block[half * t : half * (t + 1)] for block in blocks] for t in (0, 1)]

    def patch_of(ref):
        return dot_tn(ref[:, 0 : 3 * half], place)

    group_of = {}
    for r in range(rows):
        g = max(n for n, start in enumerate(GROUPS) if start <= r and r < start + 3)
        if r in (6, 7, 8):
            g = 2
        if r in (9, 10):
            g = 3
        group_of[r] = (g, r - GROUPS[g])
    found = {}

    def patches_for(r):
        g, t = group_of[r]
        if g not in found:
            found.clear()
            found[g] = (patch_of(strip_in.at[h, g]), patch_of(strip_in.at[other, g]))
        return [value[half * t : half * (t + 1)] for value in found[g]]

    own_copy.wait_recv()
    for q in range(rows // 2):
        mine, theirs = rows_of(own, q), rows_of(partner, q)
        for t in (0, 1):
            assemble(HALO + 2 * q + t, (mine[t], theirs[t]), (None, None))

    def relay(arrived, condition, n, source, target):
        copy = remote(n, source, target, (i, j, other))

        @pl.when(condition)
        def _():
            arrived.wait_recv()
            copy.start()

        return copy

    relays_s = [relay(near_s, has_down, 4, south.at[1], south_in.at[1])]
    relays_n = [relay(near_n, has_up, 5, north.at[0], north_in.at[0])]

    for k in (0, 1):
        remote(6, strip_e, strip_in.at[k], (i, east, 0), 6 + k).wait_recv()
    for r in range(rows):
        patches = patches_for(r)
        for f in range(3):
            for span, patch in zip((here, there), patches):
                current = targets[f][span, at_row(HALO + r)]
                targets[f][span, at_row(HALO + r)] = jnp.where(patched, patch[:, at_row(f)], current)

    diffusion = full[2]
    centre = 1.0 - 4.0 * diffusion

    def step_row(x, e):
        value, above, below = x[:, at_row(e)], x[:, at_row(e + 1)], x[:, at_row(e - 1)]
        eastern = pltpu.roll(value, LANES - 1, 1)
        western = pltpu.roll(value, 1, 1)
        return (
            centre * value
            + diffusion * ((above + below) + (eastern + western))
            + hu[:, at_row(e)] * (western - eastern)
            + hv[:, at_row(e)] * (below - above)
        )

    def back_row(x, e):
        value, above, below = x[:, at_row(e)], x[:, at_row(e + 1)], x[:, at_row(e - 1)]
        spread, drift = diffusion * value, hu[:, at_row(e)] * value
        eastern = pltpu.roll(spread + drift, LANES - 1, 1)
        western = pltpu.roll(spread - drift, 1, 1)
        return (
            centre * value
            + (eastern + western)
            + (diffusion + hv[:, at_row(e + 1)]) * above
            + (diffusion - hv[:, at_row(e - 1)]) * below
        )

    def coupled(matrix, values):
        joined = jnp.concatenate(values, axis=1).astype(BF16)
        mixed = dot(matrix, joined)
        return [value + mixed[:, at_row(n)] for n, value in enumerate(values)]

    def pairwise(first, last):
        return [tuple(range(e, min(e + 2, last + 1))) for e in range(first, last + 1, 2)]

    def advance(pair):
        values = coupled(mixing, [step_row(x0, e) for e in pair])
        for e, value in zip(pair, values):
            x1[:, at_row(e)] = keep(e, value)

    def image_of(states, pair, target):
        halves = [state.astype(BF16) for state in states]
        joined = jnp.concatenate(halves, axis=1)
        image = dot(gram, jnp.concatenate([joined, joined], axis=0))
        for n, e in enumerate(pair):
            target[:, at_row(e)] = image[:, at_row(n)]
        return halves

    def misfit(halves, pair, target, step):
        parts = []
        for half_state, e in zip(halves, pair):
            r = e - HALO
            moved = grid[full_levels * step : full_levels * (step + 1), at_row(r)].astype(F32)
            alive = grid[2 * full_levels : depth, at_row(r)].astype(F32)[0:1]
            parts.append(half_state.astype(F32) * (alive * target[:, at_row(e)] - 2.0 * moved))
        return sum(parts)

    def image_first(pair):
        return image_of([x1[:, at_row(e)] for e in pair], pair, hold)

    def image_second(pair):
        return image_of(coupled(mixing, [step_row(x1, e) for e in pair]), pair, sm)

    for pair in pairwise(5, 18):
        advance(pair)
    total = jnp.zeros((full_levels, LANES), F32)
    for pair in pairwise(6, 17):
        total = total + misfit(image_first(pair), pair, hold, 0)
        total = total + misfit(image_second(pair), pair, sm, 1)

    @pl.when(has_down)
    def _():
        relays_s[0].wait_recv()
        for k in (0, 1):
            remote(8, strip_e.at[5], strip_s.at[k], (i, east, 0), 8 + k).wait_recv()

    @pl.when(has_up)
    def _():
        relays_n[0].wait_recv()
        for k in (0, 1):
            remote(9, strip_e.at[0], strip_n.at[k], (i, east, 0), 10 + k).wait_recv()

    patch_s = (patch_of(strip_s.at[h]), patch_of(strip_s.at[other]))
    patch_n = (patch_of(strip_n.at[h]), patch_of(strip_n.at[other]))

    def outer_rows(which):
        q = 1 - which
        mine, theirs = rows_of(south, q), rows_of(south_in, q)
        for t in (0, 1):
            e = 2 * q + t
            fit = [None if e == 0 else value[half * (e - 1) : half * e] for value in patch_s]
            assemble(e, (mine[t], theirs[t]), fit)
        q = which
        mine, theirs = rows_of(north, q), rows_of(north_in, q)
        for t in (0, 1):
            e = 2 * q + t
            fit = [None if e == 3 else value[half * e : half * (e + 1)] for value in patch_n]
            assemble(HALO + rows + e, (mine[t], theirs[t]), fit)

    outer_rows(0)
    for pair in ((3, 4), (19, 20)):
        advance(pair)
    for pair in ((4, 5), (18, 19)):
        total = total + misfit(image_first(pair), pair, hold, 0)
        total = total + misfit(image_second(pair), pair, sm, 1)
    near[0] = known + 0.5 * jnp.sum(jnp.where(own_lanes, total, 0.0), axis=0, keepdims=True)
    first_round = [remote(22, near.at[0], near.at[t + 1], device) for t, device in enumerate(companions)]
    for copy in first_round:
        copy.start()

    relays_s.append(relay(far_s, has_down, 19, south.at[0], south_in.at[0]))
    relays_n.append(relay(far_n, has_up, 20, north.at[1], north_in.at[1]))
    late_side[0].wait_recv()

    @pl.when(has_down)
    def _():
        for copy in late_up:
            copy.wait_recv()

    @pl.when(has_up)
    def _():
        for copy in late_down:
            copy.wait_recv()

    for q in range(4):
        value = dot_tn(edge_in[:, 256 * q : 256 * q + depth], incoming)
        for g in range(4):
            r = 4 * g + q
            f1[:, at_row(r + 2)] = jnp.where(patched, value[:, at_row(g)], grid[:, at_row(r)].astype(F32))
    f1[:, at_row(0)] = grid_s[:, at_row(0)].astype(F32)
    value = dot_tn(edge_s[:, 0:depth], incoming)
    f1[:, at_row(1)] = jnp.where(patched, value[:, at_row(3)], grid_s[:, at_row(1)].astype(F32))
    value = dot_tn(edge_n[:, 0:depth], incoming)
    f1[:, at_row(18)] = jnp.where(patched, value[:, at_row(0)], grid_n[:, at_row(0)].astype(F32))
    f1[:, at_row(19)] = grid_n[:, at_row(1)].astype(F32)

    @pl.when(has_down)
    def _():
        relays_s[1].wait_recv()

    @pl.when(has_up)
    def _():
        relays_n[1].wait_recv()

    outer_rows(1)
    for pair in ((1, 2), (21, 22)):
        advance(pair)
    for pair in ((3,), (20,)):
        image_first(pair)
    for pair in ((2, 3), (20, 21)):
        image_second(pair)

    def force(e, target, step):
        moved = f1[full_levels * step : full_levels * (step + 1), at_row(e - 2)]
        alive = f1[2 * full_levels : 2 * full_levels + 1, at_row(e - 2)]
        return alive * target[:, at_row(e)] - moved

    for pair in pairwise(2, 21):
        values = coupled(mixing_back, [force(e, sm, 1) for e in pair])
        for e, value in zip(pair, values):
            x0[:, at_row(e)] = keep(e, value)

    for pair in pairwise(3, 20):
        values = [back_row(x0, e) + force(e, hold, 0) for e in pair]
        for e, value in zip(pair, coupled(mixing_back, values)):
            sm[:, at_row(e)] = keep(e, value)

    for r in range(rows):
        x1[:, at_row(r)] = back_row(sm, r + HALO)
    for q in range(rows // 2):
        back[q] = jnp.concatenate([x1[there, at_row(2 * q)], x1[there, at_row(2 * q + 1)]], axis=0).astype(BF16)
    final = remote(21, back, back_in, (i, j, other))
    final.start()

    whole_first = remote(22, near.at[1:crowd], near.at[1:crowd], (i, j, other))
    whole_first.wait_recv()
    part = near[0]
    for t in range(1, crowd):
        part = part + near[t]
    far[0] = part
    second_round = [remote(23, far.at[0], far.at[t + 1], device) for t, device in enumerate(followers)]
    for copy in second_round:
        copy.start()

    final.wait_recv()
    for q in range(rows // 2):
        received = back_in[q].astype(F32)
        for t in (0, 1):
            r = 2 * q + t
            adjoint = jnp.where(own_lanes, x1[here, at_row(r)], received[half * t : half * (t + 1)])
            out_ref[pl.ds(r, half, stride=rows), :] = inc[pl.ds(r, half, stride=rows), :] + adjoint
    whole_second = remote(23, far.at[1:ring], far.at[1:ring], (i, j, other))
    whole_second.wait_recv()
    part = far[0]
    for t in range(1, ring):
        part = part + far[t]
    cells = full_levels * rows * LANES * nlat * nlon
    cost_ref[...] = jnp.broadcast_to(jnp.sum(part, axis=1, keepdims=True) * (1.0 / cells), (1, LANES))
    for copy in boths + [final, whole_first, whole_second]:
        copy.wait_send()

    @pl.when(has_up)
    def _():
        for copy in ups + relays_n:
            copy.wait_send()

    @pl.when(has_down)
    def _():
        for copy in downs + relays_s:
            copy.wait_send()


def deliver(gradient, cost, gradient_out, cost_out, single, sem):
    single[...] = cost[:, 0:1]
    copies = (
        pltpu.make_async_copy(gradient, gradient_out, sem.at[0]),
        pltpu.make_async_copy(single, cost_out, sem.at[1]),
    )
    for copy in copies:
        copy.start()
    for copy in copies:
        copy.wait()


def body(nlat, nlon, increment, wind_u, wind_v, diffusion, mixing, jacobian, obs_weight, innovation, counts, column_lookup):
    half, rows, width = increment.shape
    channels = jacobian.shape[0]
    wide = (HALO * 2 + rows) * width
    levels = 2 * half
    depth = 2 * levels + 16
    anywhere = pl.BlockSpec(memory_space=pltpu.MemorySpace.HBM)
    vmem = pl.BlockSpec(memory_space=pltpu.VMEM)
    grid_size = rows * width
    far = nlon // 2 if nlon % 2 == 0 else nlon
    near = nlat * (nlon // far) * 2
    copies = 24
    strip = (16, width)
    scratch = [
        ((half * rows, width), F32), ((half * rows, width), F32), ((half * rows, width), F32),
        ((1, half), F32), ((half, levels), F32), ((half, channels), BF16), ((1, channels), F32),
        ((32, channels, width), BF16), ((16, width), jnp.int32),
        ((8, 3, levels, width), BF16), ((8, 3, levels, width), BF16),
        ((3, half, width), F32), ((3, half, width), F32), ((3, levels, width), F32),
        ((2, 3, levels, width), BF16), ((2, 3, levels, width), BF16),
        ((2, 3, levels, width), BF16), ((2, 3, levels, width), BF16),
        ((6, *strip), BF16), ((6, *strip), BF16), ((2, 6, *strip), BF16), ((2, *strip), BF16), ((2, *strip), BF16),
        ((depth, grid_size), BF16), ((grid_size, 2 * width), BF16), ((depth, grid_size), BF16),
        ((depth, 2 * width), BF16), ((depth, 2 * width), BF16),
        ((16, 1024), BF16), ((16, 1024), BF16), ((16, 256), BF16), ((16, 256), BF16),
        ((levels, wide), F32), ((levels, wide), F32), ((levels, wide), F32), ((levels, wide), F32), ((levels, wide), F32),
        ((depth, 20 * width), F32),
        ((levels, wide), F32), ((8, levels, width), BF16), ((8, levels, width), BF16),
        ((near, 1, width), F32), ((far, 1, width), F32),
    ]
    gradient, cost = pl.pallas_call(
        functools.partial(kernel, (nlat, nlon, half, rows)),
        out_shape=(
            jax.ShapeDtypeStruct((half * rows, width), F32),
            jax.ShapeDtypeStruct((1, width), F32),
        ),
        in_specs=[anywhere] * 9 + [vmem],
        out_specs=(vmem, vmem),
        scratch_shapes=[pltpu.VMEM(*entry) for entry in scratch]
        + [
            pltpu.SemaphoreType.DMA((9,)),
            pltpu.SemaphoreType.DMA((copies,)),
            pltpu.SemaphoreType.DMA((copies,)),
        ],
        compiler_params=pltpu.CompilerParams(
            collective_id=0, has_side_effects=True, vmem_limit_bytes=24 * 1024 * 1024
        ),
    )(
        *[
            pltpu.with_memory_space_constraint(operand, pltpu.MemorySpace.HBM)
            for operand in (
                increment.reshape(half * rows, width),
                wind_u.reshape(half * rows, width),
                wind_v.reshape(half * rows, width),
                diffusion.reshape(1, half),
                mixing,
                jacobian.T,
                obs_weight.reshape(1, channels),
                innovation.reshape(32, channels, width),
                column_lookup.reshape(16, width),
            )
        ],
        counts,
    )
    gradient, cost = pl.pallas_call(
        deliver,
        out_shape=(
            jax.ShapeDtypeStruct((half * rows, width), F32),
            jax.ShapeDtypeStruct((1, 1), F32),
        ),
        in_specs=[vmem, vmem],
        out_specs=(pl.BlockSpec(memory_space=pl.ANY), pl.BlockSpec(memory_space=pl.ANY)),
        scratch_shapes=[pltpu.VMEM((1, 1), F32), pltpu.SemaphoreType.DMA((2,))],
        compiler_params=pltpu.CompilerParams(vmem_limit_bytes=1024 * 1024),
    )(gradient, cost)
    return gradient.reshape(increment.shape), cost.reshape(())


def solution(mesh):
    field = P("lev", "lat", "lon")
    in_specs = (
        field,
        field,
        field,
        P("lev"),
        P("lev", None),
        P(None, "lev"),
        P(),
        P(None, "lat", "lon", None, None, None),
        P("lat", "lon"),
        P("lat", "lon", None),
    )
    return jax.shard_map(
        functools.partial(body, mesh.shape["lat"], mesh.shape["lon"]),
        mesh=mesh,
        in_specs=in_specs,
        out_specs=(field, P()),
        check_vma=False,
    )
```

```python
import functools

import jax
import jax.numpy as jnp
from jax import lax
from jax.experimental import pallas as pl
from jax.experimental.pallas import tpu as pltpu
from jax.sharding import PartitionSpec as P

F32 = jnp.float32
BF16 = jnp.bfloat16
MESH = pl.DeviceIdType.MESH
HALO = 4
GROUPS = (0, 3, 6, 8, 10, 13)
LANES = 128


def dot(a, b):
    return lax.dot_general(a, b, (((1,), (0,)), ((), ())), preferred_element_type=F32)


def dot_nt(a, b):
    return lax.dot_general(a, b, (((1,), (1,)), ((), ())), preferred_element_type=F32)


def dot_tn(a, b):
    return lax.dot_general(a, b, (((0,), (0,)), ((), ())), preferred_element_type=F32)


def iota(shape, dim):
    return lax.broadcasted_iota(jnp.int32, shape, dim)


def one_hot(condition):
    return jnp.where(condition, 1.0, 0.0).astype(BF16)


def at_row(e):
    return slice(LANES * e, LANES * (e + 1))


def kernel(
    sizes,
    inc_h, u_h, v_h, dif_h, mix_h, jac_h, w_h, y_h, lut_h, cnt,
    out_ref, cost_ref,
    inc, u, v, dif, mix, jac, w, y, lut,
    own, partner, misc, misc_in, full,
    halo_up, halo_down, south, north, south_in, north_in,
    strip_e, strip_w, strip_in, strip_s, strip_n,
    slots, pick, grid, grid_s, grid_n, edge, edge_in, edge_s, edge_n,
    x0, x1, hu, hv, sm, f1, hold, back, back_in, near, far, far_sent,
    load_sem, send_sem, recv_sem,
):
    nlat, nlon, half, rows = sizes
    full_levels = 2 * half
    i, j, h = lax.axis_index("lat"), lax.axis_index("lon"), lax.axis_index("lev")
    other = 1 - h
    up, down = lax.rem(i + 1, nlat), lax.rem(i + nlat - 1, nlat)
    east, west = lax.rem(j + 1, nlon), lax.rem(j + nlon - 1, nlon)
    side = lax.rem(j + nlon - 1 + 2 * h, nlon)

    loads = {}
    pairs = ((inc_h, inc), (u_h, u), (v_h, v), (dif_h, dif), (mix_h, mix), (jac_h, jac), (w_h, w), (lut_h, lut), (y_h, y))
    for n, (source, target) in enumerate(pairs):
        loads[n] = pltpu.make_async_copy(source, target, load_sem.at[n])
        loads[n].start()

    barrier = pltpu.get_barrier_semaphore()
    has_up, has_down = i < nlat - 1, i > 0

    def signal(device):
        pl.semaphore_signal(barrier, inc=1, device_id=device, device_id_type=MESH)

    for device in [(i, j, other), (i, side, 0), (i, side, 1)]:
        signal(device)

    @pl.when(has_up)
    def _():
        for device in [(up, j, h), (up, side, 0), (up, side, 1)]:
            signal(device)

    @pl.when(has_down)
    def _():
        for device in [(down, j, h), (down, side, 0), (down, side, 1)]:
            signal(device)

    ring = nlon // 2 if nlon % 2 == 0 else nlon
    laps = nlon // ring
    crowd = nlat * laps * 2
    leads, follows = h == 1, h == 0
    lap = lax.div(j, ring)
    latitudes = [lax.rem(i + k, nlat) for k in range(nlat)]
    longitudes = [lax.rem(j + ring * k, nlon) for k in range(laps)]
    plane = [(a, b) for a in latitudes for b in longitudes][1:]
    line = [(i, lap * ring + lax.rem(j - lap * ring + t, ring)) for t in range(1, ring)]

    @pl.when(leads)
    def _():
        for a, b in plane:
            signal((a, b, 0))
            signal((a, b, 1))

    for a, b in line:
        signal((a, b, 1))
    arrivals = 3 + 3 * has_up.astype(jnp.int32) + 3 * has_down.astype(jnp.int32) + len(plane) + 2 * len(line) * h

    def remote(n, source, target, device, arrival=None):
        return pltpu.make_async_remote_copy(
            src_ref=source,
            dst_ref=target,
            send_sem=send_sem.at[n],
            recv_sem=recv_sem.at[n if arrival is None else arrival],
            device_id=device,
            device_id_type=MESH,
        )

    for n in range(3):
        loads[n].wait()
    fields = (inc, u, v)

    def own_row(f, r):
        value = fields[f][pl.ds(r, half, stride=rows), :]
        return value if f == 0 else 0.5 * value

    def pack(q):
        for f in range(3):
            own[q, f] = jnp.concatenate([own_row(f, 2 * q), own_row(f, 2 * q + 1)], axis=0).astype(BF16)

    def halo_block(ref, n, first, second):
        ref[n] = jnp.concatenate([own_row(*first), own_row(*second)], axis=0).astype(BF16)

    def near_blocks(ref, order):
        halo_block(ref, 0, (0, order[0]), (0, order[1]))
        halo_block(ref, 1, (1, order[0]), (2, order[0]))

    def far_blocks(ref, order):
        halo_block(ref, 2, (0, order[2]), (0, order[3]))
        halo_block(ref, 3, (1, order[1]), (2, order[1]))
        halo_block(ref, 4, (1, order[2]), (2, order[2]))

    top, bottom = tuple(range(rows - 1, rows - 5, -1)), (0, 1, 2, 3)
    near_blocks(halo_up, top)
    near_blocks(halo_down, bottom)
    pl.semaphore_wait(barrier, arrivals)
    near_s = remote(2, halo_up.at[0:2], south.at[0:2], (up, j, h))
    near_n = remote(3, halo_down.at[0:2], north.at[0:2], (down, j, h))

    def launch(copies_up=(), copies_down=(), copies_both=()):
        for condition, group in ((has_up, copies_up), (has_down, copies_down)):
            if group:

                @pl.when(condition)
                def _(group=group):
                    for copy in group:
                        copy.start()

        for copy in copies_both:
            copy.start()

    ups, downs, boths = [near_s], [near_n], []
    launch([near_s], [near_n])

    @pl.when(jnp.logical_not(has_down))
    def _():
        for ref in (south, south_in, strip_s, grid_s, edge_s):
            ref[...] = jnp.zeros(ref.shape, ref.dtype)

    @pl.when(jnp.logical_not(has_up))
    def _():
        for ref in (north, north_in, strip_n, grid_n, edge_n):
            ref[...] = jnp.zeros(ref.shape, ref.dtype)

    wide = (32, 3 * LANES)
    number, lane = iota(wide, 0), iota(wide, 1)
    inner = number & 15
    west_edge = number >> 4
    spot = (inner >> 2) * LANES + (inner & 3) + (1 - west_edge) * (LANES - HALO)
    selector = one_hot((spot == lane) & (inner < 12))
    for g, start in enumerate(GROUPS):
        block = jnp.concatenate(
            [
                jnp.concatenate([own_row(f, start + t) for t in range(3)], axis=0).astype(BF16)
                for f in range(3)
            ],
            axis=1,
        )
        strip = dot_nt(selector, block).astype(BF16)
        strip_e[g, :, 0 : 3 * half] = strip[0:16]
        strip_w[g, :, 0 : 3 * half] = strip[16:32]
        strip_e[g, :, 3 * half : LANES] = jnp.zeros((16, LANES - 3 * half), BF16)
        strip_w[g, :, 3 * half : LANES] = jnp.zeros((16, LANES - 3 * half), BF16)

    up_copies = [
        remote(8, strip_e.at[5], strip_s.at[h], (up, east, 0), 8 + h),
        remote(10, strip_w.at[5], strip_s.at[h], (up, west, 1), 8 + h),
    ]
    down_copies = [
        remote(9, strip_e.at[0], strip_n.at[h], (down, east, 0), 10 + h),
        remote(11, strip_w.at[0], strip_n.at[h], (down, west, 1), 10 + h),
    ]
    side_copies = [
        remote(6, strip_e, strip_in.at[h], (i, east, 0), 6 + h),
        remote(7, strip_w, strip_in.at[h], (i, west, 1), 6 + h),
    ]
    launch(up_copies, down_copies, side_copies)
    ups, downs, boths = ups + up_copies, downs + down_copies, boths + side_copies

    for n in range(3, 8):
        loads[n].wait()
    misc[0] = jnp.zeros((half, LANES), F32)
    misc[0, :, 0:full_levels] = mix[...]
    eye = iota((half, half), 0) == iota((half, half), 1)
    misc[1] = jac[...].astype(F32)
    column = jnp.sum(jnp.where(eye, dif[...], 0.0), axis=1, keepdims=True)
    misc[2] = jnp.broadcast_to(column, (half, LANES))
    misc_copy = remote(1, misc, misc_in, (i, j, other))
    misc_copy.start()
    for q in range(rows // 2):
        pack(q)
    far_blocks(halo_up, top)
    far_blocks(halo_down, bottom)
    own_copy = remote(0, own, partner, (i, j, other))
    far_s = remote(17, halo_up.at[2:5], south.at[2:5], (up, j, h))
    far_n = remote(18, halo_down.at[2:5], north.at[2:5], (down, j, h))
    own_copy.start()
    launch([far_s], [far_n])
    ups, downs, boths = ups + [far_s], downs + [far_n], boths + [misc_copy, own_copy]

    table = lut[...]
    low = dot_nt(one_hot(iota((LANES, LANES), 0) == iota((LANES, LANES), 1)), (table & 255).astype(F32).astype(BF16))
    pair_lane = iota((LANES, 2 * LANES), 1).astype(F32)
    for s in range(16):
        pick[LANES * s : LANES * (s + 1)] = one_hot(jnp.broadcast_to(low[:, s : s + 1], (LANES, 2 * LANES)) == pair_lane)
    pair_of = (table >> 8).astype(F32)

    count = cnt[...]
    live = [jnp.where(count > s, 1.0, 0.0).astype(F32) for s in range(16)]
    loads[8].wait()
    w_row = w[...]
    w_column = jnp.sum(
        jnp.where(iota((LANES, LANES), 0) == iota((LANES, LANES), 1), w_row, 0.0), axis=1, keepdims=True
    )
    squares = jnp.zeros((LANES, LANES), F32)
    for s in range(16):
        first, second = y[s].astype(F32), y[16 + s].astype(F32)
        squares = squares + live[s] * (first * first + second * second)
    squares = squares * w_column

    increment = inc[...]
    known = 0.5 * jnp.sum(increment * increment, axis=0, keepdims=True)
    known = known + 0.25 * jnp.sum(squares, axis=0, keepdims=True)

    misc_copy.wait_recv()
    here, there = pl.ds(pl.multiple_of(h * half, 8), half), pl.ds(pl.multiple_of(other * half, 8), half)
    for n in range(3):
        full[n, here, :] = misc[n]
        full[n, there, :] = misc_in[n]
    mixing = full[0][:, 0:full_levels].astype(BF16)
    eye80 = one_hot(iota((full_levels, full_levels), 0) == iota((full_levels, full_levels), 1))
    mixing_back = dot_tn(mixing, eye80).astype(BF16)
    jac_t = full[1].astype(BF16)
    weighted = (full[1] * w_row).astype(BF16)
    gram_full = dot_nt(weighted, jac_t)
    gram = gram_full.astype(BF16)
    gram = jnp.concatenate([gram, (gram_full - gram.astype(F32)).astype(BF16)], axis=1)

    for s in range(16):
        span = slice(LANES * s, LANES * (s + 1))
        first = dot(weighted, y[s]) * live[s]
        second = dot(weighted, y[16 + s]) * live[s]
        slots[:, span] = jnp.concatenate(
            [first, second, jnp.broadcast_to(live[s], (16, LANES))], axis=0
        ).astype(BF16)
    for q in range(rows // 2):
        masked = jnp.concatenate(
            [
                slots[:, LANES * s : LANES * (s + 1)]
                * jnp.broadcast_to(jnp.where(pair_of[s : s + 1, :] == q, 1.0, 0.0), (slots.shape[0], LANES)).astype(BF16)
                for s in range(16)
            ],
            axis=1,
        )
        grid[:, 2 * LANES * q : 2 * LANES * (q + 1)] = dot(masked, pick[...]).astype(BF16)

    def edge_selector(core):
        number, lane = iota((16, 4 * LANES), 0), iota((16, 4 * LANES), 1)
        return one_hot((number >> 2) * LANES + (number & 3) + core * (LANES - HALO) == lane)

    outgoing, incoming = edge_selector(h), edge_selector(other)
    depth = slots.shape[0]
    for q in range(4):
        block = jnp.concatenate([grid[:, at_row(4 * g + q)] for g in range(4)], axis=1)
        edge[:, 256 * q : 256 * q + depth] = dot_nt(outgoing, block).astype(BF16)
        edge[:, 256 * q + depth : 256 * (q + 1)] = jnp.zeros((16, 256 - depth), BF16)
    late_up = [
        remote(12, grid.at[:, 14 * LANES : 16 * LANES], grid_s, (up, j, h)),
        remote(15, edge.at[:, 768:1024], edge_s, (up, side, other)),
    ]
    late_down = [
        remote(13, grid.at[:, 0 : 2 * LANES], grid_n, (down, j, h)),
        remote(16, edge.at[:, 0:256], edge_n, (down, side, other)),
    ]
    late_side = [remote(14, edge, edge_in, (i, side, other))]
    launch(late_up, late_down, late_side)
    ups, downs, boths = ups + late_up, downs + late_down, boths + late_side

    lane_row = iota((1, LANES), 1)
    patched = jnp.where(h == 0, lane_row - (LANES - HALO), HALO - 1 - lane_row) >= 0
    own_lanes = jnp.where(h == 0, LANES // 2 - 1 - lane_row, lane_row - LANES // 2) >= 0
    number, lane = iota((16, 3 * LANES), 0), iota((16, 3 * LANES), 1)
    place = one_hot(((number >> 2) * LANES + (number & 3) + other * (LANES - HALO) == lane) & (number < 12))
    mask_s = jnp.where(i > 0, 1.0, 0.0).astype(F32)
    mask_n = jnp.where(i < nlat - 1, 1.0, 0.0).astype(F32)

    def row_mask(e):
        return mask_s if e < HALO else mask_n if e >= HALO + rows else None

    def keep(e, value):
        mask = row_mask(e)
        return value if mask is None else value * mask

    targets = (x0, hu, hv)

    def assemble(e, sources, patches):
        for f in range(len(sources[0])):
            for span, source, patch in zip((here, there), sources, patches):
                value = source[f]
                if patch is not None:
                    value = jnp.where(patched, patch[:, at_row(f)], value)
                targets[f][span, at_row(e)] = keep(e, value)

    def rows_of(ref, q):
        blocks = [ref[q, f].astype(F32) for f in range(3)]
        return [[block[half * t : half * (t + 1)] for block in blocks] for t in (0, 1)]

    def patch_of(ref):
        return dot_tn(ref[:, 0 : 3 * half], place)

    group_of = {}
    for r in range(rows):
        g = max(n for n, start in enumerate(GROUPS) if start <= r and r < start + 3)
        if r in (6, 7, 8):
            g = 2
        if r in (9, 10):
            g = 3
        group_of[r] = (g, r - GROUPS[g])
    found = {}

    def patches_for(r):
        g, t = group_of[r]
        if g not in found:
            found.clear()
            found[g] = (patch_of(strip_in.at[h, g]), patch_of(strip_in.at[other, g]))
        return [value[half * t : half * (t + 1)] for value in found[g]]

    own_copy.wait_recv()
    for q in range(rows // 2):
        mine, theirs = rows_of(own, q), rows_of(partner, q)
        for t in (0, 1):
            assemble(HALO + 2 * q + t, (mine[t], theirs[t]), (None, None))

    def relay(arrived, condition, n, source, target):
        copy = remote(n, source, target, (i, j, other))

        @pl.when(condition)
        def _():
            arrived.wait_recv()
            copy.start()

        return copy

    relays_s = [relay(near_s, has_down, 4, south.at[0:2], south_in.at[0:2])]
    relays_n = [relay(near_n, has_up, 5, north.at[0:2], north_in.at[0:2])]

    for k in (0, 1):
        remote(6, strip_e, strip_in.at[k], (i, east, 0), 6 + k).wait_recv()
    for r in range(rows):
        patches = patches_for(r)
        for f in range(3):
            for span, patch in zip((here, there), patches):
                current = targets[f][span, at_row(HALO + r)]
                targets[f][span, at_row(HALO + r)] = jnp.where(patched, patch[:, at_row(f)], current)

    diffusion = full[2]
    centre = 1.0 - 4.0 * diffusion

    def step_row(x, e):
        value, above, below = x[:, at_row(e)], x[:, at_row(e + 1)], x[:, at_row(e - 1)]
        eastern = pltpu.roll(value, LANES - 1, 1)
        western = pltpu.roll(value, 1, 1)
        return (
            centre * value
            + diffusion * ((above + below) + (eastern + western))
            + hu[:, at_row(e)] * (western - eastern)
            + hv[:, at_row(e)] * (below - above)
        )

    def back_row(x, e):
        value, above, below = x[:, at_row(e)], x[:, at_row(e + 1)], x[:, at_row(e - 1)]
        spread, drift = diffusion * value, hu[:, at_row(e)] * value
        eastern = pltpu.roll(spread + drift, LANES - 1, 1)
        western = pltpu.roll(spread - drift, 1, 1)
        return (
            centre * value
            + (eastern + western)
            + (diffusion + hv[:, at_row(e + 1)]) * above
            + (diffusion - hv[:, at_row(e - 1)]) * below
        )

    def coupled(matrix, values):
        joined = jnp.concatenate(values, axis=1).astype(BF16)
        mixed = dot(matrix, joined)
        return [value + mixed[:, at_row(n)] for n, value in enumerate(values)]

    def pairwise(first, last):
        return [tuple(range(e, min(e + 2, last + 1))) for e in range(first, last + 1, 2)]

    def advance(pair):
        values = coupled(mixing, [step_row(x0, e) for e in pair])
        for e, value in zip(pair, values):
            x1[:, at_row(e)] = keep(e, value)

    def image_of(states, pair, target):
        halves = [state.astype(BF16) for state in states]
        joined = jnp.concatenate(halves, axis=1)
        image = dot(gram, jnp.concatenate([joined, joined], axis=0))
        for n, e in enumerate(pair):
            target[:, at_row(e)] = image[:, at_row(n)]
        return halves

    def misfit(halves, pair, target, step):
        parts = []
        for half_state, e in zip(halves, pair):
            r = e - HALO
            moved = grid[full_levels * step : full_levels * (step + 1), at_row(r)].astype(F32)
            alive = grid[2 * full_levels : depth, at_row(r)].astype(F32)[0:1]
            parts.append(half_state.astype(F32) * (alive * target[:, at_row(e)] - 2.0 * moved))
        return sum(parts)

    def image_first(pair):
        return image_of([x1[:, at_row(e)] for e in pair], pair, hold)

    def image_second(pair):
        return image_of(coupled(mixing, [step_row(x1, e) for e in pair]), pair, sm)

    for pair in pairwise(5, 18):
        advance(pair)
    total = jnp.zeros((full_levels, LANES), F32)
    for pair in pairwise(6, 17):
        total = total + misfit(image_first(pair), pair, hold, 0)
        total = total + misfit(image_second(pair), pair, sm, 1)

    @pl.when(has_down)
    def _():
        relays_s[0].wait_recv()
        for k in (0, 1):
            remote(8, strip_e.at[5], strip_s.at[k], (i, east, 0), 8 + k).wait_recv()

    @pl.when(has_up)
    def _():
        relays_n[0].wait_recv()
        for k in (0, 1):
            remote(9, strip_e.at[0], strip_n.at[k], (i, east, 0), 10 + k).wait_recv()

    patch_s = (patch_of(strip_s.at[h]), patch_of(strip_s.at[other]))
    patch_n = (patch_of(strip_n.at[h]), patch_of(strip_n.at[other]))

    def halo_rows(ref, which):
        first = ref[2 * which].astype(F32)
        winds = [ref[1 if which == 0 else 4].astype(F32), None]
        return [
            [first[half * t : half * (t + 1)]] + ([] if winds[t] is None else [winds[t][0:half], winds[t][half:]])
            for t in (0, 1)
        ]

    def outer_rows(which):
        for sign, edge_row, refs, patches in (
            (-1, HALO - 1, (south, south_in), patch_s),
            (1, HALO + rows, (north, north_in), patch_n),
        ):
            blocks = [halo_rows(ref, which) for ref in refs]
            for t in (0, 1):
                r = 2 * which + t
                e = edge_row + sign * r
                spot = 2 - r if sign < 0 else r
                fit = [None if r == 3 else value[half * spot : half * (spot + 1)] for value in patches]
                assemble(e, [block[t] for block in blocks], fit)
            if which == 1:
                winds = [ref[3].astype(F32) for ref in refs]
                fit = [value[half : 2 * half] for value in patches]
                e = edge_row + sign
                for f in (1, 2):
                    for span, wind, patch in zip((here, there), winds, fit):
                        value = wind[half * (f - 1) : half * f]
                        targets[f][span, at_row(e)] = keep(e, jnp.where(patched, patch[:, at_row(f)], value))

    outer_rows(0)
    for pair in ((3, 4), (19, 20)):
        advance(pair)
    for pair in ((4, 5), (18, 19)):
        total = total + misfit(image_first(pair), pair, hold, 0)
        total = total + misfit(image_second(pair), pair, sm, 1)
    near[0] = known + 0.5 * jnp.sum(jnp.where(own_lanes, total, 0.0), axis=0, keepdims=True)
    own_part = remote(22, near.at[0], near.at[1], (i, j, 1))
    first_round = [remote(22, near.at[0], near.at[2 + 2 * t + h], (a, b, 1)) for t, (a, b) in enumerate(plane)]
    for copy in first_round:
        copy.start()

    @pl.when(follows)
    def _():
        own_part.start()

    relays_s.append(relay(far_s, has_down, 19, south.at[2:5], south_in.at[2:5]))
    relays_n.append(relay(far_n, has_up, 20, north.at[2:5], north_in.at[2:5]))
    late_side[0].wait_recv()

    @pl.when(has_down)
    def _():
        for copy in late_up:
            copy.wait_recv()

    @pl.when(has_up)
    def _():
        for copy in late_down:
            copy.wait_recv()

    for q in range(4):
        value = dot_tn(edge_in[:, 256 * q : 256 * q + depth], incoming)
        for g in range(4):
            r = 4 * g + q
            f1[:, at_row(r + 2)] = jnp.where(patched, value[:, at_row(g)], grid[:, at_row(r)].astype(F32))
    f1[:, at_row(0)] = grid_s[:, at_row(0)].astype(F32)
    value = dot_tn(edge_s[:, 0:depth], incoming)
    f1[:, at_row(1)] = jnp.where(patched, value[:, at_row(3)], grid_s[:, at_row(1)].astype(F32))
    value = dot_tn(edge_n[:, 0:depth], incoming)
    f1[:, at_row(18)] = jnp.where(patched, value[:, at_row(0)], grid_n[:, at_row(0)].astype(F32))
    f1[:, at_row(19)] = grid_n[:, at_row(1)].astype(F32)

    @pl.when(has_down)
    def _():
        relays_s[1].wait_recv()

    @pl.when(has_up)
    def _():
        relays_n[1].wait_recv()

    outer_rows(1)
    for pair in ((1, 2), (21, 22)):
        advance(pair)
    for pair in ((3,), (20,)):
        image_first(pair)
    for pair in ((2, 3), (20, 21)):
        image_second(pair)

    def force(e, target, step):
        moved = f1[full_levels * step : full_levels * (step + 1), at_row(e - 2)]
        alive = f1[2 * full_levels : 2 * full_levels + 1, at_row(e - 2)]
        return alive * target[:, at_row(e)] - moved

    for pair in pairwise(2, 21):
        values = coupled(mixing_back, [force(e, sm, 1) for e in pair])
        for e, value in zip(pair, values):
            x0[:, at_row(e)] = keep(e, value)

    for pair in pairwise(3, 20):
        values = [back_row(x0, e) + force(e, hold, 0) for e in pair]
        for e, value in zip(pair, coupled(mixing_back, values)):
            sm[:, at_row(e)] = keep(e, value)

    for r in range(rows):
        x1[:, at_row(r)] = back_row(sm, r + HALO)
    for q in range(rows // 2):
        back[q] = jnp.concatenate([x1[there, at_row(2 * q)], x1[there, at_row(2 * q + 1)]], axis=0).astype(BF16)
    final = remote(21, back, back_in, (i, j, other))
    final.start()

    whole_first = remote(22, near.at[1:crowd], near.at[1:crowd], (i, j, other))
    sent_first = remote(22, near.at[1 : crowd // 2], near.at[1 : crowd // 2], (i, j, other))
    second_round = [remote(23, far.at[0], far.at[t + 1], (a, b, c)) for t, (a, b) in enumerate(line) for c in (0, 1)]
    handed = remote(24, far.at[0], far.at[ring], (i, j, 0))

    @pl.when(leads)
    def _():
        whole_first.wait_recv()
        part = near[0]
        for t in range(1, crowd):
            part = part + near[t]
        far[0] = part
        for copy in second_round:
            copy.start()
        handed.start()

    final.wait_recv()
    for q in range(rows // 2):
        received = back_in[q].astype(F32)
        for t in (0, 1):
            r = 2 * q + t
            adjoint = jnp.where(own_lanes, x1[here, at_row(r)], received[half * t : half * (t + 1)])
            out_ref[pl.ds(r, half, stride=rows), :] = inc[pl.ds(r, half, stride=rows), :] + adjoint
    whole_second = remote(23, far.at[1:ring], far.at[1:ring], (i, j, other))
    sent_second = remote(23, far_sent, far_sent, (i, j, other))
    whole_second.wait_recv()

    @pl.when(follows)
    def _():
        handed.wait_recv()
        far[0] = far[ring]

    part = far[0]
    for t in range(1, ring):
        part = part + far[t]
    cells = full_levels * rows * LANES * nlat * nlon
    cost_ref[...] = jnp.broadcast_to(jnp.sum(part, axis=1, keepdims=True) * (1.0 / cells), (1, LANES))
    for copy in boths + [final, sent_first]:
        copy.wait_send()

    @pl.when(follows)
    def _():
        own_part.wait_send()

    @pl.when(leads)
    def _():
        sent_second.wait_send()
        handed.wait_send()

    @pl.when(has_up)
    def _():
        for copy in ups + relays_n:
            copy.wait_send()

    @pl.when(has_down)
    def _():
        for copy in downs + relays_s:
            copy.wait_send()


def deliver(gradient, cost, gradient_out, cost_out, single, sem):
    single[...] = cost[:, 0:1]
    copies = (
        pltpu.make_async_copy(gradient, gradient_out, sem.at[0]),
        pltpu.make_async_copy(single, cost_out, sem.at[1]),
    )
    for copy in copies:
        copy.start()
    for copy in copies:
        copy.wait()


def body(nlat, nlon, increment, wind_u, wind_v, diffusion, mixing, jacobian, obs_weight, innovation, counts, column_lookup):
    half, rows, width = increment.shape
    channels = jacobian.shape[0]
    wide = (HALO * 2 + rows) * width
    levels = 2 * half
    depth = 2 * levels + 16
    anywhere = pl.BlockSpec(memory_space=pltpu.MemorySpace.HBM)
    vmem = pl.BlockSpec(memory_space=pltpu.VMEM)
    grid_size = rows * width
    far = nlon // 2 if nlon % 2 == 0 else nlon
    near = nlat * (nlon // far) * 2
    copies = 25
    strip = (16, width)
    scratch = [
        ((half * rows, width), F32), ((half * rows, width), F32), ((half * rows, width), F32),
        ((1, half), F32), ((half, levels), F32), ((half, channels), BF16), ((1, channels), F32),
        ((32, channels, width), BF16), ((16, width), jnp.int32),
        ((8, 3, levels, width), BF16), ((8, 3, levels, width), BF16),
        ((3, half, width), F32), ((3, half, width), F32), ((3, levels, width), F32),
        *[((5, levels, width), BF16)] * 6,
        ((6, *strip), BF16), ((6, *strip), BF16), ((2, 6, *strip), BF16), ((2, *strip), BF16), ((2, *strip), BF16),
        ((depth, grid_size), BF16), ((grid_size, 2 * width), BF16), ((depth, grid_size), BF16),
        ((depth, 2 * width), BF16), ((depth, 2 * width), BF16),
        ((16, 1024), BF16), ((16, 1024), BF16), ((16, 256), BF16), ((16, 256), BF16),
        ((levels, wide), F32), ((levels, wide), F32), ((levels, wide), F32), ((levels, wide), F32), ((levels, wide), F32),
        ((depth, 20 * width), F32),
        ((levels, wide), F32), ((8, levels, width), BF16), ((8, levels, width), BF16),
        ((near, 1, width), F32), ((far + 1, 1, width), F32), ((2 * far - 2, 1, width), F32),
    ]
    gradient, cost = pl.pallas_call(
        functools.partial(kernel, (nlat, nlon, half, rows)),
        out_shape=(
            jax.ShapeDtypeStruct((half * rows, width), F32),
            jax.ShapeDtypeStruct((1, width), F32),
        ),
        in_specs=[anywhere] * 9 + [vmem],
        out_specs=(vmem, vmem),
        scratch_shapes=[pltpu.VMEM(*entry) for entry in scratch]
        + [
            pltpu.SemaphoreType.DMA((9,)),
            pltpu.SemaphoreType.DMA((copies,)),
            pltpu.SemaphoreType.DMA((copies,)),
        ],
        compiler_params=pltpu.CompilerParams(
            collective_id=0, has_side_effects=True, vmem_limit_bytes=24 * 1024 * 1024
        ),
    )(
        *[
            pltpu.with_memory_space_constraint(operand, pltpu.MemorySpace.HBM)
            for operand in (
                increment.reshape(half * rows, width),
                wind_u.reshape(half * rows, width),
                wind_v.reshape(half * rows, width),
                diffusion.reshape(1, half),
                mixing,
                jacobian.T,
                obs_weight.reshape(1, channels),
                innovation.reshape(32, channels, width),
                column_lookup.reshape(16, width),
            )
        ],
        counts,
    )
    gradient, cost = pl.pallas_call(
        deliver,
        out_shape=(
            jax.ShapeDtypeStruct((half * rows, width), F32),
            jax.ShapeDtypeStruct((1, 1), F32),
        ),
        in_specs=[vmem, vmem],
        out_specs=(pl.BlockSpec(memory_space=pl.ANY), pl.BlockSpec(memory_space=pl.ANY)),
        scratch_shapes=[pltpu.VMEM((1, 1), F32), pltpu.SemaphoreType.DMA((2,))],
        compiler_params=pltpu.CompilerParams(vmem_limit_bytes=1024 * 1024),
    )(gradient, cost)
    return gradient.reshape(increment.shape), cost.reshape(())


def solution(mesh):
    field = P("lev", "lat", "lon")
    in_specs = (
        field,
        field,
        field,
        P("lev"),
        P("lev", None),
        P(None, "lev"),
        P(),
        P(None, "lat", "lon", None, None, None),
        P("lat", "lon"),
        P("lat", "lon", None),
    )
    return jax.shard_map(
        functools.partial(body, mesh.shape["lat"], mesh.shape["lon"]),
        mesh=mesh,
        in_specs=in_specs,
        out_specs=(field, P()),
        check_vma=False,
    )
```

```python
import functools

import jax
import jax.numpy as jnp
from jax import lax
from jax.experimental import pallas as pl
from jax.experimental.pallas import tpu as pltpu
from jax.sharding import PartitionSpec as P

F32 = jnp.float32
BF16 = jnp.bfloat16
MESH = pl.DeviceIdType.MESH
HALO = 4
GROUPS = (0, 3, 6, 8, 10, 13)
LANES = 128


def dot(a, b):
    return lax.dot_general(a, b, (((1,), (0,)), ((), ())), preferred_element_type=F32)


def dot_nt(a, b):
    return lax.dot_general(a, b, (((1,), (1,)), ((), ())), preferred_element_type=F32)


def dot_tn(a, b):
    return lax.dot_general(a, b, (((0,), (0,)), ((), ())), preferred_element_type=F32)


def iota(shape, dim):
    return lax.broadcasted_iota(jnp.int32, shape, dim)


def one_hot(condition):
    return jnp.where(condition, 1.0, 0.0).astype(BF16)


def at_row(e):
    return slice(LANES * e, LANES * (e + 1))


def kernel(
    sizes,
    inc_h, u_h, v_h, dif_h, mix_h, jac_h, w_h, y_h, lut_h, cnt,
    out_ref, cost_ref,
    inc, u, v, dif, mix, jac, w, y, lut,
    own, partner, misc, misc_in, full,
    halo_up, halo_down, south, north, south_in, north_in,
    strip_e, strip_w, strip_in, strip_s, strip_n,
    slots, pick, grid, grid_s, grid_n, edge, edge_in, edge_s, edge_n,
    x0, x1, hu, hv, sm, f1, hold, back, back_in, near, far, far_sent,
    load_sem, send_sem, recv_sem,
):
    nlat, nlon, half, rows = sizes
    full_levels = 2 * half
    i, j, h = lax.axis_index("lat"), lax.axis_index("lon"), lax.axis_index("lev")
    other = 1 - h
    up, down = lax.rem(i + 1, nlat), lax.rem(i + nlat - 1, nlat)
    east, west = lax.rem(j + 1, nlon), lax.rem(j + nlon - 1, nlon)
    side = lax.rem(j + nlon - 1 + 2 * h, nlon)

    loads = {}
    pairs = ((inc_h, inc), (u_h, u), (v_h, v), (dif_h, dif), (mix_h, mix), (jac_h, jac), (w_h, w), (lut_h, lut), (y_h, y))
    for n, (source, target) in enumerate(pairs):
        loads[n] = pltpu.make_async_copy(source, target, load_sem.at[n])
        loads[n].start()

    barrier = pltpu.get_barrier_semaphore()
    has_up, has_down = i < nlat - 1, i > 0

    def signal(device):
        pl.semaphore_signal(barrier, inc=1, device_id=device, device_id_type=MESH)

    for device in [(i, j, other), (i, side, 0), (i, side, 1)]:
        signal(device)

    @pl.when(has_up)
    def _():
        for device in [(up, j, h), (up, side, 0), (up, side, 1)]:
            signal(device)

    @pl.when(has_down)
    def _():
        for device in [(down, j, h), (down, side, 0), (down, side, 1)]:
            signal(device)

    ring = nlon // 2 if nlon % 2 == 0 else nlon
    laps = nlon // ring
    crowd = nlat * laps * 2
    leads, follows = h == 1, h == 0
    lap = lax.div(j, ring)
    latitudes = [lax.rem(i + k, nlat) for k in range(nlat)]
    longitudes = [lax.rem(j + ring * k, nlon) for k in range(laps)]
    plane = [(a, b) for a in latitudes for b in longitudes][1:]
    line = [(i, lap * ring + lax.rem(j - lap * ring + t, ring)) for t in range(1, ring)]

    @pl.when(leads)
    def _():
        for a, b in plane:
            signal((a, b, 0))
            signal((a, b, 1))

    for a, b in line:
        signal((a, b, 1))
    arrivals = 3 + 3 * has_up.astype(jnp.int32) + 3 * has_down.astype(jnp.int32) + len(plane) + 2 * len(line) * h

    def remote(n, source, target, device, arrival=None):
        return pltpu.make_async_remote_copy(
            src_ref=source,
            dst_ref=target,
            send_sem=send_sem.at[n],
            recv_sem=recv_sem.at[n if arrival is None else arrival],
            device_id=device,
            device_id_type=MESH,
        )

    for n in range(3):
        loads[n].wait()
    fields = (inc, u, v)

    def own_row(f, r):
        value = fields[f][pl.ds(r, half, stride=rows), :]
        return value if f == 0 else 0.5 * value

    def pack(q):
        for f in range(3):
            own[q, f] = jnp.concatenate([own_row(f, 2 * q), own_row(f, 2 * q + 1)], axis=0).astype(BF16)

    def halo_block(ref, n, first, second):
        ref[n] = jnp.concatenate([own_row(*first), own_row(*second)], axis=0).astype(BF16)

    def near_blocks(ref, order):
        halo_block(ref, 0, (0, order[0]), (0, order[1]))
        halo_block(ref, 1, (1, order[0]), (2, order[0]))

    def far_blocks(ref, order):
        halo_block(ref, 2, (0, order[2]), (0, order[3]))
        halo_block(ref, 3, (1, order[1]), (2, order[1]))
        halo_block(ref, 4, (1, order[2]), (2, order[2]))

    top, bottom = tuple(range(rows - 1, rows - 5, -1)), (0, 1, 2, 3)
    near_blocks(halo_up, top)
    near_blocks(halo_down, bottom)
    pl.semaphore_wait(barrier, arrivals)
    near_s = remote(2, halo_up.at[0:2], south.at[0:2], (up, j, h))
    near_n = remote(3, halo_down.at[0:2], north.at[0:2], (down, j, h))

    def launch(copies_up=(), copies_down=(), copies_both=()):
        for condition, group in ((has_up, copies_up), (has_down, copies_down)):
            if group:

                @pl.when(condition)
                def _(group=group):
                    for copy in group:
                        copy.start()

        for copy in copies_both:
            copy.start()

    ups, downs, boths = [near_s], [near_n], []
    launch([near_s], [near_n])

    @pl.when(jnp.logical_not(has_down))
    def _():
        for ref in (south, south_in, strip_s, grid_s, edge_s):
            ref[...] = jnp.zeros(ref.shape, ref.dtype)

    @pl.when(jnp.logical_not(has_up))
    def _():
        for ref in (north, north_in, strip_n, grid_n, edge_n):
            ref[...] = jnp.zeros(ref.shape, ref.dtype)

    wide = (32, 3 * LANES)
    number, lane = iota(wide, 0), iota(wide, 1)
    inner = number & 15
    west_edge = number >> 4
    spot = (inner >> 2) * LANES + (inner & 3) + (1 - west_edge) * (LANES - HALO)
    selector = one_hot((spot == lane) & (inner < 12))
    for g, start in enumerate(GROUPS):
        block = jnp.concatenate(
            [
                jnp.concatenate([own_row(f, start + t) for t in range(3)], axis=0).astype(BF16)
                for f in range(3)
            ],
            axis=1,
        )
        strip = dot_nt(selector, block).astype(BF16)
        strip_e[g, :, 0 : 3 * half] = strip[0:16]
        strip_w[g, :, 0 : 3 * half] = strip[16:32]
        strip_e[g, :, 3 * half : LANES] = jnp.zeros((16, LANES - 3 * half), BF16)
        strip_w[g, :, 3 * half : LANES] = jnp.zeros((16, LANES - 3 * half), BF16)

    up_copies = [
        remote(8, strip_e.at[5], strip_s.at[h], (up, east, 0), 8 + h),
        remote(10, strip_w.at[5], strip_s.at[h], (up, west, 1), 8 + h),
    ]
    down_copies = [
        remote(9, strip_e.at[0], strip_n.at[h], (down, east, 0), 10 + h),
        remote(11, strip_w.at[0], strip_n.at[h], (down, west, 1), 10 + h),
    ]
    side_copies = [
        remote(6, strip_e, strip_in.at[h], (i, east, 0), 6 + h),
        remote(7, strip_w, strip_in.at[h], (i, west, 1), 6 + h),
    ]
    launch(up_copies, down_copies, side_copies)
    ups, downs, boths = ups + up_copies, downs + down_copies, boths + side_copies

    for n in range(3, 8):
        loads[n].wait()
    misc[0] = jnp.zeros((half, LANES), F32)
    misc[0, :, 0:full_levels] = mix[...]
    eye = iota((half, half), 0) == iota((half, half), 1)
    misc[1] = jac[...].astype(F32)
    column = jnp.sum(jnp.where(eye, dif[...], 0.0), axis=1, keepdims=True)
    misc[2] = jnp.broadcast_to(column, (half, LANES))
    misc_copy = remote(1, misc, misc_in, (i, j, other))
    misc_copy.start()
    for q in range(rows // 2):
        pack(q)
    far_blocks(halo_up, top)
    far_blocks(halo_down, bottom)
    own_copy = remote(0, own, partner, (i, j, other))
    far_s = remote(17, halo_up.at[2:5], south.at[2:5], (up, j, h))
    far_n = remote(18, halo_down.at[2:5], north.at[2:5], (down, j, h))
    own_copy.start()
    launch([far_s], [far_n])
    ups, downs, boths = ups + [far_s], downs + [far_n], boths + [misc_copy, own_copy]

    table = lut[...]
    low = dot_nt(one_hot(iota((LANES, LANES), 0) == iota((LANES, LANES), 1)), (table & 255).astype(F32).astype(BF16))
    pair_lane = iota((LANES, 2 * LANES), 1).astype(F32)
    for s in range(16):
        pick[LANES * s : LANES * (s + 1)] = one_hot(jnp.broadcast_to(low[:, s : s + 1], (LANES, 2 * LANES)) == pair_lane)
    pair_of = (table >> 8).astype(F32)

    count = cnt[...]
    live = [jnp.where(count > s, 1.0, 0.0).astype(F32) for s in range(16)]
    loads[8].wait()
    w_row = w[...]
    w_column = jnp.sum(
        jnp.where(iota((LANES, LANES), 0) == iota((LANES, LANES), 1), w_row, 0.0), axis=1, keepdims=True
    )
    squares = jnp.zeros((LANES, LANES), F32)
    for s in range(8):
        first, second = y[8 * h + s].astype(F32), y[16 + 8 * h + s].astype(F32)
        squares = squares + jnp.where(count > 8 * h + s, 1.0, 0.0) * (first * first + second * second)
    squares = squares * w_column

    increment = inc[...]
    known = 0.5 * jnp.sum(increment * increment, axis=0, keepdims=True)
    known = known + 0.5 * jnp.sum(squares, axis=0, keepdims=True)

    misc_copy.wait_recv()
    here, there = pl.ds(pl.multiple_of(h * half, 8), half), pl.ds(pl.multiple_of(other * half, 8), half)
    for n in range(3):
        full[n, here, :] = misc[n]
        full[n, there, :] = misc_in[n]
    mixing = full[0][:, 0:full_levels].astype(BF16)
    eye80 = one_hot(iota((full_levels, full_levels), 0) == iota((full_levels, full_levels), 1))
    mixing_back = dot_tn(mixing, eye80).astype(BF16)
    jac_t = full[1].astype(BF16)
    weighted = (full[1] * w_row).astype(BF16)
    gram_full = dot_nt(weighted, jac_t)
    image_matrix = gram_full + dot(gram_full.astype(BF16), mixing)
    both = jnp.concatenate([mixing, image_matrix.astype(BF16)], axis=0)

    for s in range(16):
        span = slice(LANES * s, LANES * (s + 1))
        first = dot(weighted, y[s]) * live[s]
        second = dot(weighted, y[16 + s]) * live[s]
        slots[:, span] = jnp.concatenate(
            [first, second, jnp.broadcast_to(live[s], (16, LANES))], axis=0
        ).astype(BF16)
    def masked(q):
        return jnp.concatenate(
            [
                slots[:, LANES * s : LANES * (s + 1)]
                * jnp.broadcast_to(jnp.where(pair_of[s : s + 1, :] == q, 1.0, 0.0), (slots.shape[0], LANES)).astype(BF16)
                for s in range(16)
            ],
            axis=1,
        )

    for q in range(0, rows // 2, 2):
        moved = dot(jnp.concatenate([masked(q), masked(q + 1)], axis=0), pick[...]).astype(BF16)
        for t in (0, 1):
            grid[:, 2 * LANES * (q + t) : 2 * LANES * (q + t + 1)] = moved[slots.shape[0] * t : slots.shape[0] * (t + 1)]

    def edge_selector(core):
        number, lane = iota((16, 4 * LANES), 0), iota((16, 4 * LANES), 1)
        return one_hot((number >> 2) * LANES + (number & 3) + core * (LANES - HALO) == lane)

    outgoing, incoming = edge_selector(h), edge_selector(other)
    depth = slots.shape[0]
    for q in range(4):
        block = jnp.concatenate([grid[:, at_row(4 * g + q)] for g in range(4)], axis=1)
        edge[:, 256 * q : 256 * q + depth] = dot_nt(outgoing, block).astype(BF16)
        edge[:, 256 * q + depth : 256 * (q + 1)] = jnp.zeros((16, 256 - depth), BF16)
    late_up = [
        remote(12, grid.at[:, 14 * LANES : 16 * LANES], grid_s, (up, j, h)),
        remote(15, edge.at[:, 768:1024], edge_s, (up, side, other)),
    ]
    late_down = [
        remote(13, grid.at[:, 0 : 2 * LANES], grid_n, (down, j, h)),
        remote(16, edge.at[:, 0:256], edge_n, (down, side, other)),
    ]
    late_side = [remote(14, edge, edge_in, (i, side, other))]
    launch(late_up, late_down, late_side)
    ups, downs, boths = ups + late_up, downs + late_down, boths + late_side

    lane_row = iota((1, LANES), 1)
    patched = jnp.where(h == 0, lane_row - (LANES - HALO), HALO - 1 - lane_row) >= 0
    own_lanes = jnp.where(h == 0, LANES // 2 - 1 - lane_row, lane_row - LANES // 2) >= 0
    number, lane = iota((16, 3 * LANES), 0), iota((16, 3 * LANES), 1)
    place = one_hot(((number >> 2) * LANES + (number & 3) + other * (LANES - HALO) == lane) & (number < 12))
    mask_s = jnp.where(i > 0, 1.0, 0.0).astype(F32)
    mask_n = jnp.where(i < nlat - 1, 1.0, 0.0).astype(F32)

    def row_mask(e):
        return mask_s if e < HALO else mask_n if e >= HALO + rows else None

    def keep(e, value):
        mask = row_mask(e)
        return value if mask is None else value * mask

    targets = (x0, hu, hv)

    def assemble(e, sources, patches):
        for f in range(len(sources[0])):
            for span, source, patch in zip((here, there), sources, patches):
                value = source[f]
                if patch is not None:
                    value = jnp.where(patched, patch[:, at_row(f)], value)
                targets[f][span, at_row(e)] = keep(e, value)

    def rows_of(ref, q):
        blocks = [ref[q, f].astype(F32) for f in range(3)]
        return [[block[half * t : half * (t + 1)] for block in blocks] for t in (0, 1)]

    def patch_of(ref):
        return dot_tn(ref[:, 0 : 3 * half], place)

    group_of = {}
    for r in range(rows):
        g = max(n for n, start in enumerate(GROUPS) if start <= r and r < start + 3)
        if r in (6, 7, 8):
            g = 2
        if r in (9, 10):
            g = 3
        group_of[r] = (g, r - GROUPS[g])
    found = {}

    def patches_for(r):
        g, t = group_of[r]
        if g not in found:
            found.clear()
            found[g] = (patch_of(strip_in.at[h, g]), patch_of(strip_in.at[other, g]))
        return [value[half * t : half * (t + 1)] for value in found[g]]

    own_copy.wait_recv()
    for q in range(rows // 2):
        mine, theirs = rows_of(own, q), rows_of(partner, q)
        for t in (0, 1):
            assemble(HALO + 2 * q + t, (mine[t], theirs[t]), (None, None))

    def relay(arrived, condition, n, source, target):
        copy = remote(n, source, target, (i, j, other))

        @pl.when(condition)
        def _():
            arrived.wait_recv()
            copy.start()

        return copy

    relays_s = [relay(near_s, has_down, 4, south.at[0:2], south_in.at[0:2])]
    relays_n = [relay(near_n, has_up, 5, north.at[0:2], north_in.at[0:2])]

    for k in (0, 1):
        remote(6, strip_e, strip_in.at[k], (i, east, 0), 6 + k).wait_recv()
    for r in range(rows):
        patches = patches_for(r)
        for f in range(3):
            for span, patch in zip((here, there), patches):
                current = targets[f][span, at_row(HALO + r)]
                targets[f][span, at_row(HALO + r)] = jnp.where(patched, patch[:, at_row(f)], current)

    diffusion = full[2]
    centre = 1.0 - 4.0 * diffusion

    def step_row(x, e):
        value, above, below = x[:, at_row(e)], x[:, at_row(e + 1)], x[:, at_row(e - 1)]
        eastern = pltpu.roll(value, LANES - 1, 1)
        western = pltpu.roll(value, 1, 1)
        return (
            centre * value
            + diffusion * ((above + below) + (eastern + western))
            + hu[:, at_row(e)] * (western - eastern)
            + hv[:, at_row(e)] * (below - above)
        )

    def back_row(x, e):
        value, above, below = x[:, at_row(e)], x[:, at_row(e + 1)], x[:, at_row(e - 1)]
        spread, drift = diffusion * value, hu[:, at_row(e)] * value
        eastern = pltpu.roll(spread + drift, LANES - 1, 1)
        western = pltpu.roll(spread - drift, 1, 1)
        return (
            centre * value
            + (eastern + western)
            + (diffusion + hv[:, at_row(e + 1)]) * above
            + (diffusion - hv[:, at_row(e - 1)]) * below
        )

    def coupled(matrix, values):
        joined = jnp.concatenate(values, axis=1).astype(BF16)
        mixed = dot(matrix, joined)
        return [value + mixed[:, at_row(n)] for n, value in enumerate(values)]

    def pairwise(first, last):
        return [tuple(range(e, min(e + 2, last + 1))) for e in range(first, last + 1, 2)]

    def both_of(pair, source, target):
        values = [step_row(source, e) for e in pair]
        joined = jnp.concatenate(values, axis=1).astype(BF16)
        result = dot(both, joined)
        for n, e in enumerate(pair):
            target[:, at_row(e)] = result[full_levels:, at_row(n)]
        return [value + result[0:full_levels, at_row(n)] for n, value in enumerate(values)]

    def misfit(states, pair, target, step):
        parts = []
        for state, e in zip(states, pair):
            r = e - HALO
            if 0 <= r < rows:
                moved = grid[full_levels * step : full_levels * (step + 1), at_row(r)].astype(F32)
                alive = grid[2 * full_levels : depth, at_row(r)].astype(F32)[0:1]
                parts.append(state * (alive * target[:, at_row(e)] - 2.0 * moved))
        return sum(parts)

    def advance(pair):
        states = both_of(pair, x0, hold)
        for e, value in zip(pair, states):
            x1[:, at_row(e)] = keep(e, value)
        return misfit(states, pair, hold, 0)

    def advance_second(pair):
        return misfit(both_of(pair, x1, sm), pair, sm, 1)

    total = jnp.zeros((full_levels, LANES), F32)
    for pair in pairwise(5, 18):
        total = total + advance(pair)
    for pair in pairwise(6, 17):
        total = total + advance_second(pair)

    @pl.when(has_down)
    def _():
        relays_s[0].wait_recv()
        for k in (0, 1):
            remote(8, strip_e.at[5], strip_s.at[k], (i, east, 0), 8 + k).wait_recv()

    @pl.when(has_up)
    def _():
        relays_n[0].wait_recv()
        for k in (0, 1):
            remote(9, strip_e.at[0], strip_n.at[k], (i, east, 0), 10 + k).wait_recv()

    patch_s = (patch_of(strip_s.at[h]), patch_of(strip_s.at[other]))
    patch_n = (patch_of(strip_n.at[h]), patch_of(strip_n.at[other]))

    def halo_rows(ref, which):
        first = ref[2 * which].astype(F32)
        winds = [ref[1 if which == 0 else 4].astype(F32), None]
        return [
            [first[half * t : half * (t + 1)]] + ([] if winds[t] is None else [winds[t][0:half], winds[t][half:]])
            for t in (0, 1)
        ]

    def outer_rows(which):
        for sign, edge_row, refs, patches in (
            (-1, HALO - 1, (south, south_in), patch_s),
            (1, HALO + rows, (north, north_in), patch_n),
        ):
            blocks = [halo_rows(ref, which) for ref in refs]
            for t in (0, 1):
                r = 2 * which + t
                e = edge_row + sign * r
                spot = 2 - r if sign < 0 else r
                fit = [None if r == 3 else value[half * spot : half * (spot + 1)] for value in patches]
                assemble(e, [block[t] for block in blocks], fit)
            if which == 1:
                winds = [ref[3].astype(F32) for ref in refs]
                fit = [value[half : 2 * half] for value in patches]
                e = edge_row + sign
                for f in (1, 2):
                    for span, wind, patch in zip((here, there), winds, fit):
                        value = wind[half * (f - 1) : half * f]
                        targets[f][span, at_row(e)] = keep(e, jnp.where(patched, patch[:, at_row(f)], value))

    outer_rows(0)
    for pair in ((3, 4), (19, 20)):
        total = total + advance(pair)
    for pair in ((4, 5), (18, 19)):
        total = total + advance_second(pair)
    near[0] = known + 0.5 * jnp.sum(jnp.where(own_lanes, total, 0.0), axis=0, keepdims=True)
    own_part = remote(22, near.at[0], near.at[1], (i, j, 1))
    first_round = [remote(22, near.at[0], near.at[2 + 2 * t + h], (a, b, 1)) for t, (a, b) in enumerate(plane)]
    for copy in first_round:
        copy.start()

    @pl.when(follows)
    def _():
        own_part.start()

    relays_s.append(relay(far_s, has_down, 19, south.at[2:5], south_in.at[2:5]))
    relays_n.append(relay(far_n, has_up, 20, north.at[2:5], north_in.at[2:5]))
    late_side[0].wait_recv()

    @pl.when(has_down)
    def _():
        for copy in late_up:
            copy.wait_recv()

    @pl.when(has_up)
    def _():
        for copy in late_down:
            copy.wait_recv()

    for q in range(4):
        value = dot_tn(edge_in[:, 256 * q : 256 * q + depth], incoming)
        for g in range(4):
            r = 4 * g + q
            f1[:, at_row(r + 2)] = jnp.where(patched, value[:, at_row(g)], grid[:, at_row(r)].astype(F32))
    f1[:, at_row(0)] = grid_s[:, at_row(0)].astype(F32)
    value = dot_tn(edge_s[:, 0:depth], incoming)
    f1[:, at_row(1)] = jnp.where(patched, value[:, at_row(3)], grid_s[:, at_row(1)].astype(F32))
    value = dot_tn(edge_n[:, 0:depth], incoming)
    f1[:, at_row(18)] = jnp.where(patched, value[:, at_row(0)], grid_n[:, at_row(0)].astype(F32))
    f1[:, at_row(19)] = grid_n[:, at_row(1)].astype(F32)

    @pl.when(has_down)
    def _():
        relays_s[1].wait_recv()

    @pl.when(has_up)
    def _():
        relays_n[1].wait_recv()

    outer_rows(1)
    for pair in ((1, 2), (21, 22)):
        advance(pair)
    for pair in ((2, 3), (20, 21)):
        advance_second(pair)

    def force(e, target, step):
        moved = f1[full_levels * step : full_levels * (step + 1), at_row(e - 2)]
        alive = f1[2 * full_levels : 2 * full_levels + 1, at_row(e - 2)]
        return alive * target[:, at_row(e)] - moved

    for pair in pairwise(2, 21):
        values = coupled(mixing_back, [force(e, sm, 1) for e in pair])
        for e, value in zip(pair, values):
            x0[:, at_row(e)] = keep(e, value)

    for pair in pairwise(3, 20):
        values = [back_row(x0, e) + force(e, hold, 0) for e in pair]
        for e, value in zip(pair, coupled(mixing_back, values)):
            sm[:, at_row(e)] = keep(e, value)

    for r in range(rows):
        x1[:, at_row(r)] = back_row(sm, r + HALO)
    for q in range(rows // 2):
        back[q] = jnp.concatenate([x1[there, at_row(2 * q)], x1[there, at_row(2 * q + 1)]], axis=0).astype(BF16)
    final = remote(21, back, back_in, (i, j, other))
    final.start()

    whole_first = remote(22, near.at[1:crowd], near.at[1:crowd], (i, j, other))
    sent_first = remote(22, near.at[1 : crowd // 2], near.at[1 : crowd // 2], (i, j, other))
    second_round = [remote(23, far.at[0], far.at[t + 1], (a, b, c)) for t, (a, b) in enumerate(line) for c in (0, 1)]
    handed = remote(24, far.at[0], far.at[ring], (i, j, 0))

    @pl.when(leads)
    def _():
        whole_first.wait_recv()
        part = near[0]
        for t in range(1, crowd):
            part = part + near[t]
        far[0] = part
        for copy in second_round:
            copy.start()
        handed.start()

    final.wait_recv()
    for q in range(rows // 2):
        received = back_in[q].astype(F32)
        for t in (0, 1):
            r = 2 * q + t
            adjoint = jnp.where(own_lanes, x1[here, at_row(r)], received[half * t : half * (t + 1)])
            out_ref[pl.ds(r, half, stride=rows), :] = inc[pl.ds(r, half, stride=rows), :] + adjoint
    whole_second = remote(23, far.at[1:ring], far.at[1:ring], (i, j, other))
    sent_second = remote(23, far_sent, far_sent, (i, j, other))
    whole_second.wait_recv()

    @pl.when(follows)
    def _():
        handed.wait_recv()
        far[0] = far[ring]

    part = far[0]
    for t in range(1, ring):
        part = part + far[t]
    cells = full_levels * rows * LANES * nlat * nlon
    cost_ref[...] = jnp.broadcast_to(jnp.sum(part, axis=1, keepdims=True) * (1.0 / cells), (1, LANES))
    for copy in boths + [final, sent_first]:
        copy.wait_send()

    @pl.when(follows)
    def _():
        own_part.wait_send()

    @pl.when(leads)
    def _():
        sent_second.wait_send()
        handed.wait_send()

    @pl.when(has_up)
    def _():
        for copy in ups + relays_n:
            copy.wait_send()

    @pl.when(has_down)
    def _():
        for copy in downs + relays_s:
            copy.wait_send()


def deliver(gradient, cost, gradient_out, cost_out, single, sem):
    single[...] = cost[:, 0:1]
    copies = (
        pltpu.make_async_copy(gradient, gradient_out, sem.at[0]),
        pltpu.make_async_copy(single, cost_out, sem.at[1]),
    )
    for copy in copies:
        copy.start()
    for copy in copies:
        copy.wait()


def body(nlat, nlon, increment, wind_u, wind_v, diffusion, mixing, jacobian, obs_weight, innovation, counts, column_lookup):
    half, rows, width = increment.shape
    channels = jacobian.shape[0]
    wide = (HALO * 2 + rows) * width
    levels = 2 * half
    depth = 2 * levels + 16
    anywhere = pl.BlockSpec(memory_space=pltpu.MemorySpace.HBM)
    vmem = pl.BlockSpec(memory_space=pltpu.VMEM)
    grid_size = rows * width
    far = nlon // 2 if nlon % 2 == 0 else nlon
    near = nlat * (nlon // far) * 2
    copies = 25
    strip = (16, width)
    scratch = [
        ((half * rows, width), F32), ((half * rows, width), F32), ((half * rows, width), F32),
        ((1, half), F32), ((half, levels), F32), ((half, channels), BF16), ((1, channels), F32),
        ((32, channels, width), BF16), ((16, width), jnp.int32),
        ((8, 3, levels, width), BF16), ((8, 3, levels, width), BF16),
        ((3, half, width), F32), ((3, half, width), F32), ((3, levels, width), F32),
        *[((5, levels, width), BF16)] * 6,
        ((6, *strip), BF16), ((6, *strip), BF16), ((2, 6, *strip), BF16), ((2, *strip), BF16), ((2, *strip), BF16),
        ((depth, grid_size), BF16), ((grid_size, 2 * width), BF16), ((depth, grid_size), BF16),
        ((depth, 2 * width), BF16), ((depth, 2 * width), BF16),
        ((16, 1024), BF16), ((16, 1024), BF16), ((16, 256), BF16), ((16, 256), BF16),
        ((levels, wide), F32), ((levels, wide), F32), ((levels, wide), F32), ((levels, wide), F32), ((levels, wide), F32),
        ((depth, 20 * width), F32),
        ((levels, wide), F32), ((8, levels, width), BF16), ((8, levels, width), BF16),
        ((near, 1, width), F32), ((far + 1, 1, width), F32), ((2 * far - 2, 1, width), F32),
    ]
    gradient, cost = pl.pallas_call(
        functools.partial(kernel, (nlat, nlon, half, rows)),
        out_shape=(
            jax.ShapeDtypeStruct((half * rows, width), F32),
            jax.ShapeDtypeStruct((1, width), F32),
        ),
        in_specs=[anywhere] * 9 + [vmem],
        out_specs=(vmem, vmem),
        scratch_shapes=[pltpu.VMEM(*entry) for entry in scratch]
        + [
            pltpu.SemaphoreType.DMA((9,)),
            pltpu.SemaphoreType.DMA((copies,)),
            pltpu.SemaphoreType.DMA((copies,)),
        ],
        compiler_params=pltpu.CompilerParams(
            collective_id=0, has_side_effects=True, vmem_limit_bytes=24 * 1024 * 1024
        ),
    )(
        *[
            pltpu.with_memory_space_constraint(operand, pltpu.MemorySpace.HBM)
            for operand in (
                increment.reshape(half * rows, width),
                wind_u.reshape(half * rows, width),
                wind_v.reshape(half * rows, width),
                diffusion.reshape(1, half),
                mixing,
                jacobian.T,
                obs_weight.reshape(1, channels),
                innovation.reshape(32, channels, width),
                column_lookup.reshape(16, width),
            )
        ],
        counts,
    )
    gradient, cost = pl.pallas_call(
        deliver,
        out_shape=(
            jax.ShapeDtypeStruct((half * rows, width), F32),
            jax.ShapeDtypeStruct((1, 1), F32),
        ),
        in_specs=[vmem, vmem],
        out_specs=(pl.BlockSpec(memory_space=pl.ANY), pl.BlockSpec(memory_space=pl.ANY)),
        scratch_shapes=[pltpu.VMEM((1, 1), F32), pltpu.SemaphoreType.DMA((2,))],
        compiler_params=pltpu.CompilerParams(vmem_limit_bytes=1024 * 1024),
    )(gradient, cost)
    return gradient.reshape(increment.shape), cost.reshape(())


def solution(mesh):
    field = P("lev", "lat", "lon")
    in_specs = (
        field,
        field,
        field,
        P("lev"),
        P("lev", None),
        P(None, "lev"),
        P(),
        P(None, "lat", "lon", None, None, None),
        P("lat", "lon"),
        P("lat", "lon", None),
    )
    return jax.shard_map(
        functools.partial(body, mesh.shape["lat"], mesh.shape["lon"]),
        mesh=mesh,
        in_specs=in_specs,
        out_specs=(field, P()),
        check_vma=False,
    )
```

```python
import functools

import jax
import jax.numpy as jnp
from jax import lax
from jax.experimental import pallas as pl
from jax.experimental.pallas import tpu as pltpu
from jax.sharding import PartitionSpec as P

F32 = jnp.float32
BF16 = jnp.bfloat16
MESH = pl.DeviceIdType.MESH
HALO = 4
GROUPS = (0, 3, 6, 8, 10, 13)
LANES = 128


def dot(a, b):
    return lax.dot_general(a, b, (((1,), (0,)), ((), ())), preferred_element_type=F32)


def dot_nt(a, b):
    return lax.dot_general(a, b, (((1,), (1,)), ((), ())), preferred_element_type=F32)


def dot_tn(a, b):
    return lax.dot_general(a, b, (((0,), (0,)), ((), ())), preferred_element_type=F32)


def iota(shape, dim):
    return lax.broadcasted_iota(jnp.int32, shape, dim)


def one_hot(condition):
    return jnp.where(condition, 1.0, 0.0).astype(BF16)


def at_row(e):
    return slice(LANES * e, LANES * (e + 1))


def kernel(
    sizes,
    inc_h, u_h, v_h, dif_h, mix_h, jac_h, w_h, y_h, lut_h, cnt,
    out_ref, cost_ref,
    inc, u, v, dif, mix, jac, w, y, lut,
    own, partner, misc, misc_in, full,
    halo_up, halo_down, south, north, south_in, north_in,
    strip_e, strip_w, strip_in, strip_s, strip_n,
    slots, pick, grid, grid_s, grid_n, edge, edge_in, edge_s, edge_n,
    x0, x1, hu, hv, sm, f1, hold, back, back_in, near, far, far_sent,
    load_sem, send_sem, recv_sem,
):
    nlat, nlon, half, rows = sizes
    full_levels = 2 * half
    i, j, h = lax.axis_index("lat"), lax.axis_index("lon"), lax.axis_index("lev")
    other = 1 - h
    up, down = lax.rem(i + 1, nlat), lax.rem(i + nlat - 1, nlat)
    east, west = lax.rem(j + 1, nlon), lax.rem(j + nlon - 1, nlon)
    side = lax.rem(j + nlon - 1 + 2 * h, nlon)

    loads = {}
    pairs = ((inc_h, inc), (u_h, u), (v_h, v), (dif_h, dif), (mix_h, mix), (jac_h, jac), (w_h, w), (lut_h, lut), (y_h, y))
    for n, (source, target) in enumerate(pairs):
        loads[n] = pltpu.make_async_copy(source, target, load_sem.at[n])
        loads[n].start()

    barrier = pltpu.get_barrier_semaphore()
    has_up, has_down = i < nlat - 1, i > 0

    def signal(device):
        pl.semaphore_signal(barrier, inc=1, device_id=device, device_id_type=MESH)

    for device in [(i, j, other), (i, side, 0), (i, side, 1)]:
        signal(device)

    @pl.when(has_up)
    def _():
        for device in [(up, j, h), (up, side, 0), (up, side, 1)]:
            signal(device)

    @pl.when(has_down)
    def _():
        for device in [(down, j, h), (down, side, 0), (down, side, 1)]:
            signal(device)

    ring = nlon // 2 if nlon % 2 == 0 else nlon
    laps = nlon // ring
    crowd = nlat * laps * 2
    leads, follows = h == 1, h == 0
    lap = lax.div(j, ring)
    latitudes = [lax.rem(i + k, nlat) for k in range(nlat)]
    longitudes = [lax.rem(j + ring * k, nlon) for k in range(laps)]
    plane = [(a, b) for a in latitudes for b in longitudes][1:]
    line = [(i, lap * ring + lax.rem(j - lap * ring + t, ring)) for t in range(1, ring)]

    @pl.when(leads)
    def _():
        for a, b in plane:
            signal((a, b, 0))
            signal((a, b, 1))

    for a, b in line:
        signal((a, b, 1))
    arrivals = 3 + 3 * has_up.astype(jnp.int32) + 3 * has_down.astype(jnp.int32) + len(plane) + 2 * len(line) * h

    def remote(n, source, target, device, arrival=None):
        return pltpu.make_async_remote_copy(
            src_ref=source,
            dst_ref=target,
            send_sem=send_sem.at[n],
            recv_sem=recv_sem.at[n if arrival is None else arrival],
            device_id=device,
            device_id_type=MESH,
        )

    for n in range(3):
        loads[n].wait()
    fields = (inc, u, v)

    def own_row(f, r):
        value = fields[f][pl.ds(r, half, stride=rows), :]
        return value if f == 0 else 0.5 * value

    def pack(q):
        for f in range(3):
            own[q, f] = jnp.concatenate([own_row(f, 2 * q), own_row(f, 2 * q + 1)], axis=0).astype(BF16)

    def halo_block(ref, n, first, second):
        ref[n] = jnp.concatenate([own_row(*first), own_row(*second)], axis=0).astype(BF16)

    def near_blocks(ref, order):
        halo_block(ref, 0, (0, order[0]), (0, order[1]))
        halo_block(ref, 1, (1, order[0]), (2, order[0]))

    def far_blocks(ref, order):
        halo_block(ref, 2, (0, order[2]), (0, order[3]))
        halo_block(ref, 3, (1, order[1]), (2, order[1]))
        halo_block(ref, 4, (1, order[2]), (2, order[2]))

    top, bottom = tuple(range(rows - 1, rows - 5, -1)), (0, 1, 2, 3)
    near_blocks(halo_up, top)
    near_blocks(halo_down, bottom)
    pl.semaphore_wait(barrier, arrivals)
    near_s = remote(2, halo_up.at[0:2], south.at[0:2], (up, j, h))
    near_n = remote(3, halo_down.at[0:2], north.at[0:2], (down, j, h))

    def launch(copies_up=(), copies_down=(), copies_both=()):
        for condition, group in ((has_up, copies_up), (has_down, copies_down)):
            if group:

                @pl.when(condition)
                def _(group=group):
                    for copy in group:
                        copy.start()

        for copy in copies_both:
            copy.start()

    ups, downs, boths = [near_s], [near_n], []
    launch([near_s], [near_n])

    @pl.when(jnp.logical_not(has_down))
    def _():
        for ref in (south, south_in, strip_s, grid_s, edge_s):
            ref[...] = jnp.zeros(ref.shape, ref.dtype)

    @pl.when(jnp.logical_not(has_up))
    def _():
        for ref in (north, north_in, strip_n, grid_n, edge_n):
            ref[...] = jnp.zeros(ref.shape, ref.dtype)

    wide = (32, 3 * LANES)
    number, lane = iota(wide, 0), iota(wide, 1)
    inner = number & 15
    west_edge = number >> 4
    spot = (inner >> 2) * LANES + (inner & 3) + (1 - west_edge) * (LANES - HALO)
    selector = one_hot((spot == lane) & (inner < 12))
    for g, start in enumerate(GROUPS):
        block = jnp.concatenate(
            [
                jnp.concatenate([own_row(f, start + t) for t in range(3)], axis=0).astype(BF16)
                for f in range(3)
            ],
            axis=1,
        )
        strip = dot_nt(selector, block).astype(BF16)
        strip_e[g, :, 0 : 3 * half] = strip[0:16]
        strip_w[g, :, 0 : 3 * half] = strip[16:32]
        strip_e[g, :, 3 * half : LANES] = jnp.zeros((16, LANES - 3 * half), BF16)
        strip_w[g, :, 3 * half : LANES] = jnp.zeros((16, LANES - 3 * half), BF16)

    up_copies = [
        remote(8, strip_e.at[5], strip_s.at[h], (up, east, 0), 8 + h),
        remote(10, strip_w.at[5], strip_s.at[h], (up, west, 1), 8 + h),
    ]
    down_copies = [
        remote(9, strip_e.at[0], strip_n.at[h], (down, east, 0), 10 + h),
        remote(11, strip_w.at[0], strip_n.at[h], (down, west, 1), 10 + h),
    ]
    side_copies = [
        remote(6, strip_e, strip_in.at[h], (i, east, 0), 6 + h),
        remote(7, strip_w, strip_in.at[h], (i, west, 1), 6 + h),
    ]
    launch(up_copies, down_copies, side_copies)
    ups, downs, boths = ups + up_copies, downs + down_copies, boths + side_copies

    for n in range(3, 8):
        loads[n].wait()
    misc[0] = jnp.zeros((half, LANES), F32)
    misc[0, :, 0:full_levels] = mix[...]
    eye = iota((half, half), 0) == iota((half, half), 1)
    misc[1] = jac[...].astype(F32)
    column = jnp.sum(jnp.where(eye, dif[...], 0.0), axis=1, keepdims=True)
    misc[2] = jnp.broadcast_to(column, (half, LANES))
    misc_copy = remote(1, misc, misc_in, (i, j, other))
    misc_copy.start()
    for q in range(rows // 2):
        pack(q)
    far_blocks(halo_up, top)
    far_blocks(halo_down, bottom)
    own_copy = remote(0, own, partner, (i, j, other))
    far_s = remote(17, halo_up.at[2:5], south.at[2:5], (up, j, h))
    far_n = remote(18, halo_down.at[2:5], north.at[2:5], (down, j, h))
    own_copy.start()
    launch([far_s], [far_n])
    ups, downs, boths = ups + [far_s], downs + [far_n], boths + [misc_copy, own_copy]

    table = lut[...]
    low = dot_nt(one_hot(iota((LANES, LANES), 0) == iota((LANES, LANES), 1)), (table & 255).astype(F32).astype(BF16))
    pair_lane = iota((LANES, 2 * LANES), 1).astype(F32)
    for s in range(16):
        pick[LANES * s : LANES * (s + 1)] = one_hot(jnp.broadcast_to(low[:, s : s + 1], (LANES, 2 * LANES)) == pair_lane)
    pair_of = (table >> 8).astype(F32)

    count = cnt[...]
    live = [jnp.where(count > s, 1.0, 0.0).astype(F32) for s in range(16)]
    loads[8].wait()
    w_row = w[...]
    w_column = jnp.sum(
        jnp.where(iota((LANES, LANES), 0) == iota((LANES, LANES), 1), w_row, 0.0), axis=1, keepdims=True
    )
    squares = jnp.zeros((LANES, LANES), F32)
    for s in range(8):
        first, second = y[8 * h + s].astype(F32), y[16 + 8 * h + s].astype(F32)
        squares = squares + jnp.where(count > 8 * h + s, 1.0, 0.0) * (first * first + second * second)
    squares = squares * w_column

    increment = inc[...]
    known = 0.5 * jnp.sum(increment * increment, axis=0, keepdims=True)
    known = known + 0.5 * jnp.sum(squares, axis=0, keepdims=True)

    misc_copy.wait_recv()
    here, there = pl.ds(pl.multiple_of(h * half, 8), half), pl.ds(pl.multiple_of(other * half, 8), half)
    for n in range(3):
        full[n, here, :] = misc[n]
        full[n, there, :] = misc_in[n]
    mixing = full[0][:, 0:full_levels].astype(BF16)
    eye80 = one_hot(iota((full_levels, full_levels), 0) == iota((full_levels, full_levels), 1))
    mixing_back = dot_tn(mixing, eye80).astype(BF16)
    jac_t = full[1].astype(BF16)
    weighted = (full[1] * w_row).astype(BF16)
    gram_full = dot_nt(weighted, jac_t)
    image_matrix = gram_full + dot(gram_full.astype(BF16), mixing)
    both = jnp.concatenate([mixing, image_matrix.astype(BF16)], axis=0)

    for s in range(16):
        span = slice(LANES * s, LANES * (s + 1))
        first = dot(weighted, y[s]) * live[s]
        second = dot(weighted, y[16 + s]) * live[s]
        slots[:, span] = jnp.concatenate(
            [first, second, jnp.broadcast_to(live[s], (16, LANES))], axis=0
        ).astype(BF16)
    def masked(q):
        pieces = []
        for s in range(16):
            match = jnp.broadcast_to(jnp.where(pair_of[s : s + 1, :] == q, 1.0, 0.0), (16, LANES)).astype(BF16)
            tiles = slots[:, LANES * s : LANES * (s + 1)].reshape(slots.shape[0] // 16, 16, LANES)
            pieces.append((tiles * match[None]).reshape(slots.shape[0], LANES))
        return jnp.concatenate(pieces, axis=1)

    for q in range(0, rows // 2, 2):
        moved = dot(jnp.concatenate([masked(q), masked(q + 1)], axis=0), pick[...]).astype(BF16)
        for t in (0, 1):
            grid[:, 2 * LANES * (q + t) : 2 * LANES * (q + t + 1)] = moved[slots.shape[0] * t : slots.shape[0] * (t + 1)]

    def edge_selector(core):
        number, lane = iota((16, 4 * LANES), 0), iota((16, 4 * LANES), 1)
        return one_hot((number >> 2) * LANES + (number & 3) + core * (LANES - HALO) == lane)

    outgoing, incoming = edge_selector(h), edge_selector(other)
    depth = slots.shape[0]
    for q in range(4):
        block = jnp.concatenate([grid[:, at_row(4 * g + q)] for g in range(4)], axis=1)
        edge[:, 256 * q : 256 * q + depth] = dot_nt(outgoing, block).astype(BF16)
        edge[:, 256 * q + depth : 256 * (q + 1)] = jnp.zeros((16, 256 - depth), BF16)
    late_up = [
        remote(12, grid.at[:, 14 * LANES : 16 * LANES], grid_s, (up, j, h)),
        remote(15, edge.at[:, 768:1024], edge_s, (up, side, other)),
    ]
    late_down = [
        remote(13, grid.at[:, 0 : 2 * LANES], grid_n, (down, j, h)),
        remote(16, edge.at[:, 0:256], edge_n, (down, side, other)),
    ]
    late_side = [remote(14, edge, edge_in, (i, side, other))]
    launch(late_up, late_down, late_side)
    ups, downs, boths = ups + late_up, downs + late_down, boths + late_side

    lane_row = iota((1, LANES), 1)
    patched = jnp.where(h == 0, lane_row - (LANES - HALO), HALO - 1 - lane_row) >= 0
    own_lanes = jnp.where(h == 0, LANES // 2 - 1 - lane_row, lane_row - LANES // 2) >= 0
    number, lane = iota((16, 3 * LANES), 0), iota((16, 3 * LANES), 1)
    place = one_hot(((number >> 2) * LANES + (number & 3) + other * (LANES - HALO) == lane) & (number < 12))
    mask_s = jnp.where(i > 0, 1.0, 0.0).astype(F32)
    mask_n = jnp.where(i < nlat - 1, 1.0, 0.0).astype(F32)

    def row_mask(e):
        return mask_s if e < HALO else mask_n if e >= HALO + rows else None

    def keep(e, value):
        mask = row_mask(e)
        return value if mask is None else value * mask

    targets = (x0, hu, hv)

    def assemble(e, sources, patches):
        for f in range(len(sources[0])):
            for span, source, patch in zip((here, there), sources, patches):
                value = source[f]
                if patch is not None:
                    value = jnp.where(patched, patch[:, at_row(f)], value)
                targets[f][span, at_row(e)] = keep(e, value)

    def rows_of(ref, q):
        blocks = [ref[q, f].astype(F32) for f in range(3)]
        return [[block[half * t : half * (t + 1)] for block in blocks] for t in (0, 1)]

    def patch_of(ref):
        return dot_tn(ref[:, 0 : 3 * half], place)

    group_of = {}
    for r in range(rows):
        g = max(n for n, start in enumerate(GROUPS) if start <= r and r < start + 3)
        if r in (6, 7, 8):
            g = 2
        if r in (9, 10):
            g = 3
        group_of[r] = (g, r - GROUPS[g])
    found = {}

    def patches_for(r):
        g, t = group_of[r]
        if g not in found:
            found.clear()
            found[g] = (patch_of(strip_in.at[h, g]), patch_of(strip_in.at[other, g]))
        return [value[half * t : half * (t + 1)] for value in found[g]]

    own_copy.wait_recv()
    for q in range(rows // 2):
        mine, theirs = rows_of(own, q), rows_of(partner, q)
        for t in (0, 1):
            assemble(HALO + 2 * q + t, (mine[t], theirs[t]), (None, None))

    def relay(arrived, condition, n, source, target):
        copy = remote(n, source, target, (i, j, other))

        @pl.when(condition)
        def _():
            arrived.wait_recv()
            copy.start()

        return copy

    relays_s = [relay(near_s, has_down, 4, south.at[0:2], south_in.at[0:2])]
    relays_n = [relay(near_n, has_up, 5, north.at[0:2], north_in.at[0:2])]

    for k in (0, 1):
        remote(6, strip_e, strip_in.at[k], (i, east, 0), 6 + k).wait_recv()
    for r in range(rows):
        patches = patches_for(r)
        for f in range(3):
            for span, patch in zip((here, there), patches):
                current = targets[f][span, at_row(HALO + r)]
                targets[f][span, at_row(HALO + r)] = jnp.where(patched, patch[:, at_row(f)], current)

    diffusion = full[2]
    centre = 1.0 - 4.0 * diffusion

    def step_row(x, e):
        value, above, below = x[:, at_row(e)], x[:, at_row(e + 1)], x[:, at_row(e - 1)]
        eastern = pltpu.roll(value, LANES - 1, 1)
        western = pltpu.roll(value, 1, 1)
        return (
            centre * value
            + diffusion * ((above + below) + (eastern + western))
            + hu[:, at_row(e)] * (western - eastern)
            + hv[:, at_row(e)] * (below - above)
        )

    def back_row(x, e):
        value, above, below = x[:, at_row(e)], x[:, at_row(e + 1)], x[:, at_row(e - 1)]
        spread, drift = diffusion * value, hu[:, at_row(e)] * value
        eastern = pltpu.roll(spread + drift, LANES - 1, 1)
        western = pltpu.roll(spread - drift, 1, 1)
        return (
            centre * value
            + (eastern + western)
            + (diffusion + hv[:, at_row(e + 1)]) * above
            + (diffusion - hv[:, at_row(e - 1)]) * below
        )

    def coupled(matrix, values):
        joined = jnp.concatenate(values, axis=1).astype(BF16)
        mixed = dot(matrix, joined)
        return [value + mixed[:, at_row(n)] for n, value in enumerate(values)]

    def pairwise(first, last):
        return [tuple(range(e, min(e + 2, last + 1))) for e in range(first, last + 1, 2)]

    def both_of(pair, source, target):
        values = [step_row(source, e) for e in pair]
        joined = jnp.concatenate(values, axis=1).astype(BF16)
        result = dot(both, joined)
        for n, e in enumerate(pair):
            target[:, at_row(e)] = result[full_levels:, at_row(n)]
        return [value + result[0:full_levels, at_row(n)] for n, value in enumerate(values)]

    def misfit(states, pair, target, step):
        parts = []
        for state, e in zip(states, pair):
            r = e - HALO
            if 0 <= r < rows:
                moved = grid[full_levels * step : full_levels * (step + 1), at_row(r)].astype(F32)
                alive = grid[2 * full_levels : depth, at_row(r)].astype(F32)[0:1]
                parts.append(state * (alive * target[:, at_row(e)] - 2.0 * moved))
        return sum(parts)

    def advance(pair):
        states = both_of(pair, x0, hold)
        for e, value in zip(pair, states):
            x1[:, at_row(e)] = keep(e, value)
        return misfit(states, pair, hold, 0)

    def advance_second(pair):
        return misfit(both_of(pair, x1, sm), pair, sm, 1)

    total = jnp.zeros((full_levels, LANES), F32)
    for pair in pairwise(5, 18):
        total = total + advance(pair)
    for pair in pairwise(6, 17):
        total = total + advance_second(pair)

    @pl.when(has_down)
    def _():
        relays_s[0].wait_recv()
        for k in (0, 1):
            remote(8, strip_e.at[5], strip_s.at[k], (i, east, 0), 8 + k).wait_recv()

    @pl.when(has_up)
    def _():
        relays_n[0].wait_recv()
        for k in (0, 1):
            remote(9, strip_e.at[0], strip_n.at[k], (i, east, 0), 10 + k).wait_recv()

    patch_s = (patch_of(strip_s.at[h]), patch_of(strip_s.at[other]))
    patch_n = (patch_of(strip_n.at[h]), patch_of(strip_n.at[other]))

    def halo_rows(ref, which):
        first = ref[2 * which].astype(F32)
        winds = [ref[1 if which == 0 else 4].astype(F32), None]
        return [
            [first[half * t : half * (t + 1)]] + ([] if winds[t] is None else [winds[t][0:half], winds[t][half:]])
            for t in (0, 1)
        ]

    def outer_rows(which):
        for sign, edge_row, refs, patches in (
            (-1, HALO - 1, (south, south_in), patch_s),
            (1, HALO + rows, (north, north_in), patch_n),
        ):
            blocks = [halo_rows(ref, which) for ref in refs]
            for t in (0, 1):
                r = 2 * which + t
                e = edge_row + sign * r
                spot = 2 - r if sign < 0 else r
                fit = [None if r == 3 else value[half * spot : half * (spot + 1)] for value in patches]
                assemble(e, [block[t] for block in blocks], fit)
            if which == 1:
                winds = [ref[3].astype(F32) for ref in refs]
                fit = [value[half : 2 * half] for value in patches]
                e = edge_row + sign
                for f in (1, 2):
                    for span, wind, patch in zip((here, there), winds, fit):
                        value = wind[half * (f - 1) : half * f]
                        targets[f][span, at_row(e)] = keep(e, jnp.where(patched, patch[:, at_row(f)], value))

    outer_rows(0)
    for pair in ((3, 4), (19, 20)):
        total = total + advance(pair)
    for pair in ((4, 5), (18, 19)):
        total = total + advance_second(pair)
    near[0] = known + 0.5 * jnp.sum(jnp.where(own_lanes, total, 0.0), axis=0, keepdims=True)
    own_part = remote(22, near.at[0], near.at[1], (i, j, 1))
    first_round = [remote(22, near.at[0], near.at[2 + 2 * t + h], (a, b, 1)) for t, (a, b) in enumerate(plane)]
    for t in sorted(range(len(plane)), key=lambda t: -min(t // laps + 1, nlat - t // laps - 1)):
        first_round[t].start()

    @pl.when(follows)
    def _():
        own_part.start()

    relays_s.append(relay(far_s, has_down, 19, south.at[2:5], south_in.at[2:5]))
    relays_n.append(relay(far_n, has_up, 20, north.at[2:5], north_in.at[2:5]))
    late_side[0].wait_recv()

    @pl.when(has_down)
    def _():
        for copy in late_up:
            copy.wait_recv()

    @pl.when(has_up)
    def _():
        for copy in late_down:
            copy.wait_recv()

    for q in range(4):
        value = dot_tn(edge_in[:, 256 * q : 256 * q + depth], incoming)
        for g in range(4):
            r = 4 * g + q
            f1[:, at_row(r + 2)] = jnp.where(patched, value[:, at_row(g)], grid[:, at_row(r)].astype(F32))
    f1[:, at_row(0)] = grid_s[:, at_row(0)].astype(F32)
    value = dot_tn(edge_s[:, 0:depth], incoming)
    f1[:, at_row(1)] = jnp.where(patched, value[:, at_row(3)], grid_s[:, at_row(1)].astype(F32))
    value = dot_tn(edge_n[:, 0:depth], incoming)
    f1[:, at_row(18)] = jnp.where(patched, value[:, at_row(0)], grid_n[:, at_row(0)].astype(F32))
    f1[:, at_row(19)] = grid_n[:, at_row(1)].astype(F32)

    @pl.when(has_down)
    def _():
        relays_s[1].wait_recv()

    @pl.when(has_up)
    def _():
        relays_n[1].wait_recv()

    outer_rows(1)
    for pair in ((1, 2), (21, 22)):
        advance(pair)
    for pair in ((2, 3), (20, 21)):
        advance_second(pair)

    def force(e, target, step):
        moved = f1[full_levels * step : full_levels * (step + 1), at_row(e - 2)]
        alive = f1[2 * full_levels : 2 * full_levels + 1, at_row(e - 2)]
        return alive * target[:, at_row(e)] - moved

    for pair in pairwise(2, 21):
        values = coupled(mixing_back, [force(e, sm, 1) for e in pair])
        for e, value in zip(pair, values):
            x0[:, at_row(e)] = keep(e, value)

    for pair in pairwise(3, 20):
        values = [back_row(x0, e) + force(e, hold, 0) for e in pair]
        for e, value in zip(pair, coupled(mixing_back, values)):
            sm[:, at_row(e)] = keep(e, value)

    whole_first = remote(22, near.at[1:crowd], near.at[1:crowd], (i, j, other))
    sent_first = remote(22, near.at[1 : crowd // 2], near.at[1 : crowd // 2], (i, j, other))
    second_round = [remote(23, far.at[0], far.at[t + 1], (a, b, c)) for t, (a, b) in enumerate(line) for c in (0, 1)]
    handed = remote(24, far.at[0], far.at[ring], (i, j, 0))

    @pl.when(leads)
    def _():
        whole_first.wait_recv()
        part = near[0]
        for t in range(1, crowd):
            part = part + near[t]
        far[0] = part
        for t in sorted(range(len(second_round)), key=lambda t: -min(t // 2 + 1, ring - t // 2 - 1)):
            second_round[t].start()
        handed.start()

    for r in range(rows):
        x1[:, at_row(r)] = back_row(sm, r + HALO)
    for q in range(rows // 2):
        back[q] = jnp.concatenate([x1[there, at_row(2 * q)], x1[there, at_row(2 * q + 1)]], axis=0).astype(BF16)
    final = remote(21, back, back_in, (i, j, other))
    final.start()

    final.wait_recv()
    for q in range(rows // 2):
        received = back_in[q].astype(F32)
        for t in (0, 1):
            r = 2 * q + t
            adjoint = jnp.where(own_lanes, x1[here, at_row(r)], received[half * t : half * (t + 1)])
            out_ref[pl.ds(r, half, stride=rows), :] = inc[pl.ds(r, half, stride=rows), :] + adjoint
    whole_second = remote(23, far.at[1:ring], far.at[1:ring], (i, j, other))
    sent_second = remote(23, far_sent, far_sent, (i, j, other))
    whole_second.wait_recv()

    @pl.when(follows)
    def _():
        handed.wait_recv()
        far[0] = far[ring]

    part = far[0]
    for t in range(1, ring):
        part = part + far[t]
    cells = full_levels * rows * LANES * nlat * nlon
    cost_ref[...] = jnp.broadcast_to(jnp.sum(part, axis=1, keepdims=True) * (1.0 / cells), (1, LANES))
    for copy in boths + [final, sent_first]:
        copy.wait_send()

    @pl.when(follows)
    def _():
        own_part.wait_send()

    @pl.when(leads)
    def _():
        sent_second.wait_send()
        handed.wait_send()

    @pl.when(has_up)
    def _():
        for copy in ups + relays_n:
            copy.wait_send()

    @pl.when(has_down)
    def _():
        for copy in downs + relays_s:
            copy.wait_send()


def deliver(gradient, cost, gradient_out, cost_out, single, sem):
    single[...] = cost[:, 0:1]
    copies = (
        pltpu.make_async_copy(gradient, gradient_out, sem.at[0]),
        pltpu.make_async_copy(single, cost_out, sem.at[1]),
    )
    for copy in copies:
        copy.start()
    for copy in copies:
        copy.wait()


def body(nlat, nlon, increment, wind_u, wind_v, diffusion, mixing, jacobian, obs_weight, innovation, counts, column_lookup):
    half, rows, width = increment.shape
    channels = jacobian.shape[0]
    wide = (HALO * 2 + rows) * width
    levels = 2 * half
    depth = 2 * levels + 16
    anywhere = pl.BlockSpec(memory_space=pltpu.MemorySpace.HBM)
    vmem = pl.BlockSpec(memory_space=pltpu.VMEM)
    grid_size = rows * width
    far = nlon // 2 if nlon % 2 == 0 else nlon
    near = nlat * (nlon // far) * 2
    copies = 25
    strip = (16, width)
    scratch = [
        ((half * rows, width), F32), ((half * rows, width), F32), ((half * rows, width), F32),
        ((1, half), F32), ((half, levels), F32), ((half, channels), BF16), ((1, channels), F32),
        ((32, channels, width), BF16), ((16, width), jnp.int32),
        ((8, 3, levels, width), BF16), ((8, 3, levels, width), BF16),
        ((3, half, width), F32), ((3, half, width), F32), ((3, levels, width), F32),
        *[((5, levels, width), BF16)] * 6,
        ((6, *strip), BF16), ((6, *strip), BF16), ((2, 6, *strip), BF16), ((2, *strip), BF16), ((2, *strip), BF16),
        ((depth, grid_size), BF16), ((grid_size, 2 * width), BF16), ((depth, grid_size), BF16),
        ((depth, 2 * width), BF16), ((depth, 2 * width), BF16),
        ((16, 1024), BF16), ((16, 1024), BF16), ((16, 256), BF16), ((16, 256), BF16),
        ((levels, wide), F32), ((levels, wide), F32), ((levels, wide), F32), ((levels, wide), F32), ((levels, wide), F32),
        ((depth, 20 * width), F32),
        ((levels, wide), F32), ((8, levels, width), BF16), ((8, levels, width), BF16),
        ((near, 1, width), F32), ((far + 1, 1, width), F32), ((2 * far - 2, 1, width), F32),
    ]
    gradient, cost = pl.pallas_call(
        functools.partial(kernel, (nlat, nlon, half, rows)),
        out_shape=(
            jax.ShapeDtypeStruct((half * rows, width), F32),
            jax.ShapeDtypeStruct((1, width), F32),
        ),
        in_specs=[anywhere] * 9 + [vmem],
        out_specs=(vmem, vmem),
        scratch_shapes=[pltpu.VMEM(*entry) for entry in scratch]
        + [
            pltpu.SemaphoreType.DMA((9,)),
            pltpu.SemaphoreType.DMA((copies,)),
            pltpu.SemaphoreType.DMA((copies,)),
        ],
        compiler_params=pltpu.CompilerParams(
            collective_id=0, has_side_effects=True, vmem_limit_bytes=24 * 1024 * 1024
        ),
    )(
        *[
            pltpu.with_memory_space_constraint(operand, pltpu.MemorySpace.HBM)
            for operand in (
                increment.reshape(half * rows, width),
                wind_u.reshape(half * rows, width),
                wind_v.reshape(half * rows, width),
                diffusion.reshape(1, half),
                mixing,
                jacobian.T,
                obs_weight.reshape(1, channels),
                innovation.reshape(32, channels, width),
                column_lookup.reshape(16, width),
            )
        ],
        counts,
    )
    gradient, cost = pl.pallas_call(
        deliver,
        out_shape=(
            jax.ShapeDtypeStruct((half * rows, width), F32),
            jax.ShapeDtypeStruct((1, 1), F32),
        ),
        in_specs=[vmem, vmem],
        out_specs=(pl.BlockSpec(memory_space=pl.ANY), pl.BlockSpec(memory_space=pl.ANY)),
        scratch_shapes=[pltpu.VMEM((1, 1), F32), pltpu.SemaphoreType.DMA((2,))],
        compiler_params=pltpu.CompilerParams(vmem_limit_bytes=1024 * 1024),
    )(gradient, cost)
    return gradient.reshape(increment.shape), cost.reshape(())


def solution(mesh):
    field = P("lev", "lat", "lon")
    in_specs = (
        field,
        field,
        field,
        P("lev"),
        P("lev", None),
        P(None, "lev"),
        P(),
        P(None, "lat", "lon", None, None, None),
        P("lat", "lon"),
        P("lat", "lon", None),
    )
    return jax.shard_map(
        functools.partial(body, mesh.shape["lat"], mesh.shape["lon"]),
        mesh=mesh,
        in_specs=in_specs,
        out_specs=(field, P()),
        check_vma=False,
    )
```
